256 devices in a mesh: row: 32 (over z_lo, y, core), col: 8 (over x, z_hi).
Axes of the slice: x: 4, y: 4, z: 8 (z_hi: 2, z_lo: 4; z = z_hi * 4 + z_lo), core: 2. Of those that a mesh axis runs over, the one named last changes fastest.
Arguments:
- pair_rep: bfloat16 [2048, 2048, 128], P('row', 'col'), may hold values from -6 to 6
- bias_weight: bfloat16 [128, 12], replicated, may hold values from -0.5 to 0.5
- head_weight: float32 [12], replicated, may hold values from -1 to 1
- queries: float32 [192, 2048], P(None, 'row'), may hold values from -48 to 48, as said below
- key_vectors: float32 [192, 2048], P(None, 'col'), may hold values from -48 to 48, as said below
- values: float32 [192, 2048], P(None, 'col'), may hold values from -6 to 6
- query_points: float32 [3, 48, 2048], P(None, None, 'row'), may hold values from -6 to 6
- key_points: float32 [3, 48, 2048], P(None, None, 'col'), may hold values from -6 to 6
- value_points: float32 [3, 96, 2048], P(None, None, 'col'), may hold values from -6 to 6
- rotations: float32 [3, 3, 2048], replicated, may hold values from -1 to 1, as said below
- translations: float32 [3, 2048], replicated, may hold values from -12 to 12
- residue_count: int32 [1], replicated, may hold values from 1024 to 2048
- grad_output: float32 [192, 2048], P(None, 'row'), may hold values from -6 to 6
- grad_points: float32 [3, 96, 2048], P(None, None, 'row'), may hold values from -6 to 6
- grad_pair: bfloat16 [2048, 12, 128], P('row'), may hold values from -2 to 2
Outputs:
- pair_grad: bfloat16 [2048, 2048, 128], P('row', 'col')
- query_grad: float32 [192, 2048], P(None, ('row', 'col'))
- query_point_grad: float32 [3, 48, 2048], P(None, None, ('row', 'col'))
- query_frame_grad: float32 [3, 4, 2048], P(None, None, ('row', 'col'))
- key_grad: float32 [192, 2048], P(None, ('col', 'row'))
- value_grad: float32 [192, 2048], P(None, ('col', 'row'))
- key_point_grad: float32 [3, 48, 2048], P(None, None, ('col', 'row'))
- value_point_grad: float32 [3, 96, 2048], P(None, None, ('col', 'row'))
- key_frame_grad: float32 [3, 4, 2048], P(None, None, ('col', 'row'))
- bias_weight_grad: float32 [128, 12], replicated
- head_weight_grad: float32 [12], replicated
The draws below stay inside these ranges and needn't reach their ends.
Inputs may be any that keep to these rules, and one draw needn't show every extreme that they name: `queries`: entries of order one, except a few residues whose vectors are much larger. `key_vectors`: entries of order one, except a few residues whose vectors are much larger. `rotations`: each residue's 3 x 3 matrix is a rotation: orthonormal with determinant one.
All inputs are finite; a program needn't handle non-finite values.
Results may differ from the reference program's by a relative error of at most 0.0049.
Values sent between devices are 32-bit elements; how exact they have to be, the bound alone decides.
A program may use at most 128 MiB of HBM per device.

```python
import math
import jax
import jax.numpy as jnp
from jax import lax

N = 2048
H = 12
C = 16
PQ = 4
PV = 8
CZ = 128


def drawn_vectors(key):
    base_key = jax.random.fold_in(key, 11)
    first, second = jax.random.split(base_key, 2)
    query_draw = jnp.clip(jax.random.normal(first, (H * C, N), jnp.float32), -4.0, 4.0)
    key_draw = jnp.clip(jax.random.normal(second, (H * C, N), jnp.float32), -4.0, 4.0)
    return (query_draw, key_draw)


def draw_queries(key, part):
    return drawn_vectors(key)[0]


def draw_key_vectors(key, part):
    return drawn_vectors(key)[1]


def draw_rotations(key, part):
    base_key = jax.random.fold_in(key, 23)
    first, second = jax.random.split(base_key)
    scalar = jax.random.uniform(first, (N,), jnp.float32, 0.5, 1.5)
    vector = jax.random.normal(second, (3, N), jnp.float32)
    length = jnp.sqrt(scalar ** 2 + jnp.sum(vector ** 2, axis=0))
    qw = scalar / length
    qx = vector[0] / length
    qy = vector[1] / length
    qz = vector[2] / length
    first_row = jnp.stack([1 - 2 * (qy * qy + qz * qz), 2 * (qx * qy - qw * qz), 2 * (qx * qz + qw * qy)])
    second_row = jnp.stack([2 * (qx * qy + qw * qz), 1 - 2 * (qx * qx + qz * qz), 2 * (qy * qz - qw * qx)])
    third_row = jnp.stack([2 * (qx * qz - qw * qy), 2 * (qy * qz + qw * qx), 1 - 2 * (qx * qx + qy * qy)])
    return jnp.stack([first_row, second_row, third_row])


def levels(stream_key, dims, shards, least, high):
    factor_of, own = 1.0, jax.random.fold_in(stream_key, 6)
    for position, parts in shards:
        heights = jnp.exp(jax.random.uniform(jax.random.fold_in(own, position), (parts,), jnp.float32, least / len(shards), high / len(shards)))
        factor_of = factor_of * jnp.repeat(heights, dims[position] // parts).reshape([-1 if axis == position else 1 for axis in range(len(dims))])
    return factor_of


def gaussian(own_key, shape, deviation, most, pieces=(), kind=jnp.bfloat16):
    loudness = levels(own_key, shape, pieces, -0.22, 0.18) if pieces else 1.0
    drawn = jax.random.normal(own_key, shape, jnp.float32) * deviation * loudness
    return jnp.minimum(jnp.maximum(drawn, -most), most).astype(kind)


def setup_inputs(seed: int = 0) -> dict:
    key_list = jax.random.split(jax.random.key(seed), 16)
    return {
        "pair_rep": gaussian(key_list[0], (N, N, CZ), 1.0, 6.0, ((0, 32), (1, 8))),
        "bias_weight": gaussian(key_list[1], (CZ, H), CZ ** -0.5, 0.5),
        "head_weight": jnp.clip(jax.random.uniform(key_list[2], (H,), jnp.float32, -1.0, 1.0), -1.0, 1.0),
        "queries": draw_queries(jax.random.fold_in(key_list[15], 71), 0),
        "key_vectors": draw_key_vectors(jax.random.fold_in(key_list[15], 71), 0),
        "values": gaussian(key_list[5], (H * C, N), 1.0, 6.0, ((1, 8),), jnp.float32),
        "query_points": gaussian(key_list[6], (3, H * PQ, N), 1.0, 6.0, ((2, 32),), jnp.float32),
        "key_points": gaussian(key_list[7], (3, H * PQ, N), 1.0, 6.0, ((2, 8),), jnp.float32),
        "value_points": gaussian(key_list[8], (3, H * PV, N), 1.0, 6.0, ((2, 8),), jnp.float32),
        "rotations": draw_rotations(jax.random.fold_in(key_list[15], 71), 0),
        "translations": gaussian(key_list[10], (3, N), 2.0, 12.0, (), jnp.float32),
        "residue_count": jax.random.randint(key_list[11], (1,), N // 2, N + 1).astype(jnp.int32),
        "grad_output": gaussian(key_list[12], (H * C, N), 1.0, 6.0, ((1, 32),), jnp.float32),
        "grad_points": gaussian(key_list[13], (3, H * PV, N), 1.0, 6.0, ((2, 32),), jnp.float32),
        "grad_pair": gaussian(key_list[14], (N, H, CZ), 0.3, 2.0, ((0, 32),)),
    }


HIGHEST = lax.Precision.HIGHEST

def globalize(rotation, offset, local):
    return jnp.einsum('xym,ykm->xkm', rotation, local, precision=HIGHEST) + offset[:, None, :]

def rotate_back(rotation, vector):
    return jnp.einsum('xym,xkm->ykm', rotation, vector, precision=HIGHEST)

def frame_terms(grad_global, local):
    rotation_part = jnp.einsum('xkm,ykm->xym', grad_global, local, precision=HIGHEST)
    return jnp.concatenate([rotation_part, lax.optimization_barrier(jnp.sum(grad_global, axis=1))[:, None, :]], axis=1)

def output_frame_terms(point_out, offset, cotan_local, grad_rotated):
    rotation_part = jnp.einsum('xkm,ykm->xym', point_out - offset[:, None, :], cotan_local, precision=HIGHEST)
    return jnp.concatenate([rotation_part, -lax.optimization_barrier(jnp.sum(grad_rotated, axis=1))[:, None, :]], axis=1)

def reference(pair_rep, bias_weight, head_weight, queries, key_vectors, values, query_points, key_points, value_points, rotations, translations, residue_count, grad_output, grad_points, grad_pair):
    logit_scale = math.sqrt(1.0 / 3.0)
    point_scale = math.sqrt(2.0 / (9.0 * PQ))
    inner_scale = 1.0 / math.sqrt(C)
    distance_coef = 0.5 * logit_scale * point_scale * jax.nn.softplus(head_weight)
    query_global = globalize(rotations, translations, query_points).reshape(3, H, PQ, N)
    key_global = globalize(rotations, translations, key_points).reshape(3, H, PQ, N)
    value_global = globalize(rotations, translations, value_points).reshape(3, H, PV, N)
    grad_global = jnp.einsum('xym,ykm->xkm', rotations, grad_points, precision=HIGHEST)
    grad_heads = grad_global.reshape(3, H, PV, N)
    key_heads = key_vectors.reshape(H, C, N)
    value_heads = values.reshape(H, C, N)
    query_heads = queries.reshape(H, C, N)
    out_heads = grad_output.reshape(H, C, N)
    valid = jnp.arange(N) < residue_count[0]
    pair_weight = bias_weight.astype(jnp.float32)
    block = min(128, N)

    def step(carry, start):
        pair_block = lax.dynamic_slice_in_dim(pair_rep, start, block, 0).astype(jnp.float32)
        cotan_pair = lax.dynamic_slice_in_dim(grad_pair, start, block, 0).astype(jnp.float32)
        query_block = lax.dynamic_slice_in_dim(query_heads, start, block, 2)
        out_block = lax.dynamic_slice_in_dim(out_heads, start, block, 2)
        qglobal_block = lax.dynamic_slice_in_dim(query_global, start, block, 3)
        gglobal_block = lax.dynamic_slice_in_dim(grad_heads, start, block, 3)
        inner = jnp.einsum('hci,hcj->hij', query_block, key_heads, precision=HIGHEST)
        cross = jnp.einsum('xhpi,xhpj->hij', qglobal_block, key_global, precision=HIGHEST)
        distance = lax.optimization_barrier(jnp.sum(qglobal_block ** 2, axis=(0, 2)))[:, :, None] + lax.optimization_barrier(jnp.sum(key_global ** 2, axis=(0, 2)))[:, None, :] - 2.0 * cross
        bias = jnp.einsum('ijc,ch->hij', pair_block, pair_weight, precision=HIGHEST)
        logits = logit_scale * (inner_scale * inner + bias) - distance_coef[:, None, None] * distance
        logits = jnp.where(valid[None, None, :], logits, jnp.float32(-1000000000.0))
        row_peak = lax.optimization_barrier(jnp.max(logits, axis=2, keepdims=True))
        exponent = jnp.exp(logits - row_peak)
        attention = exponent / lax.optimization_barrier(jnp.sum(exponent, axis=2, keepdims=True))
        product = jnp.einsum('hci,hcj->hij', out_block, value_heads, precision=HIGHEST) + jnp.einsum('xhvi,xhvj->hij', gglobal_block, value_global, precision=HIGHEST) + jnp.einsum('ijc,ihc->hij', pair_block, cotan_pair, precision=HIGHEST)
        delta = lax.optimization_barrier(jnp.sum(attention * product, axis=2, keepdims=True))
        logit_grad = attention * (product - delta)
        query_grad = logit_scale * inner_scale * jnp.einsum('hij,hcj->hci', logit_grad, key_heads, precision=HIGHEST)
        row_sum = lax.optimization_barrier(jnp.sum(logit_grad, axis=2))
        qpoint_grad = -2.0 * distance_coef[None, :, None, None] * (qglobal_block * row_sum[None, :, None, :] - jnp.einsum('hij,xhpj->xhpi', logit_grad, key_global, precision=HIGHEST))
        qpoint_flat = qpoint_grad.reshape(3, H * PQ, block)
        point_out = jnp.einsum('hij,xhvj->xhvi', attention, value_global, precision=HIGHEST).reshape(3, H * PV, block)
        rot_block = lax.dynamic_slice_in_dim(rotations, start, block, 2)
        shift_block = lax.dynamic_slice_in_dim(translations, start, block, 1)
        local_block = lax.dynamic_slice_in_dim(query_points, start, block, 2)
        cotan_local = lax.dynamic_slice_in_dim(grad_points, start, block, 2)
        gflat_block = gglobal_block.reshape(3, H * PV, block)
        qlocal_grad = rotate_back(rot_block, qpoint_flat)
        qframe = frame_terms(qpoint_flat, local_block) + output_frame_terms(point_out, shift_block, cotan_local, gflat_block)
        key_part = logit_scale * inner_scale * jnp.einsum('hij,hci->hcj', logit_grad, query_block, precision=HIGHEST)
        value_part = jnp.einsum('hij,hci->hcj', attention, out_block, precision=HIGHEST)
        col_sum = lax.optimization_barrier(jnp.sum(logit_grad, axis=1))
        kpoint_part = 2.0 * distance_coef[None, :, None, None] * (jnp.einsum('hij,xhpi->xhpj', logit_grad, qglobal_block, precision=HIGHEST) - key_global * col_sum[None, :, None, :])
        vpoint_part = jnp.einsum('hij,xhvi->xhvj', attention, gglobal_block, precision=HIGHEST)
        grad_rounded = lax.optimization_barrier(logit_grad.astype(jnp.bfloat16)).astype(jnp.float32)
        attn_rounded = lax.optimization_barrier(attention.astype(jnp.bfloat16)).astype(jnp.float32)
        weight_part = logit_scale * jnp.einsum('ijc,hij->ch', pair_block, grad_rounded, precision=HIGHEST)
        distance_part = lax.optimization_barrier(jnp.sum(logit_grad * distance, axis=(1, 2)))
        pair_grad = (logit_scale * jnp.einsum('hij,ch->ijc', grad_rounded, pair_weight, precision=HIGHEST) + jnp.einsum('hij,ihc->ijc', attn_rounded, cotan_pair, precision=HIGHEST)).astype(jnp.bfloat16)
        new_carry = (carry[0] + key_part, carry[1] + value_part, carry[2] + kpoint_part, carry[3] + vpoint_part, carry[4] + weight_part, carry[5] + distance_part)
        return (new_carry, (pair_grad, query_grad.reshape(H * C, block), qlocal_grad, qframe))
    initial = (jnp.zeros((H, C, N), jnp.float32), jnp.zeros((H, C, N), jnp.float32), jnp.zeros((3, H, PQ, N), jnp.float32), jnp.zeros((3, H, PV, N), jnp.float32), jnp.zeros((CZ, H), jnp.float32), jnp.zeros((H,), jnp.float32))
    starts = jnp.arange(N // block, dtype=jnp.int32) * block
    carry, stacked = lax.scan(step, initial, starts)
    pair_grad = stacked[0].reshape(N, N, CZ)
    query_grad = jnp.transpose(stacked[1], (1, 0, 2)).reshape(H * C, N)
    query_point_grad = jnp.transpose(stacked[2], (1, 2, 0, 3)).reshape(3, H * PQ, N)
    query_frame_grad = jnp.transpose(stacked[3], (1, 2, 0, 3)).reshape(3, 4, N)
    kpoint_flat = carry[2].reshape(3, H * PQ, N)
    vpoint_flat = carry[3].reshape(3, H * PV, N)
    key_point_grad = rotate_back(rotations, kpoint_flat)
    value_point_grad = rotate_back(rotations, vpoint_flat)
    key_frame_grad = frame_terms(kpoint_flat, key_points) + frame_terms(vpoint_flat, value_points)
    head_weight_grad = carry[5] * (-0.5 * logit_scale * point_scale) * jax.nn.sigmoid(head_weight)
    return (pair_grad, query_grad, query_point_grad, query_frame_grad, carry[0].reshape(H * C, N), carry[1].reshape(H * C, N), key_point_grad, value_point_grad, key_frame_grad, carry[4], head_weight_grad)
```

```python
import functools
import math

import jax
import jax.numpy as jnp
from jax import lax
from jax.experimental import pallas as pl
from jax.experimental.pallas import tpu as pltpu
from jax.sharding import PartitionSpec as P

F32 = jnp.float32
BF16 = jnp.bfloat16
PAD = 16
VMEM_LIMIT = 48 * 1024 * 1024
ZL, YN, CORES = 4, 4, 2
XN, ZH = 4, 2
STRIDE = 40
MESH = pl.DeviceIdType.MESH


def dot(a, b, dims):
    return lax.dot_general(a, b, (dims, ((), ())), preferred_element_type=F32)


TN = ((0,), (0,))
NT = ((1,), (1,))
NN = ((1,), (0,))


def split2(x):
    hi = x.astype(BF16)
    return hi, (x - hi.astype(F32)).astype(BF16)


def split3(x):
    hi = x.astype(BF16)
    rest = x - hi.astype(F32)
    mid = rest.astype(BF16)
    return hi, mid, (rest - mid.astype(F32)).astype(BF16)


def lane_of(shape):
    return lax.broadcasted_iota(jnp.int32, shape, 1)


def merge_stats(parts):
    top = functools.reduce(jnp.maximum, parts)
    lane = lax.rem(lane_of(top.shape), 64)
    out = None
    for part in parts:
        f = jnp.exp(part - top)
        spread = jnp.where(lane < 2 * PAD, pltpu.roll(f, PAD, 1), pltpu.roll(f, 2 * PAD, 1))
        term = part * spread
        out = term if out is None else out + term
    return jnp.where(lane < PAD, top, out)


def push(src, dst, send, recv, row, col):
    copy = pltpu.make_async_remote_copy(
        src_ref=src, dst_ref=dst, send_sem=send, recv_sem=recv,
        device_id={"row": row, "col": col}, device_id_type=MESH,
    )
    copy.start()
    return copy


def mega_kernel(
    heads, n_rows, n_cols, scale,
    rc, pair_hbm, w_t, scaled, gpair, qcat, kcat, gcat, vcat, wq,
    pg_out, kf_out, qf_out, wr_out,
    pair, lbase, dbase, fb0, fb1, rd0, rd1, a_hi, a_lo, d_hi, d_lo,
    qb, gb, stat, stat_z, stat_m, stat_x,
    ks, ks_rx, sy, sy_rx, sz, sz_rx, qs, qs_rx, qz, qz_rx,
    ar_c, ar_y, ar_x, ar_z, ar_s,
    pair_sem, s_send, s_recv, k_send, k_recv, y_send, y_recv, z_send, z_recv,
    q_send, q_recv, a_send, a_recv,
):
    rw = lax.axis_index("row")
    cl = lax.axis_index("col")
    core = lax.rem(rw, CORES)
    yy = lax.rem(rw // CORES, YN)
    zl = rw // (CORES * YN)
    zh = lax.rem(cl, ZH)
    xx = cl // ZH
    row_of = lambda z, y, c: (z * YN + y) * CORES + c
    sibling = (row_of(zl, yy, 1 - core), cl)
    y_peer = lambda k: (row_of(zl, lax.rem(yy + k, YN), core), cl)
    z_peer = lambda k: (row_of(lax.rem(zl + k, ZL), yy, core), cl)
    x_peer = lambda k: (rw, lax.rem(xx + k, XN) * ZH + zh)
    h_peer = (rw, xx * ZH + 1 - zh)
    z8 = zh * ZL + zl

    def ring_peer(k):
        idx = lax.rem(z8 + k, ZL * ZH)
        return (row_of(lax.rem(idx, ZL), yy, core), xx * ZH + idx // ZL)

    everyone = [sibling]
    everyone += [y_peer(k) for k in range(1, YN)]
    everyone += [x_peer(k) for k in range(1, XN)]
    everyone += [ring_peer(k) for k in range(1, ZL * ZH)]
    barrier = pltpu.get_barrier_semaphore()
    for peer in everyone:
        pl.semaphore_signal(
            barrier, inc=1, device_id={"row": peer[0], "col": peer[1]}, device_id_type=MESH
        )

    parts = 4
    rows_per = n_rows // parts
    loads = []
    for p in range(parts):
        piece = pl.ds(p * rows_per, rows_per)
        load = pltpu.make_async_copy(pair_hbm.at[piece], pair.at[piece], pair_sem.at[p])
        load.start()
        loads.append(load)

    for h in range(heads):
        q0, q1, q2 = split3(qcat[h][:, :n_rows])
        k0, k1, k2 = split3(kcat[h])
        lbase[h] = dot(
            jnp.concatenate([q0, q0, q1, q0, q2, q1], 0),
            jnp.concatenate([k0, k1, k0, k2, k0, k1], 0),
            TN,
        )
        g0, g1 = split2(gcat[h][:, :n_rows])
        v0, v1 = split2(vcat[h])
        dbase[h] = dot(
            jnp.concatenate([g0, g0, g1], 0), jnp.concatenate([v0, v1, v0], 0), TN
        )

    for p in range(parts):
        loads[p].wait()

        for i in range(rows_per):
            r = p * rows_per + i
            w = jnp.concatenate([w_t[...], gpair[r]], 0)
            res = dot(w, pair[r], NT)
            fb0[r * STRIDE : r * STRIDE + 2 * PAD, :] = res[:, :128]
            fb1[r * STRIDE : r * STRIDE + 2 * PAD, :] = res[:, 128:]

    limit = rc[0] - cl * n_cols
    valid = lane_of((n_rows, n_cols)) < limit
    lane = lane_of((n_rows, 128))
    packed = jnp.ones((n_rows, 128), F32)
    picked = lambda ref0, ref1, h: jnp.concatenate(
        [ref0[pl.ds(h, n_rows, stride=STRIDE), :], ref1[pl.ds(h, n_rows, stride=STRIDE), :]], 1
    )
    for h in range(heads):
        logit = lbase[h] + scale * picked(fb0, fb1, h)
        logit = jnp.where(valid, logit, F32(-1000000000.0))
        peak = jnp.max(logit, axis=1, keepdims=True)
        e = jnp.exp(logit - peak)
        d = dbase[h] + picked(fb0, fb1, PAD + h)
        lbase[h] = e
        dbase[h] = d
        packed = jnp.where(lane == h, peak, packed)
        packed = jnp.where(lane == PAD + h, jnp.sum(e, axis=1, keepdims=True), packed)
        packed = jnp.where(lane == 2 * PAD + h, jnp.sum(e * d, axis=1, keepdims=True), packed)
    half = n_rows // 2
    own = jnp.where(lane[:half] < 64, packed[:half], pltpu.roll(packed[half:], 64, 1))
    stat[...] = own

    pl.semaphore_wait(barrier, len(everyone))
    sends = []
    sends.append(push(stat, stat_z, s_send.at[0], s_recv.at[0], *h_peer))

    rd0[...] = jnp.zeros_like(rd0)
    rd1[...] = jnp.zeros_like(rd1)
    qb[...] = jnp.zeros_like(qb)
    gb[...] = jnp.zeros_like(gb)
    for h in range(heads):
        g, k = h // 4, h % 4
        x = qcat[h]
        if k % 2:
            x = pltpu.roll(x, 64, 1)
        c0 = 128 * (k // 2)
        hi, lo = split2(x)
        qb[g, 32 * k : 32 * k + 32, c0 : c0 + 128] = hi
        qb[g, 128 + 32 * k : 160 + 32 * k, c0 : c0 + 128] = lo
        g, k = h // 3, h % 3
        x = gcat[h]
        if k % 2:
            x = pltpu.roll(x, 64, 1)
        c0 = 128 * (k // 2)
        hi, lo = split2(x)
        gb[g, 48 * k : 48 * k + 48, c0 : c0 + 128] = hi
        gb[g, 144 + 48 * k : 192 + 48 * k, c0 : c0 + 128] = lo

    def landed(dst, send, recv, peer):
        pltpu.make_async_remote_copy(
            src_ref=dst, dst_ref=dst, send_sem=send, recv_sem=recv,
            device_id={"row": peer[0], "col": peer[1]}, device_id_type=MESH,
        ).wait_recv()

    landed(stat_z, s_send.at[0], s_recv.at[0], h_peer)
    pairwise = merge_stats([stat[...], stat_z[...]])
    stat_m[...] = pairwise
    for k in range(1, XN):
        sends.append(
            push(stat_m, stat_x.at[k - 1], s_send.at[k], s_recv.at[k], *x_peer(k))
        )
    for k in range(1, XN):
        landed(stat_x.at[k - 1], s_send.at[k], s_recv.at[k], x_peer(k))
    total = merge_stats([stat_m[...]] + [stat_x[k] for k in range(XN - 1)])
    mass = pltpu.roll(total, 128 - PAD, 1)
    factor = jnp.exp(stat[...] - total) / mass
    delta = pltpu.roll(total, 128 - 2 * PAD, 1) / mass
    factor = jnp.concatenate([factor, pltpu.roll(factor, 64, 1)], 0)
    delta = jnp.concatenate([delta, pltpu.roll(delta, 64, 1)], 0)

    def make_head(h):
        att = lbase[h] * factor[:, h : h + 1]
        dl = att * (dbase[h] - delta[:, h : h + 1])
        rows = pl.ds(h * n_rows, n_rows)
        a_hi[rows], a_lo[rows] = split2(att)
        d_hi[rows], d_lo[rows] = split2(dl)
        rd0[pl.ds(h, n_rows, stride=STRIDE), :] = dl[:, :128]
        rd1[pl.ds(h, n_rows, stride=STRIDE), :] = dl[:, 128:]
        rd0[pl.ds(PAD + h, n_rows, stride=STRIDE), :] = att[:, :128]
        rd1[pl.ds(PAD + h, n_rows, stride=STRIDE), :] = att[:, 128:]

    def key_group(g, left, hi, lo, first, count, width):
        depth = count * n_rows
        rows = pl.ds(first * n_rows, depth)
        lanes = count * width
        left = left[:, :depth]
        res = dot(left, hi[rows], NN)
        res = res[:lanes] + res[lanes:] + dot(left[:lanes], lo[rows], NN)
        if lanes > 128:
            res = jnp.concatenate([res[width * k : width * k + 40] for k in range(count)], 0)
            res = jnp.concatenate([res, jnp.zeros((8, n_cols), F32)], 0)
        flat = res.T.reshape(ZL * YN, CORES, 8, 128)
        for c in range(CORES):
            ks[g, c] = flat[:, c]
        sends.append(
            push(ks.at[g, 1 - core], ks_rx.at[g], k_send.at[g], k_recv.at[g], *sibling)
        )

    def y_stage(g):
        landed(ks_rx.at[g], k_send.at[g], k_recv.at[g], sibling)
        both = (ks[g, core] + ks_rx[g]).reshape(ZL, YN, 8, 128)
        for y in range(YN):
            sy[y, g] = both[:, y]
        for k in range(1, YN):
            sends.append(
                push(
                    sy.at[lax.rem(yy + k, YN), g], sy_rx.at[k - 1, g],
                    y_send.at[k - 1, g], y_recv.at[k - 1, g], *y_peer(k)
                )
            )

    for h in range(4):
        make_head(h)
    key_group(0, qb[0], d_hi, d_lo, 0, 4, 32)
    key_group(3, gb[0], a_hi, a_lo, 0, 3, 48)
    for h in range(4, 8):
        make_head(h)
    key_group(1, qb[1], d_hi, d_lo, 4, 4, 32)
    key_group(4, gb[1], a_hi, a_lo, 3, 3, 48)
    y_stage(0)
    y_stage(3)
    for h in range(8, 12):
        make_head(h)
    key_group(2, qb[2], d_hi, d_lo, 8, 4, 32)
    key_group(5, gb[2], a_hi, a_lo, 6, 3, 48)
    key_group(6, gb[3], a_hi, a_lo, 9, 3, 48)
    y_stage(1)
    y_stage(4)

    def query_group(source, first, skip):
        hi_cat, lo_cat, left_hi, left_lo = [], [], [], []
        for k in range(4):
            h = first + k
            block = source[h]
            if skip:
                block = jnp.concatenate([block[PAD:40], jnp.zeros((8, n_cols), F32)], 0)
            hi, lo = split2(block)
            zero = lambda n: [jnp.zeros((n, n_cols), BF16)] if n else []
            hi_cat.append(jnp.concatenate(zero(32 * k) + [hi] + zero(96 - 32 * k), 0))
            lo_cat.append(jnp.concatenate(zero(32 * k) + [lo] + zero(96 - 32 * k), 0))
            rows = pl.ds(h * n_rows, n_rows)
            left_hi.append((a_hi if skip else d_hi)[rows])
            left_lo.append((a_lo if skip else d_lo)[rows])
        hi_cat = jnp.concatenate(hi_cat, 1)
        lo_cat = jnp.concatenate(lo_cat, 1)
        left_hi = jnp.concatenate(left_hi, 1)
        left_lo = jnp.concatenate(left_lo, 1)
        res = dot(jnp.concatenate([left_hi, left_lo], 0), hi_cat, NT)
        return res[:n_rows] + res[n_rows:] + dot(left_hi, lo_cat, NT)

    distance = []
    for g in range(6):
        res = query_group(kcat if g < 3 else vcat, 4 * (g % 3), g >= 3)
        if g < 3:
            distance.append(jnp.sum(res * wq[g], axis=0, keepdims=True))
        flat = res.reshape(XN, ZH, 8, 128)
        for x in range(XN):
            for z in range(ZH):
                qs[x, z, g] = flat[x, z]
    for k in range(1, XN):
        sends.append(
            push(
                qs.at[lax.rem(xx + k, XN)], qs_rx.at[k - 1],
                q_send.at[k - 1], q_recv.at[k - 1], *x_peer(k)
            )
        )
    y_stage(2)
    y_stage(5)
    y_stage(6)

    row_block = lambda r: jnp.concatenate(
        [rd0[r * STRIDE : r * STRIDE + 2 * PAD, :], rd1[r * STRIDE : r * STRIDE + 2 * PAD, :]], 1
    ).astype(BF16)
    acc = jnp.zeros((PAD, 128), F32)
    for r in range(n_rows):
        acc = acc + dot(row_block(r)[:PAD], pair[r], NN)
    acc = scale * acc
    sub = lax.broadcasted_iota(jnp.int32, (PAD, 128), 0)
    for g in range(3):
        acc = jnp.where(sub == heads + g, distance[g], acc)
    ar_s[0] = acc
    sends.append(push(ar_s.at[0], ar_c, a_send.at[0], a_recv.at[0], *sibling))

    w_hi, w_lo = split2(scaled[...])

    def pair_rows(first, count):
        for r in range(first, first + count):
            a = row_block(r)
            lhs = jnp.concatenate([a, a[:PAD]], 0)
            rhs = jnp.concatenate([w_hi, gpair[r], w_lo], 0)
            pg_out[r] = dot(lhs, rhs, TN).astype(BF16)

    quarter = n_rows // 4
    pair_rows(0, quarter)

    landed(ar_c, a_send.at[0], a_recv.at[0], sibling)
    ar_s[1] = ar_s[0] + ar_c[...]
    ar_y[yy] = ar_s[1]
    for k in range(1, YN):
        sends.append(push(ar_s.at[1], ar_y.at[yy], a_send.at[k], a_recv.at[k], *y_peer(k)))

    pair_rows(quarter, quarter)

    for k in range(1, XN):
        landed(qs_rx.at[k - 1], q_send.at[k - 1], q_recv.at[k - 1], x_peer(k))
    qz[...] = qs[xx] + qs_rx[0] + qs_rx[1] + qs_rx[2]
    sends.append(push(qz.at[1 - zh], qz_rx, q_send.at[3], q_recv.at[3], *h_peer))

    for k in range(1, YN):
        landed(ar_y.at[lax.rem(yy + YN - k, YN)], a_send.at[k], a_recv.at[k], y_peer(k))
    ar_s[2] = ar_y[0] + ar_y[1] + ar_y[2] + ar_y[3]
    ar_x[xx] = ar_s[2]
    for k in range(1, XN):
        sends.append(
            push(ar_s.at[2], ar_x.at[xx], a_send.at[3 + k], a_recv.at[3 + k], *x_peer(k))
        )

    for g in (0, 3, 1, 4, 2, 5, 6):
        for k in range(1, YN):
            landed(sy_rx.at[k - 1, g], y_send.at[k - 1, g], y_recv.at[k - 1, g], y_peer(k))
        mine = sy[yy, g] + sy_rx[0, g] + sy_rx[1, g] + sy_rx[2, g]
        for z in range(ZL):
            sz[z, g] = mine[z]
    for k in range(1, ZL):
        sends.append(
            push(
                sz.at[lax.rem(zl + k, ZL)], sz_rx.at[k - 1],
                z_send.at[k - 1], z_recv.at[k - 1], *z_peer(k)
            )
        )
    pair_rows(2 * quarter, quarter)

    for k in range(1, XN):
        landed(ar_x.at[lax.rem(xx + XN - k, XN)], a_send.at[3 + k], a_recv.at[3 + k], x_peer(k))
    ar_s[3] = ar_x[0] + ar_x[1] + ar_x[2] + ar_x[3]
    ar_z[z8] = ar_s[3]
    for k in range(1, ZL * ZH):
        sends.append(
            push(ar_s.at[3], ar_z.at[z8], a_send.at[6 + k], a_recv.at[6 + k], *ring_peer(k))
        )

    pair_rows(3 * quarter, quarter)

    for k in range(1, ZL):
        landed(sz_rx.at[k - 1], z_send.at[k - 1], z_recv.at[k - 1], z_peer(k))
    kf_out[...] = sz[zl] + sz_rx[0] + sz_rx[1] + sz_rx[2]
    landed(qz_rx, q_send.at[3], q_recv.at[3], h_peer)
    qf_out[...] = qz[zh] + qz_rx[...]
    for k in range(1, ZL * ZH):
        landed(
            ar_z.at[lax.rem(z8 + ZL * ZH - k, ZL * ZH)], a_send.at[6 + k], a_recv.at[6 + k],
            ring_peer(k),
        )
    grand = ar_z[0]
    for k in range(1, ZL * ZH):
        grand = grand + ar_z[k]
    wr_out[...] = grand
    for copy in sends:
        copy.wait_send()


def turn(rotation, local):
    return jnp.sum(rotation[:, :, None, :] * local[None], axis=1)


def turn_back(rotation, vector):
    return jnp.sum(rotation[:, :, None, :] * vector[:, None], axis=0)


def frame_terms(grad_global, local):
    rotation_part = jnp.sum(grad_global[:, None] * local[None], axis=2)
    return jnp.concatenate([rotation_part, jnp.sum(grad_global, axis=1)[:, None, :]], axis=1)


def by_head(x, heads):
    points = x.shape[1] // heads
    return x.reshape(3, heads, points, -1).transpose(1, 0, 2, 3).reshape(heads, 3 * points, -1)


def by_axis(x):
    heads, rows, m = x.shape
    return x.reshape(heads, 3, rows // 3, m).transpose(1, 0, 2, 3).reshape(3, heads * rows // 3, m)


def pad_to(x, rows, lanes):
    return jnp.pad(x, ((0, 0), (0, rows - x.shape[1]), (0, lanes - x.shape[2])))


def per_device(
    pair_rep, bias_weight, head_weight, queries, key_vectors, values, query_points, key_points,
    value_points, rotations, translations, residue_count, grad_output, grad_points, grad_pair,
):
    channels, heads = bias_weight.shape
    width = queries.shape[0] // heads
    qpoints = query_points.shape[1] // heads
    vpoints = value_points.shape[1] // heads
    n_rows = queries.shape[1]
    n_cols = key_vectors.shape[1]
    logit_scale = math.sqrt(1.0 / 3.0)
    point_scale = math.sqrt(2.0 / (9.0 * qpoints))
    inner_scale = 1.0 / math.sqrt(width)
    coef = 0.5 * logit_scale * point_scale * jax.nn.softplus(head_weight)
    row_start = lax.axis_index("row") * n_rows
    col_start = lax.axis_index("col") * n_cols
    rot_rows = lax.dynamic_slice_in_dim(rotations, row_start, n_rows, 2)
    shift_rows = lax.dynamic_slice_in_dim(translations, row_start, n_rows, 1)
    rot_cols = lax.dynamic_slice_in_dim(rotations, col_start, n_cols, 2)
    shift_cols = lax.dynamic_slice_in_dim(translations, col_start, n_cols, 1)
    qg = by_head(turn(rot_rows, query_points) + shift_rows[:, None, :], heads)
    kg = by_head(turn(rot_cols, key_points) + shift_cols[:, None, :], heads)
    vg = by_head(turn(rot_cols, value_points) + shift_cols[:, None, :], heads)
    grad_flat = turn(rot_rows, grad_points)
    gg = by_head(grad_flat, heads)
    q = queries.reshape(heads, width, n_rows)
    k = key_vectors.reshape(heads, width, n_cols)
    qsize = width + 3 * qpoints
    nq = 32
    nv = width + 3 * vpoints
    nvp = 48
    c3 = coef[:, None, None]
    q_square = jnp.sum(qg * qg, axis=1, keepdims=True)
    k_square = jnp.sum(kg * kg, axis=1, keepdims=True)
    qcat = pad_to(
        jnp.concatenate(
            [
                logit_scale * inner_scale * q,
                2.0 * c3 * qg,
                jnp.broadcast_to(-c3, (heads, 1, n_rows)),
                -c3 * q_square,
            ],
            axis=1,
        ),
        nq, 128,
    )
    kcat = pad_to(
        jnp.concatenate([k, kg, k_square, jnp.ones((heads, 1, n_cols), F32)], axis=1), nq, n_cols
    )
    gcat = pad_to(
        jnp.concatenate([grad_output.reshape(heads, width, n_rows), gg], axis=1), nvp, 128
    )
    vcat = pad_to(
        jnp.concatenate([values.reshape(heads, width, n_cols), vg], axis=1), nvp, n_cols
    )
    wq = pad_to(
        jnp.concatenate(
            [
                jnp.zeros((heads, width, n_rows), F32), -2.0 * qg,
                jnp.ones((heads, 1, n_rows), F32), q_square,
            ],
            axis=1,
        ),
        nq, n_rows,
    )
    wq = wq.reshape(heads // 4, 4 * nq, n_rows).transpose(0, 2, 1)
    w_t = jnp.pad(bias_weight.T, ((0, PAD - heads), (0, 0)))
    scaled = logit_scale * w_t.astype(F32)
    gpair = jnp.pad(grad_pair, ((0, 0), (0, PAD - heads), (0, 0)))

    vm = pl.BlockSpec(memory_space=pltpu.VMEM)
    big = (heads, n_rows, n_cols)
    flat = (heads * n_rows, n_cols)
    dma = pltpu.SemaphoreType.DMA
    pair_grad, kf, qf, wr = pl.pallas_call(
        functools.partial(mega_kernel, heads, n_rows, n_cols, logit_scale),
        in_specs=[
            pl.BlockSpec(memory_space=pltpu.SMEM),
            pl.BlockSpec(memory_space=pl.ANY),
            *[vm] * 8,
        ],
        out_specs=[vm] * 4,
        out_shape=[
            jax.ShapeDtypeStruct(pair_rep.shape, BF16),
            jax.ShapeDtypeStruct((7, 8, 128), F32),
            jax.ShapeDtypeStruct((6, 8, 128), F32),
            jax.ShapeDtypeStruct((PAD, 128), F32),
        ],
        scratch_shapes=[
            pltpu.VMEM(pair_rep.shape, BF16),
            pltpu.VMEM(big, F32),
            pltpu.VMEM(big, F32),
            *[pltpu.VMEM((n_rows * STRIDE, 128), F32)] * 4,
            *[pltpu.VMEM(flat, BF16)] * 4,
            pltpu.VMEM((3, 256, 256), BF16),
            pltpu.VMEM((4, 288, 256), BF16),
            pltpu.VMEM((32, 128), F32),
            pltpu.VMEM((32, 128), F32),
            pltpu.VMEM((32, 128), F32),
            pltpu.VMEM((3, 32, 128), F32),
            pltpu.VMEM((7, CORES, ZL * YN, 8, 128), F32),
            pltpu.VMEM((7, ZL * YN, 8, 128), F32),
            pltpu.VMEM((YN, 7, ZL, 8, 128), F32),
            pltpu.VMEM((YN - 1, 7, ZL, 8, 128), F32),
            pltpu.VMEM((ZL, 7, 8, 128), F32),
            pltpu.VMEM((ZL - 1, 7, 8, 128), F32),
            pltpu.VMEM((XN, ZH, 6, 8, 128), F32),
            pltpu.VMEM((XN - 1, ZH, 6, 8, 128), F32),
            pltpu.VMEM((ZH, 6, 8, 128), F32),
            pltpu.VMEM((6, 8, 128), F32),
            pltpu.VMEM((PAD, 128), F32),
            pltpu.VMEM((YN, PAD, 128), F32),
            pltpu.VMEM((XN, PAD, 128), F32),
            pltpu.VMEM((ZL * ZH, PAD, 128), F32),
            pltpu.VMEM((4, PAD, 128), F32),
            dma((4,)),
            dma((4,)), dma((4,)),
            dma((7,)), dma((7,)),
            dma((3, 7)), dma((3, 7)),
            dma((3,)), dma((3,)),
            dma((4,)), dma((4,)),
            dma((14,)), dma((14,)),
        ],
        compiler_params=pltpu.CompilerParams(
            collective_id=0, has_side_effects=True, vmem_limit_bytes=VMEM_LIMIT
        ),
        name="mega",
    )(residue_count, pair_rep, w_t, scaled, gpair, qcat, kcat, gcat, vcat, wq)

    weight_total = wr[:heads].T
    distance_total = jnp.sum(wr[heads : heads + 3].reshape(heads, nq), axis=1)
    head_weight_grad = (
        distance_total * (-0.5 * logit_scale * point_scale) * jax.nn.sigmoid(head_weight)
    )
    share = 8
    ksum = kf[:3].reshape(3, share, 4, nq).transpose(0, 2, 3, 1).reshape(heads, nq, share)
    vsum = (
        kf[3:, :, :120].reshape(4, share, 3, nv).transpose(0, 2, 3, 1).reshape(heads, nv, share)
    )
    qsum = qf[:3].reshape(3, share, 4, nq).transpose(0, 2, 3, 1).reshape(heads, nq, share)
    osum = qf[3:].reshape(3, share, 4, nq).transpose(0, 2, 3, 1).reshape(heads, nq, share)

    start = lax.axis_index("col") * share
    own_rows = lambda x: lax.dynamic_slice_in_dim(x, start, share, x.ndim - 1)
    rot_own = own_rows(rot_rows)
    shift_own = own_rows(shift_rows)
    query_grad = (logit_scale * inner_scale * qsum[:, :width]).reshape(heads * width, share)
    dqg = by_axis(
        -2.0 * c3 * (own_rows(qg) * qsum[:, qsize + 1][:, None] - qsum[:, width:qsize])
    )
    point_out = by_axis(osum[:, : nv - width])
    query_point_grad = turn_back(rot_own, dqg)
    cotan_own = own_rows(grad_points)
    out_part = jnp.sum((point_out - shift_own[:, None, :])[:, None] * cotan_own[None], axis=2)
    out_part = jnp.concatenate(
        [out_part, -jnp.sum(own_rows(grad_flat), axis=1)[:, None, :]], axis=1
    )
    query_frame_grad = frame_terms(dqg, own_rows(query_points)) + out_part

    kstart = lax.axis_index("row") * share
    own_cols = lambda x: lax.dynamic_slice_in_dim(x, kstart, share, x.ndim - 1)
    rot_keys = own_cols(rot_cols)
    key_grad = ksum[:, :width].reshape(heads * width, share)
    value_grad = vsum[:, :width].reshape(heads * width, share)
    dkg = by_axis(ksum[:, width:qsize] + 2.0 * own_cols(kg) * ksum[:, qsize][:, None])
    dvg = by_axis(vsum[:, width:])
    key_point_grad = turn_back(rot_keys, dkg)
    value_point_grad = turn_back(rot_keys, dvg)
    key_frame_grad = frame_terms(dkg, own_cols(key_points)) + frame_terms(
        dvg, own_cols(value_points)
    )
    return (
        pair_grad, query_grad, query_point_grad, query_frame_grad, key_grad, value_grad,
        key_point_grad, value_point_grad, key_frame_grad, weight_total, head_weight_grad,
    )


def solution(mesh):
    return jax.shard_map(
        per_device,
        mesh=mesh,
        in_specs=(
            P("row", "col", None),
            P(),
            P(),
            P(None, "row"),
            P(None, "col"),
            P(None, "col"),
            P(None, None, "row"),
            P(None, None, "col"),
            P(None, None, "col"),
            P(),
            P(),
            P(),
            P(None, "row"),
            P(None, None, "row"),
            P("row", None, None),
        ),
        out_specs=(
            P("row", "col", None),
            P(None, ("row", "col")),
            P(None, None, ("row", "col")),
            P(None, None, ("row", "col")),
            P(None, ("col", "row")),
            P(None, ("col", "row")),
            P(None, None, ("col", "row")),
            P(None, None, ("col", "row")),
            P(None, None, ("col", "row")),
            P(),
            P(),
        ),
        check_vma=False,
    )
```

```python
import functools
import math

import jax
import jax.numpy as jnp
from jax import lax
from jax.experimental import pallas as pl
from jax.experimental.pallas import tpu as pltpu
from jax.sharding import PartitionSpec as P

F32 = jnp.float32
BF16 = jnp.bfloat16
PAD = 16
VMEM_LIMIT = 62700000
ZL, YN, CORES = 4, 4, 2
XN, ZH = 4, 2
STRIDE = 40
MESH = pl.DeviceIdType.MESH


def dot(a, b, dims):
    return lax.dot_general(a, b, (dims, ((), ())), preferred_element_type=F32)


TN = ((0,), (0,))
NT = ((1,), (1,))
NN = ((1,), (0,))


def split2(x):
    hi = x.astype(BF16)
    return hi, (x - hi.astype(F32)).astype(BF16)


def split3(x):
    hi = x.astype(BF16)
    rest = x - hi.astype(F32)
    mid = rest.astype(BF16)
    return hi, mid, (rest - mid.astype(F32)).astype(BF16)


def lane_of(shape):
    return lax.broadcasted_iota(jnp.int32, shape, 1)


def merge_stats(parts):
    top = functools.reduce(jnp.maximum, parts)
    lane = lax.rem(lane_of(top.shape), 64)
    out = None
    for part in parts:
        f = jnp.exp(part - top)
        spread = jnp.where(lane < 2 * PAD, pltpu.roll(f, PAD, 1), pltpu.roll(f, 2 * PAD, 1))
        term = part * spread
        out = term if out is None else out + term
    return jnp.where(lane < PAD, top, out)


def push(src, dst, send, recv, row, col):
    copy = pltpu.make_async_remote_copy(
        src_ref=src, dst_ref=dst, send_sem=send, recv_sem=recv,
        device_id={"row": row, "col": col}, device_id_type=MESH,
    )
    copy.start()
    return copy


def group_mask(width, point, spread):
    row = lax.broadcasted_iota(jnp.int32, (128, 256), 0)
    lane = lane_of((128, 256))
    if width:
        body = (row - width * PAD) % (width * point)
        head = jnp.where(row < width * PAD, row // PAD, body // point)
    else:
        head = (row % 32) // point
    return head, lane // spread


def spread_heads(left, mask):
    left = jnp.concatenate([left, jnp.zeros_like(left)], 1)
    left = left + pltpu.roll(left, 64, 1)
    return jnp.where(mask, jnp.concatenate([left, left], 1), 0.0)


def soft(head_weight):
    return jnp.maximum(head_weight, 0.0) + jnp.log(1.0 + jnp.exp(-jnp.abs(head_weight)))


def mega_kernel(
    heads, n_rows, n_cols, scale, inner, coef_scale,
    rc, pair_hbm, *refs,
):
    sources, refs = refs[:13], refs[13:]
    pg_out, kf_out, qf_out, wr_out = refs[:4]
    staged, refs = refs[4:17], refs[17:]
    bw, hw, gp_t, qt, kt, vt, qp, kp, vp, rot, shift, got, gpt = staged
    (
    pair, lbase, dbase, fb0, fb1, rd0, rd1, a_hi, a_lo, d_hi, d_lo,
    wgf, wgb, qc, kc, wq, stat, stat_z, stat_m, stat_x,
    ks, ks_rx, sy, sy_rx, sz, sz_rx, qs, qs_rx, qz, qz_rx,
    ar_c, ar_y, ar_x, ar_z, ar_s,
    pair_sem, in_sem, s_send, s_recv, k_send, k_recv, y_send, y_recv, z_send, z_recv,
    q_send, q_recv, a_send, a_recv,
    ) = refs
    rw = lax.axis_index("row")
    cl = lax.axis_index("col")
    core = lax.rem(rw, CORES)
    yy = lax.rem(rw // CORES, YN)
    zl = rw // (CORES * YN)
    zh = lax.rem(cl, ZH)
    xx = cl // ZH
    row_of = lambda z, y, c: (z * YN + y) * CORES + c
    sibling = (row_of(zl, yy, 1 - core), cl)
    y_peer = lambda k: (row_of(zl, lax.rem(yy + k, YN), core), cl)
    z_peer = lambda k: (row_of(lax.rem(zl + k, ZL), yy, core), cl)
    x_peer = lambda k: (rw, lax.rem(xx + k, XN) * ZH + zh)
    h_peer = (rw, xx * ZH + 1 - zh)
    z8 = zh * ZL + zl

    def ring_peer(k):
        idx = lax.rem(z8 + k, ZL * ZH)
        return (row_of(lax.rem(idx, ZL), yy, core), xx * ZH + idx // ZL)

    everyone = [sibling]
    everyone += [y_peer(k) for k in range(1, YN)]
    everyone += [x_peer(k) for k in range(1, XN)]
    everyone += [ring_peer(k) for k in range(1, ZL * ZH)]
    barrier = pltpu.get_barrier_semaphore()
    for peer in everyone:
        pl.semaphore_signal(
            barrier, inc=1, device_id={"row": peer[0], "col": peer[1]}, device_id_type=MESH
        )

    incoming = []
    for n, (source, target) in enumerate(zip(sources, staged)):
        incoming.append(pltpu.make_async_copy(source, target, in_sem.at[n]))
        incoming[-1].start()
    parts = 4
    rows_per = n_rows // parts
    loads = []
    for p in range(parts):
        piece = pl.ds(p * rows_per, rows_per)
        load = pltpu.make_async_copy(pair_hbm.at[piece], pair.at[piece], pair_sem.at[p])
        load.start()
        loads.append(load)

    wgf[...] = jnp.zeros_like(wgf)
    for copy in incoming:
        copy.wait()
    w_all = bw[...].astype(F32)
    w_t = jnp.concatenate([w_all, jnp.zeros((PAD - heads, 128), F32)], 0)
    for h in range(heads):
        wgf[pl.ds(PAD + h, n_rows, stride=STRIDE), :] = gp_t[h].astype(F32)
    w_bf = w_t.astype(BF16)
    for r in range(n_rows):
        wgb[r, :PAD, :] = w_bf
        wgb[r, PAD:, :] = wgf[r * STRIDE + PAD : r * STRIDE + 2 * PAD, :].astype(BF16)

    row_block = pl.multiple_of((rw // 2) * 128, 128)
    col_block = pl.multiple_of(cl * n_cols, 128)

    def row_vec(ref, *index):
        v = ref[index + (pl.ds(row_block, 128),)]
        return jnp.where(core == 1, pltpu.roll(v, 64, 1), v)[:, :n_rows]

    rot_q = [[row_vec(rot, x, pl.ds(y, 1)) for y in range(3)] for x in range(3)]
    rot_k = [
        [rot[x, pl.ds(y, 1), pl.ds(col_block, n_cols)] for y in range(3)] for x in range(3)
    ]
    apply = lambda m, p: [m[x][0] * p[0] + m[x][1] * p[1] + m[x][2] * p[2] for x in range(3)]
    add_shift = lambda g, t: [g[x] + t[x] for x in range(3)]
    qg = add_shift(
        apply(rot_q, [qp[y] for y in range(3)]),
        [row_vec(shift, pl.ds(x, 1)) for x in range(3)],
    )
    shift_k = [shift[pl.ds(x, 1), pl.ds(col_block, n_cols)] for x in range(3)]
    kg = add_shift(apply(rot_k, [kp[y] for y in range(3)]), shift_k)
    vg = add_shift(apply(rot_k, [vp[y] for y in range(3)]), shift_k)
    gg = apply(rot_q, [gpt[y].T for y in range(3)])
    tall = lambda ref: jnp.concatenate([ref[:, :128].T, ref[:, 128:].T], 0)
    q_all = tall(qt)
    g_all = tall(got)
    q_sq = qg[0] * qg[0] + qg[1] * qg[1] + qg[2] * qg[2]
    k_sq = kg[0] * kg[0] + kg[1] * kg[1] + kg[2] * kg[2]
    size = q_sq.shape[0]
    back = lambda x, n: pltpu.roll(x, size - n, 0)
    q_sq = q_sq + back(q_sq, 1) + back(q_sq, 2) + back(q_sq, 3)
    k_sq = k_sq + pltpu.roll(k_sq, 1, 0) + pltpu.roll(k_sq, 2, 0) + pltpu.roll(k_sq, 3, 0)
    coef = coef_scale * soft(hw[...])

    for h in range(heads):
        c = coef[:, h : h + 1]
        qc[h, :PAD, :] = (scale * inner) * q_all[PAD * h : PAD * h + PAD]
        kc[h, :PAD, :] = kt[PAD * h : PAD * h + PAD, :]
        for x in range(3):
            qc[h, PAD + 4 * x : PAD + 4 * x + 4, :] = (2.0 * c) * qg[x][4 * h : 4 * h + 4]
            kc[h, PAD + 4 * x : PAD + 4 * x + 4, :] = kg[x][4 * h : 4 * h + 4]
        qc[h, 28:29, :] = jnp.broadcast_to(-c, (1, n_rows))
        qc[h, 29:30, :] = -c * q_sq[4 * h : 4 * h + 1]
        qc[h, 30:32, :] = jnp.zeros((2, n_rows), F32)
        kc[h, 28:29, :] = k_sq[4 * h + 3 : 4 * h + 4]
        kc[h, 29:30, :] = jnp.ones((1, n_cols), F32)
        kc[h, 30:32, :] = jnp.zeros((2, n_cols), F32)

    def point_rows(head, points, h):
        body = [points[x][8 * h : 8 * h + 8] for x in range(3)]
        return jnp.concatenate([head] + body + [jnp.zeros_like(body[0])], 0)

    for h in range(heads):
        q0, q1, q2 = split3(qc[h])
        k0, k1, k2 = split3(kc[h])
        lbase[h] = dot(
            jnp.concatenate([q0, q0, q1, q0, q2, q1], 0),
            jnp.concatenate([k0, k1, k0, k2, k0, k1], 0),
            TN,
        )
        g0, g1 = split2(point_rows(g_all[PAD * h : PAD * h + PAD], gg, h))
        v0, v1 = split2(point_rows(vt[PAD * h : PAD * h + PAD, :], vg, h))
        dbase[h] = dot(
            jnp.concatenate([g0, g0, g1], 0), jnp.concatenate([v0, v1, v0], 0), TN
        )

    for p in range(parts):
        loads[p].wait()

        for i in range(rows_per):
            r = p * rows_per + i
            res = dot(wgb[r], pair[r], NT)
            fb0[r * STRIDE : r * STRIDE + 2 * PAD, :] = res[:, :128]
            fb1[r * STRIDE : r * STRIDE + 2 * PAD, :] = res[:, 128:]

    limit = rc[0] - cl * n_cols
    valid = lane_of((n_rows, n_cols)) < limit
    lane = lane_of((n_rows, 128))
    packed = jnp.ones((n_rows, 128), F32)
    picked = lambda ref0, ref1, h: jnp.concatenate(
        [ref0[pl.ds(h, n_rows, stride=STRIDE), :], ref1[pl.ds(h, n_rows, stride=STRIDE), :]], 1
    )
    for h in range(heads):
        logit = lbase[h] + scale * picked(fb0, fb1, h)
        logit = jnp.where(valid, logit, F32(-1000000000.0))
        peak = jnp.max(logit, axis=1, keepdims=True)
        e = jnp.exp(logit - peak)
        d = dbase[h] + picked(fb0, fb1, PAD + h)
        lbase[h] = e
        dbase[h] = d
        packed = jnp.where(lane == h, peak, packed)
        packed = jnp.where(lane == PAD + h, jnp.sum(e, axis=1, keepdims=True), packed)
        packed = jnp.where(lane == 2 * PAD + h, jnp.sum(e * d, axis=1, keepdims=True), packed)
    half = n_rows // 2
    own = jnp.where(lane[:half] < 64, packed[:half], pltpu.roll(packed[half:], 64, 1))
    stat[...] = own

    pl.semaphore_wait(barrier, len(everyone))
    sends = []
    sends.append(push(stat, stat_z, s_send.at[0], s_recv.at[0], *h_peer))

    rd0[...] = jnp.zeros_like(rd0)
    rd1[...] = jnp.zeros_like(rd1)
    key_head, lane64 = group_mask(4, 4, 64)
    key_mask = key_head == lane64
    val_head, _ = group_mask(3, 8, 64)
    val_mask = val_head == lane64
    sub16 = lax.broadcasted_iota(jnp.int32, (PAD, n_rows), 0) % 4
    sub16k = lax.broadcasted_iota(jnp.int32, (PAD, n_cols), 0) % 4
    qb, gb, kb, vb = [], [], [], []
    for g in range(3):
        pts = slice(PAD * g, PAD * g + PAD)
        base = jnp.concatenate(
            [q_all[64 * g : 64 * g + 64]] + [qg[x][pts] for x in range(3)]
            + [jnp.ones((PAD, n_rows), F32)], 0
        )
        qb.append(split2(spread_heads(base, key_mask)))
        weights = jnp.concatenate(
            [jnp.zeros((64, n_rows), F32)] + [-2.0 * qg[x][pts] for x in range(3)]
            + [jnp.where(sub16 == 0, q_sq[pts], jnp.where(sub16 == 3, 1.0, 0.0))], 0
        )
        wq[g] = weights.T
        base = jnp.concatenate(
            [kt[64 * g : 64 * g + 64, :]] + [kg[x][pts] for x in range(3)]
            + [jnp.where(sub16k == 3, k_sq[pts], jnp.where(sub16k == 0, 1.0, 0.0))], 0
        )
        kb.append(split2(base))
        oct_rows = slice(32 * g, 32 * g + 32)
        base = jnp.concatenate(
            [vg[x][oct_rows] for x in range(3)] + [jnp.zeros((32, n_cols), F32)], 0
        )
        vb.append(split2(base))
    for g in range(4):
        pts = slice(24 * g, 24 * g + 24)
        base = jnp.concatenate(
            [g_all[48 * g : 48 * g + 48]] + [gg[x][pts] for x in range(3)]
            + [jnp.zeros((8, n_rows), F32)], 0
        )
        gb.append(split2(spread_heads(base, val_mask)))
    query_masks = [key_head == k for k in range(4)]
    point_head, _ = group_mask(0, 8, 64)
    point_masks = [point_head == k for k in range(4)]

    def landed(dst, send, recv, peer):
        pltpu.make_async_remote_copy(
            src_ref=dst, dst_ref=dst, send_sem=send, recv_sem=recv,
            device_id={"row": peer[0], "col": peer[1]}, device_id_type=MESH,
        ).wait_recv()

    landed(stat_z, s_send.at[0], s_recv.at[0], h_peer)
    pairwise = merge_stats([stat[...], stat_z[...]])
    stat_m[...] = pairwise
    for k in range(1, XN):
        sends.append(
            push(stat_m, stat_x.at[k - 1], s_send.at[k], s_recv.at[k], *x_peer(k))
        )
    for k in range(1, XN):
        landed(stat_x.at[k - 1], s_send.at[k], s_recv.at[k], x_peer(k))
    total = merge_stats([stat_m[...]] + [stat_x[k] for k in range(XN - 1)])
    mass = pltpu.roll(total, 128 - PAD, 1)
    factor = jnp.exp(stat[...] - total) / mass
    delta = pltpu.roll(total, 128 - 2 * PAD, 1) / mass
    factor = jnp.concatenate([factor, pltpu.roll(factor, 64, 1)], 0)
    delta = jnp.concatenate([delta, pltpu.roll(delta, 64, 1)], 0)

    def make_head(h):
        att = lbase[h] * factor[:, h : h + 1]
        dl = att * (dbase[h] - delta[:, h : h + 1])
        rows = pl.ds(h * n_rows, n_rows)
        a_hi[rows], a_lo[rows] = split2(att)
        d_hi[rows], d_lo[rows] = split2(dl)
        rd0[pl.ds(h, n_rows, stride=STRIDE), :] = dl[:, :128]
        rd1[pl.ds(h, n_rows, stride=STRIDE), :] = dl[:, 128:]
        rd0[pl.ds(PAD + h, n_rows, stride=STRIDE), :] = att[:, :128]
        rd1[pl.ds(PAD + h, n_rows, stride=STRIDE), :] = att[:, 128:]

    def key_group(g, pairs, hi, lo, first, count):
        depth = count * n_rows
        rows = pl.ds(first * n_rows, depth)
        left, small = pairs[0][:, :depth], pairs[1][:, :depth]
        res = dot(jnp.concatenate([left, small], 0), hi[rows], NN)
        res = res[:128] + res[128:] + dot(left, lo[rows], NN)
        flat = res.T.reshape(ZL * YN, CORES, 8, 128)
        for c in range(CORES):
            ks[g, c] = flat[:, c]
        sends.append(
            push(ks.at[g, 1 - core], ks_rx.at[g], k_send.at[g], k_recv.at[g], *sibling)
        )

    def y_stage(g):
        landed(ks_rx.at[g], k_send.at[g], k_recv.at[g], sibling)
        both = (ks[g, core] + ks_rx[g]).reshape(ZL, YN, 8, 128)
        for y in range(YN):
            sy[y, g] = both[:, y]
        for k in range(1, YN):
            sends.append(
                push(
                    sy.at[lax.rem(yy + k, YN), g], sy_rx.at[k - 1, g],
                    y_send.at[k - 1, g], y_recv.at[k - 1, g], *y_peer(k)
                )
            )

    for h in range(4):
        make_head(h)
    key_group(0, qb[0], d_hi, d_lo, 0, 4)
    key_group(3, gb[0], a_hi, a_lo, 0, 3)
    for h in range(4, 8):
        make_head(h)
    key_group(1, qb[1], d_hi, d_lo, 4, 4)
    key_group(4, gb[1], a_hi, a_lo, 3, 3)
    y_stage(0)
    y_stage(3)
    for h in range(8, 12):
        make_head(h)
    key_group(2, qb[2], d_hi, d_lo, 8, 4)
    key_group(5, gb[2], a_hi, a_lo, 6, 3)
    key_group(6, gb[3], a_hi, a_lo, 9, 3)
    y_stage(1)
    y_stage(4)

    def query_group(pairs, masks, hi, lo, first):
        blocks = lambda x: jnp.concatenate(
            [jnp.where(m, x, jnp.zeros_like(x)) for m in masks], 1
        )
        lefts = lambda ref: jnp.concatenate(
            [ref[pl.ds((first + k) * n_rows, n_rows)] for k in range(4)], 1
        )
        top = lefts(hi)
        res = dot(jnp.concatenate([top, lefts(lo)], 0), blocks(pairs[0]), NT)
        return res[:n_rows] + res[n_rows:] + dot(top, blocks(pairs[1]), NT)

    distance = []
    for g in range(6):
        if g < 3:
            res = query_group(kb[g], query_masks, d_hi, d_lo, 4 * g)
        else:
            res = query_group(vb[g - 3], point_masks, a_hi, a_lo, 4 * (g - 3))
        if g < 3:
            distance.append(jnp.sum(res * wq[g], axis=0, keepdims=True))
        flat = res.reshape(XN, ZH, 8, 128)
        for x in range(XN):
            for z in range(ZH):
                qs[x, z, g] = flat[x, z]
    for k in range(1, XN):
        sends.append(
            push(
                qs.at[lax.rem(xx + k, XN)], qs_rx.at[k - 1],
                q_send.at[k - 1], q_recv.at[k - 1], *x_peer(k)
            )
        )
    y_stage(2)
    y_stage(5)
    y_stage(6)

    both_rows = lambda r: jnp.concatenate(
        [rd0[r * STRIDE : r * STRIDE + 2 * PAD, :], rd1[r * STRIDE : r * STRIDE + 2 * PAD, :]], 1
    ).astype(BF16)
    acc = jnp.zeros((PAD, 128), F32)
    for r in range(n_rows):
        acc = acc + dot(both_rows(r)[:PAD], pair[r], NN)
    acc = scale * acc
    sub = lax.broadcasted_iota(jnp.int32, (PAD, 128), 0)
    lane1 = lane_of((1, 128))
    owner = jnp.where(lane1 < 112, (lane1 % PAD) // 4, (lane1 - 112) // 4)
    dist_row = jnp.zeros((1, 128), F32)
    for h in range(heads):
        part = jnp.sum(jnp.where(owner == h % 4, distance[h // 4], 0.0), axis=1, keepdims=True)
        dist_row = jnp.where(lane1 == h, part, dist_row)
    acc = jnp.where(sub == heads, dist_row, acc)
    ar_s[0] = acc
    sends.append(push(ar_s.at[0], ar_c, a_send.at[0], a_recv.at[0], *sibling))

    w_hi, w_lo = split2(scale * w_t)

    def pair_rows(first, count):
        for r in range(first, first + count):
            a = both_rows(r)
            lhs = jnp.concatenate([a, a[:PAD]], 0)
            rhs = jnp.concatenate([w_hi, wgb[r, PAD:, :], w_lo], 0)
            pg_out[r] = dot(lhs, rhs, TN).astype(BF16)

    quarter = n_rows // 4
    pair_rows(0, quarter)

    landed(ar_c, a_send.at[0], a_recv.at[0], sibling)
    ar_s[1] = ar_s[0] + ar_c[...]
    ar_y[yy] = ar_s[1]
    for k in range(1, YN):
        sends.append(push(ar_s.at[1], ar_y.at[yy], a_send.at[k], a_recv.at[k], *y_peer(k)))

    pair_rows(quarter, quarter)

    for k in range(1, XN):
        landed(qs_rx.at[k - 1], q_send.at[k - 1], q_recv.at[k - 1], x_peer(k))
    qz[...] = qs[xx] + qs_rx[0] + qs_rx[1] + qs_rx[2]
    sends.append(push(qz.at[1 - zh], qz_rx, q_send.at[3], q_recv.at[3], *h_peer))

    for k in range(1, YN):
        landed(ar_y.at[lax.rem(yy + YN - k, YN)], a_send.at[k], a_recv.at[k], y_peer(k))
    ar_s[2] = ar_y[0] + ar_y[1] + ar_y[2] + ar_y[3]
    ar_x[xx] = ar_s[2]
    for k in range(1, XN):
        sends.append(
            push(ar_s.at[2], ar_x.at[xx], a_send.at[3 + k], a_recv.at[3 + k], *x_peer(k))
        )

    for g in (0, 3, 1, 4, 2, 5, 6):
        for k in range(1, YN):
            landed(sy_rx.at[k - 1, g], y_send.at[k - 1, g], y_recv.at[k - 1, g], y_peer(k))
        mine = sy[yy, g] + sy_rx[0, g] + sy_rx[1, g] + sy_rx[2, g]
        for z in range(ZL):
            sz[z, g] = mine[z]
    for k in range(1, ZL):
        sends.append(
            push(
                sz.at[lax.rem(zl + k, ZL)], sz_rx.at[k - 1],
                z_send.at[k - 1], z_recv.at[k - 1], *z_peer(k)
            )
        )
    pair_rows(2 * quarter, quarter)

    for k in range(1, XN):
        landed(ar_x.at[lax.rem(xx + XN - k, XN)], a_send.at[3 + k], a_recv.at[3 + k], x_peer(k))
    ar_s[3] = ar_x[0] + ar_x[1] + ar_x[2] + ar_x[3]
    ar_z[z8] = ar_s[3]
    for k in range(1, ZL * ZH):
        sends.append(
            push(ar_s.at[3], ar_z.at[z8], a_send.at[6 + k], a_recv.at[6 + k], *ring_peer(k))
        )

    pair_rows(3 * quarter, quarter)

    for k in range(1, ZL):
        landed(sz_rx.at[k - 1], z_send.at[k - 1], z_recv.at[k - 1], z_peer(k))
    kf_out[...] = sz[zl] + sz_rx[0] + sz_rx[1] + sz_rx[2]
    landed(qz_rx, q_send.at[3], q_recv.at[3], h_peer)
    qf_out[...] = qz[zh] + qz_rx[...]
    for k in range(1, ZL * ZH):
        landed(
            ar_z.at[lax.rem(z8 + ZL * ZH - k, ZL * ZH)], a_send.at[6 + k], a_recv.at[6 + k],
            ring_peer(k),
        )
    grand = ar_z[0]
    for k in range(1, ZL * ZH):
        grand = grand + ar_z[k]
    wr_out[...] = grand
    for copy in sends:
        copy.wait_send()


def finish_kernel(
    heads, n_rows, scale, inner, coef_scale,
    pg, kf, qf, wr, hw_hbm, qp_hbm, kp_hbm, vp_hbm, rot_hbm, shift_hbm, gpt_hbm,
    pg_out, qgrad, qpgrad, qframe, kgrad, vgrad, kpgrad, vpgrad, kframe, weight, head_out,
    hw, qp, kp, vp, rot, shift, gpt, turned, in_sem, sem,
):
    incoming = []
    sources = (hw_hbm, qp_hbm, kp_hbm, vp_hbm, rot_hbm, shift_hbm, gpt_hbm)
    for n, (source, target) in enumerate(zip(sources, (hw, qp, kp, vp, rot, shift, gpt))):
        incoming.append(pltpu.make_async_copy(source, target, in_sem.at[n]))
        incoming[-1].start()
    copy = pltpu.make_async_copy(pg, pg_out, sem)
    copy.start()
    rw = lax.axis_index("row")
    cl = lax.axis_index("col")
    weight[...] = wr[:heads, :]
    for load in incoming:
        load.wait()
    sig = 1.0 / (1.0 + jnp.exp(-hw[...]))
    head_out[...] = wr[heads : heads + 1, :heads] * (-coef_scale) * sig
    coef = coef_scale * soft(hw[...])

    def frames(start):
        block = pl.multiple_of((start // 128) * 128, 128)
        rows = [rot[x, pl.ds(y, 1), pl.ds(block, 128)] for x in range(3) for y in range(3)]
        rows += [shift[pl.ds(x, 1), pl.ds(block, 128)] for x in range(3)]
        rows = jnp.concatenate(rows + [jnp.zeros((4, 128), F32)], 0)
        turned[:, :PAD] = rows.T
        own = turned[pl.ds(pl.multiple_of(start % 128, 8), 8), :PAD]
        entry = lambda k: own[:, k : k + 1]
        return [[entry(3 * x + y) for y in range(3)] for x in range(3)], [
            entry(9 + x) for x in range(3)
        ]

    def local(ref, lanes, offset):
        out = []
        for y in range(3):
            x = ref[y] if lanes is None else ref[y, :, lanes]
            x = x.T
            turned[: x.shape[0], : x.shape[1]] = x
            out.append(turned[pl.ds(pl.multiple_of(offset, 8), 8), : x.shape[1]])
        return out

    apply = lambda m, p: [m[x][0] * p[0] + m[x][1] * p[1] + m[x][2] * p[2] for x in range(3)]
    undo = lambda m, v: [m[0][y] * v[0] + m[1][y] * v[1] + m[2][y] * v[2] for y in range(3)]
    add_all = lambda x: jnp.sum(x, axis=1, keepdims=True)
    lane8 = lane_of((8, 128))

    def gather(parts, offset, size):
        return jnp.concatenate([p[:, offset : offset + size] for p in parts], 1)

    c48 = jnp.zeros((1, 128), F32)
    lane1 = lane_of((1, 128))
    for h in range(heads):
        c48 = jnp.where(lane1 // 4 == h, coef[:, h : h + 1], c48)
    c48 = c48[:, :48]

    def frame_out(ref, entries):
        tile = jnp.zeros((8, 128), F32)
        for k, value in enumerate(entries):
            tile = jnp.where(lane8 == k, value, tile)
        tile = tile.T
        for x in range(3):
            ref[x] = tile[4 * x : 4 * x + 4, :]

    rot_q, shift_q = frames(rw * n_rows + cl * 8)
    points = local(qp, None, cl * 8)
    cotan = [gpt[y, pl.ds(pl.multiple_of(cl * 8, 8), 8), :] for y in range(3)]
    qg = [v + shift_q[x] for x, v in enumerate(apply(rot_q, points))]
    gg = apply(rot_q, cotan)
    parts = [qf[g] for g in range(3)]
    qgrad[...] = (scale * inner) * gather(parts, 0, 64)
    ones = []
    for p in parts:
        v = jnp.where((lane8 >= 112) & (lane8 % 4 == 0), p, 0.0)
        ones.append(v + pltpu.roll(v, 1, 1) + pltpu.roll(v, 2, 1) + pltpu.roll(v, 3, 1))
    ones = gather(ones, 112, PAD)
    dqg = [
        -2.0 * c48 * (qg[x] * ones - gather(parts, 64 + PAD * x, PAD)) for x in range(3)
    ]
    parts = [qf[3 + g] for g in range(3)]
    opt = [gather(parts, 32 * x, 32) - shift_q[x] for x in range(3)]
    for y, v in enumerate(undo(rot_q, dqg)):
        qpgrad[y] = v
    entries = []
    for x in range(3):
        for y in range(3):
            entries.append(add_all(dqg[x] * points[y]) + add_all(opt[x] * cotan[y]))
        entries.append(add_all(dqg[x]) - add_all(gg[x]))
    frame_out(qframe, entries)

    rot_k, shift_k = frames(cl * 256 + rw * 8)
    lanes = pl.ds(pl.multiple_of((rw // 16) * 128, 128), 128)
    points = local(kp, lanes, (rw % 16) * 8)
    vpoints = local(vp, lanes, (rw % 16) * 8)
    kg = [v + shift_k[x] for x, v in enumerate(apply(rot_k, points))]
    parts = [kf[g] for g in range(3)]
    kgrad[...] = (scale * inner) * gather(parts, 0, 64)
    ones = gather(parts, 112, PAD)
    dkg = [2.0 * c48 * (gather(parts, 64 + PAD * x, PAD) - kg[x] * ones) for x in range(3)]
    parts = [kf[3 + g] for g in range(4)]
    vgrad[...] = gather(parts, 0, 48)
    dvg = [gather(parts, 48 + 24 * x, 24) for x in range(3)]
    for y, v in enumerate(undo(rot_k, dkg)):
        kpgrad[y] = v
    for y, v in enumerate(undo(rot_k, dvg)):
        vpgrad[y] = v
    entries = []
    for x in range(3):
        for y in range(3):
            entries.append(add_all(dkg[x] * points[y]) + add_all(dvg[x] * vpoints[y]))
        entries.append(add_all(dkg[x]) + add_all(dvg[x]))
    frame_out(kframe, entries)
    copy.wait()


def per_device(
    pair_rep, bias_weight, head_weight, queries, key_vectors, values, query_points, key_points,
    value_points, rotations, translations, residue_count, grad_output, grad_points, grad_pair,
):
    channels, heads = bias_weight.shape
    width = queries.shape[0] // heads
    qpoints = query_points.shape[1] // heads
    n_rows = queries.shape[1]
    n_cols = key_vectors.shape[1]
    logit_scale = math.sqrt(1.0 / 3.0)
    point_scale = math.sqrt(2.0 / (9.0 * qpoints))
    inner_scale = 1.0 / math.sqrt(width)
    coef_scale = 0.5 * logit_scale * point_scale
    hw = head_weight.reshape(1, heads)
    gpt = grad_points.transpose(0, 2, 1)

    vm = pl.BlockSpec(memory_space=pltpu.VMEM)
    hbm = pl.BlockSpec(memory_space=pltpu.HBM)
    big = (heads, n_rows, n_cols)
    flat = (heads * n_rows, n_cols)
    dma = pltpu.SemaphoreType.DMA
    inputs = (
        bias_weight.T, hw, grad_pair.transpose(1, 0, 2), queries.T, key_vectors, values,
        query_points, key_points, value_points, rotations, translations, grad_output.T, gpt,
    )
    like = lambda x: pltpu.VMEM(x.shape, x.dtype)
    pg, kf, qf, wr = pl.pallas_call(
        functools.partial(
            mega_kernel, heads, n_rows, n_cols, logit_scale, inner_scale, coef_scale
        ),
        in_specs=[pl.BlockSpec(memory_space=pltpu.SMEM), *[hbm] * 14],
        out_specs=[vm] * 4,
        out_shape=[
            jax.ShapeDtypeStruct(pair_rep.shape, BF16),
            jax.ShapeDtypeStruct((7, 8, 128), F32),
            jax.ShapeDtypeStruct((6, 8, 128), F32),
            jax.ShapeDtypeStruct((PAD, 128), F32),
        ],
        scratch_shapes=[
            *[like(x) for x in inputs],
            pltpu.VMEM(pair_rep.shape, BF16),
            pltpu.VMEM(big, F32),
            pltpu.VMEM(big, F32),
            *[pltpu.VMEM((n_rows * STRIDE, 128), F32)] * 4,
            *[pltpu.VMEM(flat, BF16)] * 4,
            pltpu.VMEM((n_rows * STRIDE, 128), F32),
            pltpu.VMEM((n_rows, 2 * PAD, 128), BF16),
            pltpu.VMEM((heads, 32, n_rows), F32),
            pltpu.VMEM((heads, 32, n_cols), F32),
            pltpu.VMEM((3, n_rows, 128), F32),
            pltpu.VMEM((32, 128), F32),
            pltpu.VMEM((32, 128), F32),
            pltpu.VMEM((32, 128), F32),
            pltpu.VMEM((3, 32, 128), F32),
            pltpu.VMEM((7, CORES, ZL * YN, 8, 128), F32),
            pltpu.VMEM((7, ZL * YN, 8, 128), F32),
            pltpu.VMEM((YN, 7, ZL, 8, 128), F32),
            pltpu.VMEM((YN - 1, 7, ZL, 8, 128), F32),
            pltpu.VMEM((ZL, 7, 8, 128), F32),
            pltpu.VMEM((ZL - 1, 7, 8, 128), F32),
            pltpu.VMEM((XN, ZH, 6, 8, 128), F32),
            pltpu.VMEM((XN - 1, ZH, 6, 8, 128), F32),
            pltpu.VMEM((ZH, 6, 8, 128), F32),
            pltpu.VMEM((6, 8, 128), F32),
            pltpu.VMEM((PAD, 128), F32),
            pltpu.VMEM((YN, PAD, 128), F32),
            pltpu.VMEM((XN, PAD, 128), F32),
            pltpu.VMEM((ZL * ZH, PAD, 128), F32),
            pltpu.VMEM((4, PAD, 128), F32),
            dma((4,)), dma((13,)),
            dma((4,)), dma((4,)),
            dma((7,)), dma((7,)),
            dma((3, 7)), dma((3, 7)),
            dma((3,)), dma((3,)),
            dma((4,)), dma((4,)),
            dma((14,)), dma((14,)),
        ],
        compiler_params=pltpu.CompilerParams(
            collective_id=0, has_side_effects=True, vmem_limit_bytes=VMEM_LIMIT
        ),
        name="mega",
    )(
        residue_count, pair_rep, *inputs
    )
    share = 8
    late = (hw, query_points, key_points, value_points, rotations, translations, gpt)
    f32 = lambda *shape: jax.ShapeDtypeStruct(shape, F32)
    outs = pl.pallas_call(
        functools.partial(
            finish_kernel, heads, n_rows, logit_scale, inner_scale, coef_scale
        ),
        in_specs=[vm] * 4 + [hbm] * 7,
        out_specs=[hbm] + [vm] * 10,
        out_shape=[
            jax.ShapeDtypeStruct(pair_rep.shape, BF16),
            f32(share, heads * width),
            f32(3, share, 48),
            f32(3, 4, share),
            f32(share, heads * width),
            f32(share, heads * width),
            f32(3, share, 48),
            f32(3, share, 96),
            f32(3, 4, share),
            f32(heads, channels),
            f32(1, heads),
        ],
        scratch_shapes=[*[like(x) for x in late], pltpu.VMEM((128, 128), F32), dma((7,)), dma],
        compiler_params=pltpu.CompilerParams(vmem_limit_bytes=VMEM_LIMIT),
        name="finish",
    )(pg, kf, qf, wr, *late)
    (pair_grad, qgrad, qpgrad, qframe, kgrad, vgrad, kpgrad, vpgrad, kframe, weight, head) = outs
    flip = lambda x: x.transpose(0, 2, 1)
    return (
        pair_grad, qgrad.T, flip(qpgrad), qframe, kgrad.T, vgrad.T, flip(kpgrad), flip(vpgrad),
        kframe, weight.T, head.reshape(heads),
    )


def solution(mesh):
    return jax.shard_map(
        per_device,
        mesh=mesh,
        in_specs=(
            P("row", "col", None),
            P(),
            P(),
            P(None, "row"),
            P(None, "col"),
            P(None, "col"),
            P(None, None, "row"),
            P(None, None, "col"),
            P(None, None, "col"),
            P(),
            P(),
            P(),
            P(None, "row"),
            P(None, None, "row"),
            P("row", None, None),
        ),
        out_specs=(
            P("row", "col", None),
            P(None, ("row", "col")),
            P(None, None, ("row", "col")),
            P(None, None, ("row", "col")),
            P(None, ("col", "row")),
            P(None, ("col", "row")),
            P(None, None, ("col", "row")),
            P(None, None, ("col", "row")),
            P(None, None, ("col", "row")),
            P(),
            P(),
        ),
        check_vma=False,
    )
```

```python
import functools
import math

import jax
import jax.numpy as jnp
from jax import lax
from jax.experimental import pallas as pl
from jax.experimental.pallas import tpu as pltpu
from jax.sharding import PartitionSpec as P

F32 = jnp.float32
BF16 = jnp.bfloat16
PAD = 16
VMEM_LIMIT = 50331648
ZL, YN, CORES = 4, 4, 2
XN, ZH = 4, 2
STRIDE = 40
MESH = pl.DeviceIdType.MESH


def dot(a, b, dims):
    return lax.dot_general(a, b, (dims, ((), ())), preferred_element_type=F32)


TN = ((0,), (0,))
NT = ((1,), (1,))
NN = ((1,), (0,))


def split2(x):
    hi = x.astype(BF16)
    return hi, (x - hi.astype(F32)).astype(BF16)


def split3(x):
    hi = x.astype(BF16)
    rest = x - hi.astype(F32)
    mid = rest.astype(BF16)
    return hi, mid, (rest - mid.astype(F32)).astype(BF16)


def lane_of(shape):
    return lax.broadcasted_iota(jnp.int32, shape, 1)


def merge_stats(parts):
    top = functools.reduce(jnp.maximum, parts)
    lane = lax.rem(lane_of(top.shape), 64)
    out = None
    for part in parts:
        f = jnp.exp(part - top)
        spread = jnp.where(lane < 2 * PAD, pltpu.roll(f, PAD, 1), pltpu.roll(f, 2 * PAD, 1))
        term = part * spread
        out = term if out is None else out + term
    return jnp.where(lane < PAD, top, out)


def push(src, dst, send, recv, row, col):
    copy = pltpu.make_async_remote_copy(
        src_ref=src, dst_ref=dst, send_sem=send, recv_sem=recv,
        device_id={"row": row, "col": col}, device_id_type=MESH,
    )
    copy.start()
    return copy


def group_mask(width, point, spread):
    row = lax.broadcasted_iota(jnp.int32, (128, 256), 0)
    lane = lane_of((128, 256))
    if width:
        body = (row - width * PAD) % (width * point)
        head = jnp.where(row < width * PAD, row // PAD, body // point)
    else:
        head = (row % 32) // point
    return head, lane // spread


def spread_heads(left, mask):
    left = jnp.concatenate([left, jnp.zeros_like(left)], 1)
    left = left + pltpu.roll(left, 64, 1)
    return jnp.where(mask, jnp.concatenate([left, left], 1), 0.0)


def soft(head_weight):
    return jnp.maximum(head_weight, 0.0) + jnp.log(1.0 + jnp.exp(-jnp.abs(head_weight)))


def mega_kernel(
    heads, n_rows, n_cols, scale, inner, coef_scale,
    rc, pair_hbm, *refs,
):
    sources, refs = refs[:13], refs[13:]
    pg_out, kf_out, qf_out, wr_out = refs[:4]
    staged, refs = refs[4:17], refs[17:]
    bw, hw, gp_t, qt, kt, vt, qp, kp, vp, rot, shift, got, gpt = staged
    (
    pair, lbase, dbase, fb0, fb1, rd0, rd1, a_hi, a_lo, d_hi, d_lo,
    wgf, wgb, qc, kc, wq, stat, stat_z, stat_m, stat_x,
    ks, ks_rx, sy, sy_rx, sz, sz_rx, qs, qs_rx, qz, qz_rx,
    ar_c, ar_y, ar_x, ar_z, ar_s,
    pair_sem, in_sem, s_send, s_recv, k_send, k_recv, y_send, y_recv, z_send, z_recv,
    q_send, q_recv, a_send, a_recv,
    ) = refs
    rw = lax.axis_index("row")
    cl = lax.axis_index("col")
    core = lax.rem(rw, CORES)
    yy = lax.rem(rw // CORES, YN)
    zl = rw // (CORES * YN)
    zh = lax.rem(cl, ZH)
    xx = cl // ZH
    row_of = lambda z, y, c: (z * YN + y) * CORES + c
    sibling = (row_of(zl, yy, 1 - core), cl)
    y_peer = lambda k: (row_of(zl, lax.rem(yy + k, YN), core), cl)
    z_peer = lambda k: (row_of(lax.rem(zl + k, ZL), yy, core), cl)
    x_peer = lambda k: (rw, lax.rem(xx + k, XN) * ZH + zh)
    h_peer = (rw, xx * ZH + 1 - zh)
    z8 = zh * ZL + zl

    def ring_peer(k):
        idx = lax.rem(z8 + k, ZL * ZH)
        return (row_of(lax.rem(idx, ZL), yy, core), xx * ZH + idx // ZL)

    incoming = []
    for n, (source, target) in enumerate(zip(sources, staged)):
        incoming.append(pltpu.make_async_copy(source, target, in_sem.at[n]))
        incoming[-1].start()
    parts = 4
    rows_per = n_rows // parts
    loads = []
    for p in range(parts):
        piece = pl.ds(p * rows_per, rows_per)
        load = pltpu.make_async_copy(pair_hbm.at[piece], pair.at[piece], pair_sem.at[p])
        load.start()
        loads.append(load)

    everyone = [sibling]
    everyone += [y_peer(k) for k in range(1, YN)]
    everyone += [x_peer(k) for k in range(1, XN)]
    everyone += [ring_peer(k) for k in range(1, ZL * ZH)]
    barrier = pltpu.get_barrier_semaphore()
    for peer in everyone:
        pl.semaphore_signal(
            barrier, inc=1, device_id={"row": peer[0], "col": peer[1]}, device_id_type=MESH
        )

    wgf[...] = jnp.zeros_like(wgf)
    for copy in incoming:
        copy.wait()
    w_all = bw[...].astype(F32)
    w_t = jnp.concatenate([w_all, jnp.zeros((PAD - heads, 128), F32)], 0)
    for h in range(heads):
        wgf[pl.ds(PAD + h, n_rows, stride=STRIDE), :] = gp_t[h].astype(F32)
    w_bf = w_t.astype(BF16)
    for r in range(n_rows):
        wgb[r, :PAD, :] = w_bf
        wgb[r, PAD:, :] = wgf[r * STRIDE + PAD : r * STRIDE + 2 * PAD, :].astype(BF16)

    row_block = pl.multiple_of((rw // 2) * 128, 128)
    col_block = pl.multiple_of(cl * n_cols, 128)

    def row_vec(ref, *index):
        v = ref[index + (pl.ds(row_block, 128),)]
        return jnp.where(core == 1, pltpu.roll(v, 64, 1), v)[:, :n_rows]

    rot_q = [[row_vec(rot, x, pl.ds(y, 1)) for y in range(3)] for x in range(3)]
    rot_k = [
        [rot[x, pl.ds(y, 1), pl.ds(col_block, n_cols)] for y in range(3)] for x in range(3)
    ]
    apply = lambda m, p: [m[x][0] * p[0] + m[x][1] * p[1] + m[x][2] * p[2] for x in range(3)]
    add_shift = lambda g, t: [g[x] + t[x] for x in range(3)]
    qg = add_shift(
        apply(rot_q, [qp[y] for y in range(3)]),
        [row_vec(shift, pl.ds(x, 1)) for x in range(3)],
    )
    shift_k = [shift[pl.ds(x, 1), pl.ds(col_block, n_cols)] for x in range(3)]
    kg = add_shift(apply(rot_k, [kp[y] for y in range(3)]), shift_k)
    vg = add_shift(apply(rot_k, [vp[y] for y in range(3)]), shift_k)
    gg = apply(rot_q, [gpt[y].T for y in range(3)])
    tall = lambda ref: jnp.concatenate([ref[:, :128].T, ref[:, 128:].T], 0)
    q_all = tall(qt)
    g_all = tall(got)
    q_sq = qg[0] * qg[0] + qg[1] * qg[1] + qg[2] * qg[2]
    k_sq = kg[0] * kg[0] + kg[1] * kg[1] + kg[2] * kg[2]
    size = q_sq.shape[0]
    back = lambda x, n: pltpu.roll(x, size - n, 0)
    q_sq = q_sq + back(q_sq, 1) + back(q_sq, 2) + back(q_sq, 3)
    k_sq = k_sq + pltpu.roll(k_sq, 1, 0) + pltpu.roll(k_sq, 2, 0) + pltpu.roll(k_sq, 3, 0)
    coef = coef_scale * soft(hw[...])

    for h in range(heads):
        c = coef[:, h : h + 1]
        qc[h, :PAD, :] = (scale * inner) * q_all[PAD * h : PAD * h + PAD]
        kc[h, :PAD, :] = kt[PAD * h : PAD * h + PAD, :]
        for x in range(3):
            qc[h, PAD + 4 * x : PAD + 4 * x + 4, :] = (2.0 * c) * qg[x][4 * h : 4 * h + 4]
            kc[h, PAD + 4 * x : PAD + 4 * x + 4, :] = kg[x][4 * h : 4 * h + 4]
        qc[h, 28:29, :] = jnp.broadcast_to(-c, (1, n_rows))
        qc[h, 29:30, :] = -c * q_sq[4 * h : 4 * h + 1]
        qc[h, 30:32, :] = jnp.zeros((2, n_rows), F32)
        kc[h, 28:29, :] = k_sq[4 * h + 3 : 4 * h + 4]
        kc[h, 29:30, :] = jnp.ones((1, n_cols), F32)
        kc[h, 30:32, :] = jnp.zeros((2, n_cols), F32)

    def point_rows(head, points, h):
        body = [points[x][8 * h : 8 * h + 8] for x in range(3)]
        return jnp.concatenate([head] + body + [jnp.zeros_like(body[0])], 0)

    for h in range(heads):
        q0, q1, q2 = split3(qc[h])
        k0, k1, k2 = split3(kc[h])
        lbase[h] = dot(
            jnp.concatenate([q0, q0, q1, q0, q2, q1], 0),
            jnp.concatenate([k0, k1, k0, k2, k0, k1], 0),
            TN,
        )
        g0, g1 = split2(point_rows(g_all[PAD * h : PAD * h + PAD], gg, h))
        v0, v1 = split2(point_rows(vt[PAD * h : PAD * h + PAD, :], vg, h))
        dbase[h] = dot(
            jnp.concatenate([g0, g0, g1], 0), jnp.concatenate([v0, v1, v0], 0), TN
        )

    for p in range(parts):
        loads[p].wait()

        for i in range(rows_per):
            r = p * rows_per + i
            res = dot(wgb[r], pair[r], NT)
            fb0[r * STRIDE : r * STRIDE + 2 * PAD, :] = res[:, :128]
            fb1[r * STRIDE : r * STRIDE + 2 * PAD, :] = res[:, 128:]

    limit = rc[0] - cl * n_cols
    valid = lane_of((n_rows, n_cols)) < limit
    lane = lane_of((n_rows, 128))
    packed = jnp.ones((n_rows, 128), F32)
    picked = lambda ref0, ref1, h: jnp.concatenate(
        [ref0[pl.ds(h, n_rows, stride=STRIDE), :], ref1[pl.ds(h, n_rows, stride=STRIDE), :]], 1
    )
    for h in range(heads):
        logit = lbase[h] + scale * picked(fb0, fb1, h)
        logit = jnp.where(valid, logit, F32(-1000000000.0))
        peak = jnp.max(logit, axis=1, keepdims=True)
        e = jnp.exp(logit - peak)
        d = dbase[h] + picked(fb0, fb1, PAD + h)
        lbase[h] = e
        dbase[h] = d
        packed = jnp.where(lane == h, peak, packed)
        packed = jnp.where(lane == PAD + h, jnp.sum(e, axis=1, keepdims=True), packed)
        packed = jnp.where(lane == 2 * PAD + h, jnp.sum(e * d, axis=1, keepdims=True), packed)
    half = n_rows // 2
    own = jnp.where(lane[:half] < 64, packed[:half], pltpu.roll(packed[half:], 64, 1))
    stat[...] = own

    pl.semaphore_wait(barrier, len(everyone))
    sends = []
    sends.append(push(stat, stat_z, s_send.at[0], s_recv.at[0], *h_peer))

    rd0[...] = jnp.zeros_like(rd0)
    rd1[...] = jnp.zeros_like(rd1)
    key_head, lane64 = group_mask(4, 4, 64)
    key_mask = key_head == lane64
    val_head, _ = group_mask(3, 8, 64)
    val_mask = val_head == lane64
    sub16 = lax.broadcasted_iota(jnp.int32, (PAD, n_rows), 0) % 4
    sub16k = lax.broadcasted_iota(jnp.int32, (PAD, n_cols), 0) % 4
    qb, gb, kb, vb = [], [], [], []
    for g in range(3):
        pts = slice(PAD * g, PAD * g + PAD)
        base = jnp.concatenate(
            [q_all[64 * g : 64 * g + 64]] + [qg[x][pts] for x in range(3)]
            + [jnp.ones((PAD, n_rows), F32)], 0
        )
        qb.append(split2(spread_heads(base, key_mask)))
        weights = jnp.concatenate(
            [jnp.zeros((64, n_rows), F32)] + [-2.0 * qg[x][pts] for x in range(3)]
            + [jnp.where(sub16 == 0, q_sq[pts], jnp.where(sub16 == 3, 1.0, 0.0))], 0
        )
        wq[g] = weights.T
        base = jnp.concatenate(
            [kt[64 * g : 64 * g + 64, :]] + [kg[x][pts] for x in range(3)]
            + [jnp.where(sub16k == 3, k_sq[pts], jnp.where(sub16k == 0, 1.0, 0.0))], 0
        )
        kb.append(split2(base))
        oct_rows = slice(32 * g, 32 * g + 32)
        base = jnp.concatenate(
            [vg[x][oct_rows] for x in range(3)] + [jnp.zeros((32, n_cols), F32)], 0
        )
        vb.append(split2(base))
    for g in range(4):
        pts = slice(24 * g, 24 * g + 24)
        base = jnp.concatenate(
            [g_all[48 * g : 48 * g + 48]] + [gg[x][pts] for x in range(3)]
            + [jnp.zeros((8, n_rows), F32)], 0
        )
        gb.append(split2(spread_heads(base, val_mask)))
    query_masks = [key_head == k for k in range(4)]
    point_head, _ = group_mask(0, 8, 64)
    point_masks = [point_head == k for k in range(4)]

    def landed(dst, send, recv, peer):
        pltpu.make_async_remote_copy(
            src_ref=dst, dst_ref=dst, send_sem=send, recv_sem=recv,
            device_id={"row": peer[0], "col": peer[1]}, device_id_type=MESH,
        ).wait_recv()

    landed(stat_z, s_send.at[0], s_recv.at[0], h_peer)
    pairwise = merge_stats([stat[...], stat_z[...]])
    stat_m[...] = pairwise
    for k in range(1, XN):
        sends.append(
            push(stat_m, stat_x.at[k - 1], s_send.at[k], s_recv.at[k], *x_peer(k))
        )
    for k in range(1, XN):
        landed(stat_x.at[k - 1], s_send.at[k], s_recv.at[k], x_peer(k))
    total = merge_stats([stat_m[...]] + [stat_x[k] for k in range(XN - 1)])
    mass = pltpu.roll(total, 128 - PAD, 1)
    factor = jnp.exp(stat[...] - total) / mass
    delta = pltpu.roll(total, 128 - 2 * PAD, 1) / mass
    factor = jnp.concatenate([factor, pltpu.roll(factor, 64, 1)], 0)
    delta = jnp.concatenate([delta, pltpu.roll(delta, 64, 1)], 0)

    def make_head(h):
        att = lbase[h] * factor[:, h : h + 1]
        dl = att * (dbase[h] - delta[:, h : h + 1])
        rows = pl.ds(h * n_rows, n_rows)
        a_hi[rows], a_lo[rows] = split2(att)
        d_hi[rows], d_lo[rows] = split2(dl)
        rd0[pl.ds(h, n_rows, stride=STRIDE), :] = dl[:, :128]
        rd1[pl.ds(h, n_rows, stride=STRIDE), :] = dl[:, 128:]
        rd0[pl.ds(PAD + h, n_rows, stride=STRIDE), :] = att[:, :128]
        rd1[pl.ds(PAD + h, n_rows, stride=STRIDE), :] = att[:, 128:]

    def key_group(g, pairs, hi, lo, first, count):
        depth = count * n_rows
        rows = pl.ds(first * n_rows, depth)
        left, small = pairs[0][:, :depth], pairs[1][:, :depth]
        res = dot(jnp.concatenate([left, small], 0), hi[rows], NN)
        res = res[:128] + res[128:] + dot(left, lo[rows], NN)
        flat = res.T.reshape(ZL * YN, CORES, 8, 128)
        for c in range(CORES):
            ks[g, c] = flat[:, c]
        sends.append(
            push(ks.at[g, 1 - core], ks_rx.at[g], k_send.at[g], k_recv.at[g], *sibling)
        )

    z_first = (0, 3)

    def order(g):
        first, second = (y_peer, yy), (z_peer, zl)
        return (second, first) if g in z_first else (first, second)

    def y_stage(g):
        landed(ks_rx.at[g], k_send.at[g], k_recv.at[g], sibling)
        both = (ks[g, core] + ks_rx[g]).reshape(ZL, YN, 8, 128)
        peer, place = order(g)[0]
        for n in range(YN):
            sy[n, g] = both[n] if g in z_first else both[:, n]
        for k in range(1, YN):
            sends.append(
                push(
                    sy.at[lax.rem(place + k, YN), g], sy_rx.at[k - 1, g],
                    y_send.at[k - 1, g], y_recv.at[k - 1, g], *peer(k)
                )
            )

    def z_stage(g):
        (peer, place), (after, slot) = order(g)
        for k in range(1, YN):
            landed(sy_rx.at[k - 1, g], y_send.at[k - 1, g], y_recv.at[k - 1, g], peer(k))
        mine = sy[place, g] + sy_rx[0, g] + sy_rx[1, g] + sy_rx[2, g]
        for n in range(ZL):
            sz[n, g] = mine[n]
        for k in range(1, ZL):
            sends.append(
                push(
                    sz.at[lax.rem(slot + k, ZL), g], sz_rx.at[k - 1, g],
                    z_send.at[k - 1, g], z_recv.at[k - 1, g], *after(k)
                )
            )

    def last_stage(g):
        _, (peer, place) = order(g)
        for k in range(1, ZL):
            landed(sz_rx.at[k - 1, g], z_send.at[k - 1, g], z_recv.at[k - 1, g], peer(k))
        kf_out[g] = sz[place, g] + sz_rx[0, g] + sz_rx[1, g] + sz_rx[2, g]

    for h in range(4):
        make_head(h)
    key_group(0, qb[0], d_hi, d_lo, 0, 4)
    key_group(3, gb[0], a_hi, a_lo, 0, 3)
    for h in range(4, 8):
        make_head(h)
    key_group(1, qb[1], d_hi, d_lo, 4, 4)
    key_group(4, gb[1], a_hi, a_lo, 3, 3)
    y_stage(0)
    y_stage(3)
    for h in range(8, 12):
        make_head(h)
    key_group(2, qb[2], d_hi, d_lo, 8, 4)
    key_group(5, gb[2], a_hi, a_lo, 6, 3)
    key_group(6, gb[3], a_hi, a_lo, 9, 3)
    y_stage(1)
    y_stage(4)

    def query_group(pairs, masks, hi, lo, first):
        blocks = lambda x: jnp.concatenate(
            [jnp.where(m, x, jnp.zeros_like(x)) for m in masks], 1
        )
        lefts = lambda ref: jnp.concatenate(
            [ref[pl.ds((first + k) * n_rows, n_rows)] for k in range(4)], 1
        )
        top = lefts(hi)
        res = dot(jnp.concatenate([top, lefts(lo)], 0), blocks(pairs[0]), NT)
        return res[:n_rows] + res[n_rows:] + dot(top, blocks(pairs[1]), NT)

    distance = []
    for g in range(6):
        if g < 3:
            res = query_group(kb[g], query_masks, d_hi, d_lo, 4 * g)
        else:
            res = query_group(vb[g - 3], point_masks, a_hi, a_lo, 4 * (g - 3))
        if g < 3:
            distance.append(jnp.sum(res * wq[g], axis=0, keepdims=True))
        flat = res.reshape(XN, ZH, 8, 128)
        for x in range(XN):
            for z in range(ZH):
                qs[x, z, g] = flat[x, z]
    for k in range(1, XN):
        sends.append(
            push(
                qs.at[lax.rem(xx + k, XN)], qs_rx.at[k - 1],
                q_send.at[k - 1], q_recv.at[k - 1], *x_peer(k)
            )
        )
    y_stage(2)
    y_stage(5)
    y_stage(6)

    both_rows = lambda r: jnp.concatenate(
        [rd0[r * STRIDE : r * STRIDE + 2 * PAD, :], rd1[r * STRIDE : r * STRIDE + 2 * PAD, :]], 1
    ).astype(BF16)
    acc = jnp.zeros((PAD, 128), F32)
    for r in range(n_rows):
        acc = acc + dot(both_rows(r)[:PAD], pair[r], NN)
    acc = scale * acc
    sub = lax.broadcasted_iota(jnp.int32, (PAD, 128), 0)
    lane1 = lane_of((1, 128))
    owner = jnp.where(lane1 < 112, (lane1 % PAD) // 4, (lane1 - 112) // 4)
    dist_row = jnp.zeros((1, 128), F32)
    for h in range(heads):
        part = jnp.sum(jnp.where(owner == h % 4, distance[h // 4], 0.0), axis=1, keepdims=True)
        dist_row = jnp.where(lane1 == h, part, dist_row)
    acc = jnp.where(sub == heads, dist_row, acc)
    ar_s[0] = acc
    sends.append(push(ar_s.at[0], ar_c, a_send.at[0], a_recv.at[0], *sibling))

    w_hi, w_lo = split2(scale * w_t)

    def pair_rows(first, count):
        for r in range(first, first + count):
            a = both_rows(r)
            lhs = jnp.concatenate([a, a[:PAD]], 0)
            rhs = jnp.concatenate([w_hi, wgb[r, PAD:, :], w_lo], 0)
            pg_out[r] = dot(lhs, rhs, TN).astype(BF16)

    quarter = n_rows // 4
    pair_rows(0, quarter)

    landed(ar_c, a_send.at[0], a_recv.at[0], sibling)
    ar_s[1] = ar_s[0] + ar_c[...]
    ar_x[xx] = ar_s[1]
    for k in range(1, XN):
        sends.append(push(ar_s.at[1], ar_x.at[xx], a_send.at[k], a_recv.at[k], *x_peer(k)))

    pair_rows(quarter, quarter)
    z_stage(0)
    z_stage(3)
    for k in range(1, XN):
        landed(qs_rx.at[k - 1], q_send.at[k - 1], q_recv.at[k - 1], x_peer(k))
    qz[...] = qs[xx] + qs_rx[0] + qs_rx[1] + qs_rx[2]
    sends.append(push(qz.at[1 - zh], qz_rx, q_send.at[3], q_recv.at[3], *h_peer))

    pair_rows(2 * quarter, quarter)
    z_stage(1)
    for k in range(1, XN):
        landed(ar_x.at[lax.rem(xx + XN - k, XN)], a_send.at[k], a_recv.at[k], x_peer(k))
    ar_s[2] = ar_x[0] + ar_x[1] + ar_x[2] + ar_x[3]
    ar_z[z8] = ar_s[2]
    for k in range(1, ZL * ZH):
        sends.append(
            push(ar_s.at[2], ar_z.at[z8], a_send.at[6 + k], a_recv.at[6 + k], *ring_peer(k))
        )

    pair_rows(3 * quarter, quarter)
    z_stage(4)
    z_stage(2)
    z_stage(5)
    z_stage(6)
    for k in range(1, ZL * ZH):
        landed(
            ar_z.at[lax.rem(z8 + ZL * ZH - k, ZL * ZH)], a_send.at[6 + k], a_recv.at[6 + k],
            ring_peer(k),
        )
    grand = ar_z[0]
    for k in range(1, ZL * ZH):
        grand = grand + ar_z[k]
    ar_s[3] = grand
    ar_y[yy] = ar_s[3]
    for k in range(1, YN):
        sends.append(
            push(ar_s.at[3], ar_y.at[yy], a_send.at[3 + k], a_recv.at[3 + k], *y_peer(k))
        )
    landed(qz_rx, q_send.at[3], q_recv.at[3], h_peer)
    qf_out[...] = qz[zh] + qz_rx[...]
    for g in (0, 3, 1, 4, 2, 5, 6):
        last_stage(g)
    for k in range(1, YN):
        landed(
            ar_y.at[lax.rem(yy + YN - k, YN)], a_send.at[3 + k], a_recv.at[3 + k], y_peer(k)
        )
    wr_out[...] = ar_y[0] + ar_y[1] + ar_y[2] + ar_y[3]
    for copy in sends:
        copy.wait_send()


def finish_kernel(
    heads, n_rows, scale, inner, coef_scale,
    pg, kf, qf, wr, hw_hbm, qp_hbm, kp_hbm, vp_hbm, rot_hbm, shift_hbm, gpt_hbm,
    pg_out, qgrad, qpgrad, qframe, kgrad, vgrad, kpgrad, vpgrad, kframe, weight, head_out,
    hw, qp, kp, vp, rot, shift, gpt, turned, in_sem, sem,
):
    incoming = []
    sources = (hw_hbm, qp_hbm, kp_hbm, vp_hbm, rot_hbm, shift_hbm, gpt_hbm)
    for n, (source, target) in enumerate(zip(sources, (hw, qp, kp, vp, rot, shift, gpt))):
        incoming.append(pltpu.make_async_copy(source, target, in_sem.at[n]))
        incoming[-1].start()
    copy = pltpu.make_async_copy(pg, pg_out, sem)
    copy.start()
    rw = lax.axis_index("row")
    cl = lax.axis_index("col")
    weight[...] = wr[:heads, :]
    for load in incoming:
        load.wait()
    sig = 1.0 / (1.0 + jnp.exp(-hw[...]))
    head_out[...] = wr[heads : heads + 1, :heads] * (-coef_scale) * sig
    coef = coef_scale * soft(hw[...])

    def frames(start):
        block = pl.multiple_of((start // 128) * 128, 128)
        rows = [rot[x, pl.ds(y, 1), pl.ds(block, 128)] for x in range(3) for y in range(3)]
        rows += [shift[pl.ds(x, 1), pl.ds(block, 128)] for x in range(3)]
        rows = jnp.concatenate(rows + [jnp.zeros((4, 128), F32)], 0)
        turned[:, :PAD] = rows.T
        own = turned[pl.ds(pl.multiple_of(start % 128, 8), 8), :PAD]
        entry = lambda k: own[:, k : k + 1]
        return [[entry(3 * x + y) for y in range(3)] for x in range(3)], [
            entry(9 + x) for x in range(3)
        ]

    def local(ref, lanes, offset):
        out = []
        for y in range(3):
            x = ref[y] if lanes is None else ref[y, :, lanes]
            x = x.T
            turned[: x.shape[0], : x.shape[1]] = x
            out.append(turned[pl.ds(pl.multiple_of(offset, 8), 8), : x.shape[1]])
        return out

    apply = lambda m, p: [m[x][0] * p[0] + m[x][1] * p[1] + m[x][2] * p[2] for x in range(3)]
    undo = lambda m, v: [m[0][y] * v[0] + m[1][y] * v[1] + m[2][y] * v[2] for y in range(3)]
    add_all = lambda x: jnp.sum(x, axis=1, keepdims=True)
    lane8 = lane_of((8, 128))

    def gather(parts, offset, size):
        return jnp.concatenate([p[:, offset : offset + size] for p in parts], 1)

    c48 = jnp.zeros((1, 128), F32)
    lane1 = lane_of((1, 128))
    for h in range(heads):
        c48 = jnp.where(lane1 // 4 == h, coef[:, h : h + 1], c48)
    c48 = c48[:, :48]

    def frame_out(ref, entries):
        tile = jnp.zeros((8, 128), F32)
        for k, value in enumerate(entries):
            tile = jnp.where(lane8 == k, value, tile)
        tile = tile.T
        for x in range(3):
            ref[x] = tile[4 * x : 4 * x + 4, :]

    rot_q, shift_q = frames(rw * n_rows + cl * 8)
    points = local(qp, None, cl * 8)
    cotan = [gpt[y, pl.ds(pl.multiple_of(cl * 8, 8), 8), :] for y in range(3)]
    qg = [v + shift_q[x] for x, v in enumerate(apply(rot_q, points))]
    gg = apply(rot_q, cotan)
    parts = [qf[g] for g in range(3)]
    qgrad[...] = (scale * inner) * gather(parts, 0, 64)
    ones = []
    for p in parts:
        v = jnp.where((lane8 >= 112) & (lane8 % 4 == 0), p, 0.0)
        ones.append(v + pltpu.roll(v, 1, 1) + pltpu.roll(v, 2, 1) + pltpu.roll(v, 3, 1))
    ones = gather(ones, 112, PAD)
    dqg = [
        -2.0 * c48 * (qg[x] * ones - gather(parts, 64 + PAD * x, PAD)) for x in range(3)
    ]
    parts = [qf[3 + g] for g in range(3)]
    opt = [gather(parts, 32 * x, 32) - shift_q[x] for x in range(3)]
    for y, v in enumerate(undo(rot_q, dqg)):
        qpgrad[y] = v
    entries = []
    for x in range(3):
        for y in range(3):
            entries.append(add_all(dqg[x] * points[y]) + add_all(opt[x] * cotan[y]))
        entries.append(add_all(dqg[x]) - add_all(gg[x]))
    frame_out(qframe, entries)

    rot_k, shift_k = frames(cl * 256 + rw * 8)
    lanes = pl.ds(pl.multiple_of((rw // 16) * 128, 128), 128)
    points = local(kp, lanes, (rw % 16) * 8)
    vpoints = local(vp, lanes, (rw % 16) * 8)
    kg = [v + shift_k[x] for x, v in enumerate(apply(rot_k, points))]
    parts = [kf[g] for g in range(3)]
    kgrad[...] = (scale * inner) * gather(parts, 0, 64)
    ones = gather(parts, 112, PAD)
    dkg = [2.0 * c48 * (gather(parts, 64 + PAD * x, PAD) - kg[x] * ones) for x in range(3)]
    parts = [kf[3 + g] for g in range(4)]
    vgrad[...] = gather(parts, 0, 48)
    dvg = [gather(parts, 48 + 24 * x, 24) for x in range(3)]
    for y, v in enumerate(undo(rot_k, dkg)):
        kpgrad[y] = v
    for y, v in enumerate(undo(rot_k, dvg)):
        vpgrad[y] = v
    entries = []
    for x in range(3):
        for y in range(3):
            entries.append(add_all(dkg[x] * points[y]) + add_all(dvg[x] * vpoints[y]))
        entries.append(add_all(dkg[x]) + add_all(dvg[x]))
    frame_out(kframe, entries)
    copy.wait()


def per_device(
    pair_rep, bias_weight, head_weight, queries, key_vectors, values, query_points, key_points,
    value_points, rotations, translations, residue_count, grad_output, grad_points, grad_pair,
):
    channels, heads = bias_weight.shape
    width = queries.shape[0] // heads
    qpoints = query_points.shape[1] // heads
    n_rows = queries.shape[1]
    n_cols = key_vectors.shape[1]
    logit_scale = math.sqrt(1.0 / 3.0)
    point_scale = math.sqrt(2.0 / (9.0 * qpoints))
    inner_scale = 1.0 / math.sqrt(width)
    coef_scale = 0.5 * logit_scale * point_scale
    hw = head_weight.reshape(1, heads)
    gpt = grad_points.transpose(0, 2, 1)

    vm = pl.BlockSpec(memory_space=pltpu.VMEM)
    hbm = pl.BlockSpec(memory_space=pltpu.HBM)
    big = (heads, n_rows, n_cols)
    flat = (heads * n_rows, n_cols)
    dma = pltpu.SemaphoreType.DMA
    inputs = (
        bias_weight.T, hw, grad_pair.transpose(1, 0, 2), queries.T, key_vectors, values,
        query_points, key_points, value_points, rotations, translations, grad_output.T, gpt,
    )
    like = lambda x: pltpu.VMEM(x.shape, x.dtype)
    inputs = tuple(pltpu.with_memory_space_constraint(x, pltpu.HBM) for x in inputs)
    pg, kf, qf, wr = pl.pallas_call(
        functools.partial(
            mega_kernel, heads, n_rows, n_cols, logit_scale, inner_scale, coef_scale
        ),
        in_specs=[pl.BlockSpec(memory_space=pltpu.SMEM), *[hbm] * 14],
        out_specs=[vm] * 4,
        out_shape=[
            pltpu.VMEM(pair_rep.shape, BF16),
            jax.ShapeDtypeStruct((7, 8, 128), F32),
            jax.ShapeDtypeStruct((6, 8, 128), F32),
            jax.ShapeDtypeStruct((PAD, 128), F32),
        ],
        scratch_shapes=[
            *[like(x) for x in inputs],
            pltpu.VMEM(pair_rep.shape, BF16),
            pltpu.VMEM(big, F32),
            pltpu.VMEM(big, F32),
            *[pltpu.VMEM((n_rows * STRIDE, 128), F32)] * 4,
            *[pltpu.VMEM(flat, BF16)] * 4,
            pltpu.VMEM((n_rows * STRIDE, 128), F32),
            pltpu.VMEM((n_rows, 2 * PAD, 128), BF16),
            pltpu.VMEM((heads, 32, n_rows), F32),
            pltpu.VMEM((heads, 32, n_cols), F32),
            pltpu.VMEM((3, n_rows, 128), F32),
            pltpu.VMEM((32, 128), F32),
            pltpu.VMEM((32, 128), F32),
            pltpu.VMEM((32, 128), F32),
            pltpu.VMEM((3, 32, 128), F32),
            pltpu.VMEM((7, CORES, ZL * YN, 8, 128), F32),
            pltpu.VMEM((7, ZL * YN, 8, 128), F32),
            pltpu.VMEM((YN, 7, ZL, 8, 128), F32),
            pltpu.VMEM((YN - 1, 7, ZL, 8, 128), F32),
            pltpu.VMEM((ZL, 7, 8, 128), F32),
            pltpu.VMEM((ZL - 1, 7, 8, 128), F32),
            pltpu.VMEM((XN, ZH, 6, 8, 128), F32),
            pltpu.VMEM((XN - 1, ZH, 6, 8, 128), F32),
            pltpu.VMEM((ZH, 6, 8, 128), F32),
            pltpu.VMEM((6, 8, 128), F32),
            pltpu.VMEM((PAD, 128), F32),
            pltpu.VMEM((YN, PAD, 128), F32),
            pltpu.VMEM((XN, PAD, 128), F32),
            pltpu.VMEM((ZL * ZH, PAD, 128), F32),
            pltpu.VMEM((4, PAD, 128), F32),
            dma((4,)), dma((13,)),
            dma((4,)), dma((4,)),
            dma((7,)), dma((7,)),
            dma((3, 7)), dma((3, 7)),
            dma((3, 7)), dma((3, 7)),
            dma((4,)), dma((4,)),
            dma((14,)), dma((14,)),
        ],
        compiler_params=pltpu.CompilerParams(
            collective_id=0, has_side_effects=True, vmem_limit_bytes=VMEM_LIMIT
        ),
        name="mega",
    )(
        residue_count, pair_rep, *inputs
    )
    share = 8
    late = (hw, query_points, key_points, value_points, rotations, translations, gpt)
    f32 = lambda *shape: jax.ShapeDtypeStruct(shape, F32)
    outs = pl.pallas_call(
        functools.partial(
            finish_kernel, heads, n_rows, logit_scale, inner_scale, coef_scale
        ),
        in_specs=[vm] * 4 + [hbm] * 7,
        out_specs=[hbm] + [vm] * 10,
        out_shape=[
            jax.ShapeDtypeStruct(pair_rep.shape, BF16),
            f32(share, heads * width),
            f32(3, share, 48),
            f32(3, 4, share),
            f32(share, heads * width),
            f32(share, heads * width),
            f32(3, share, 48),
            f32(3, share, 96),
            f32(3, 4, share),
            f32(heads, channels),
            f32(1, heads),
        ],
        scratch_shapes=[*[like(x) for x in late], pltpu.VMEM((128, 128), F32), dma((7,)), dma],
        compiler_params=pltpu.CompilerParams(vmem_limit_bytes=VMEM_LIMIT),
        name="finish",
    )(pg, kf, qf, wr, *late)
    (pair_grad, qgrad, qpgrad, qframe, kgrad, vgrad, kpgrad, vpgrad, kframe, weight, head) = outs
    flip = lambda x: x.transpose(0, 2, 1)
    return (
        pair_grad, qgrad.T, flip(qpgrad), qframe, kgrad.T, vgrad.T, flip(kpgrad), flip(vpgrad),
        kframe, weight.T, head.reshape(heads),
    )


def solution(mesh):
    return jax.shard_map(
        per_device,
        mesh=mesh,
        in_specs=(
            P("row", "col", None),
            P(),
            P(),
            P(None, "row"),
            P(None, "col"),
            P(None, "col"),
            P(None, None, "row"),
            P(None, None, "col"),
            P(None, None, "col"),
            P(),
            P(),
            P(),
            P(None, "row"),
            P(None, None, "row"),
            P("row", None, None),
        ),
        out_specs=(
            P("row", "col", None),
            P(None, ("row", "col")),
            P(None, None, ("row", "col")),
            P(None, None, ("row", "col")),
            P(None, ("col", "row")),
            P(None, ("col", "row")),
            P(None, None, ("col", "row")),
            P(None, None, ("col", "row")),
            P(None, None, ("col", "row")),
            P(),
            P(),
        ),
        check_vma=False,
    )
```

```python
import functools
import math

import jax
import jax.numpy as jnp
from jax import lax
from jax.experimental import pallas as pl
from jax.experimental.pallas import tpu as pltpu
from jax.sharding import PartitionSpec as P

F32 = jnp.float32
BF16 = jnp.bfloat16
PAD = 16
VMEM_LIMIT = 50331648
ZL, YN, CORES = 4, 4, 2
XN, ZH = 4, 2
STRIDE = 40
MESH = pl.DeviceIdType.MESH


def dot(a, b, dims):
    return lax.dot_general(a, b, (dims, ((), ())), preferred_element_type=F32)


TN = ((0,), (0,))
NT = ((1,), (1,))
NN = ((1,), (0,))


def split2(x):
    hi = x.astype(BF16)
    return hi, (x - hi.astype(F32)).astype(BF16)


def split3(x):
    hi = x.astype(BF16)
    rest = x - hi.astype(F32)
    mid = rest.astype(BF16)
    return hi, mid, (rest - mid.astype(F32)).astype(BF16)


def lane_of(shape):
    return lax.broadcasted_iota(jnp.int32, shape, 1)


def merge_stats(parts):
    top = functools.reduce(jnp.maximum, parts)
    lane = lax.rem(lane_of(top.shape), 64)
    out = None
    for part in parts:
        f = jnp.exp(part - top)
        spread = jnp.where(lane < 2 * PAD, pltpu.roll(f, PAD, 1), pltpu.roll(f, 2 * PAD, 1))
        term = part * spread
        out = term if out is None else out + term
    return jnp.where(lane < PAD, top, out)


def push(src, dst, send, recv, row, col):
    copy = pltpu.make_async_remote_copy(
        src_ref=src, dst_ref=dst, send_sem=send, recv_sem=recv,
        device_id={"row": row, "col": col}, device_id_type=MESH,
    )
    copy.start()
    return copy


def group_mask(width, point, spread):
    row = lax.broadcasted_iota(jnp.int32, (128, 256), 0)
    lane = lane_of((128, 256))
    if width:
        body = (row - width * PAD) % (width * point)
        head = jnp.where(row < width * PAD, row // PAD, body // point)
    else:
        head = (row % 32) // point
    return head, lane // spread


def spread_heads(left, mask):
    left = jnp.concatenate([left, jnp.zeros_like(left)], 1)
    left = left + pltpu.roll(left, 64, 1)
    return jnp.where(mask, jnp.concatenate([left, left], 1), 0.0)


def soft(head_weight):
    return jnp.maximum(head_weight, 0.0) + jnp.log(1.0 + jnp.exp(-jnp.abs(head_weight)))


def mega_kernel(
    heads, n_rows, n_cols, scale, inner, coef_scale,
    rc, pair_hbm, *refs,
):
    sources, refs = refs[:13], refs[13:]
    pg_out, kf_out, qf_out, wr_out = refs[:4]
    staged, refs = refs[4:17], refs[17:]
    bw, hw, gp_t, qt, kt, vt, qp, kp, vp, rot, shift, got, gpt = staged
    (
    pair, lbase, dbase, fb0, fb1, rd0, rd1, a_hi, a_lo, d_hi, d_lo,
    wgf, wgb, qc, kc, wq, tt, qu, stat, stat_z, stat_m, stat_x,
    ks, ks_rx, sy, sy_rx, sz, sz_rx, qs, qs_rx, qz, qz_rx,
    ar_y, ar_x, ar_z, ar_s,
    pair_sem, in_sem, s_send, s_recv, k_send, k_recv, y_send, y_recv, z_send, z_recv,
    q_send, q_recv, a_send, a_recv,
    ) = refs
    rw = lax.axis_index("row")
    cl = lax.axis_index("col")
    core = lax.rem(rw, CORES)
    yy = lax.rem(rw // CORES, YN)
    zl = rw // (CORES * YN)
    zh = lax.rem(cl, ZH)
    xx = cl // ZH
    row_of = lambda z, y, c: (z * YN + y) * CORES + c
    sibling = (row_of(zl, yy, 1 - core), cl)
    y_peer = lambda k: (row_of(zl, lax.rem(yy + k, YN), core), cl)
    z_peer = lambda k: (row_of(lax.rem(zl + k, ZL), yy, core), cl)
    x_peer = lambda k: (rw, lax.rem(xx + k, XN) * ZH + zh)
    xc8 = xx * CORES + core

    def plane_peer(k):
        idx = lax.rem(xc8 + k, XN * CORES)
        return (row_of(zl, yy, lax.rem(idx, CORES)), (idx // CORES) * ZH + zh)

    h_peer = (rw, xx * ZH + 1 - zh)
    z8 = zh * ZL + zl

    def ring_peer(k):
        idx = lax.rem(z8 + k, ZL * ZH)
        return (row_of(lax.rem(idx, ZL), yy, core), xx * ZH + idx // ZL)

    incoming = []
    for n, (source, target) in enumerate(zip(sources, staged)):
        incoming.append(pltpu.make_async_copy(source, target, in_sem.at[n]))
    for n in (2, 0, 11, 3, 8, 7, 12, 9, 10, 4, 5, 6, 1):
        incoming[n].start()
    parts = 4
    rows_per = n_rows // parts
    loads = []
    for p in range(parts):
        piece = pl.ds(p * rows_per, rows_per)
        load = pltpu.make_async_copy(pair_hbm.at[piece], pair.at[piece], pair_sem.at[p])
        load.start()
        loads.append(load)

    everyone = [y_peer(k) for k in range(1, YN)]
    everyone += [plane_peer(k) for k in range(1, XN * CORES)]
    everyone += [ring_peer(k) for k in range(1, ZL * ZH)]
    barrier = pltpu.get_barrier_semaphore()
    for peer in everyone:
        pl.semaphore_signal(
            barrier, inc=1, device_id={"row": peer[0], "col": peer[1]}, device_id_type=MESH
        )

    wgf[...] = jnp.zeros_like(wgf)
    incoming[2].wait()
    incoming[0].wait()
    w_all = bw[...].astype(F32)
    w_t = jnp.concatenate([w_all, jnp.zeros((PAD - heads, 128), F32)], 0)
    for h in range(heads):
        wgf[pl.ds(PAD + h, n_rows, stride=STRIDE), :] = gp_t[h].astype(F32)
    w_bf = w_t.astype(BF16)
    for r in range(n_rows):
        wgb[r, :PAD, :] = w_bf
        wgb[r, PAD:, :] = wgf[r * STRIDE + PAD : r * STRIDE + 2 * PAD, :].astype(BF16)

    for n in (11, 3, 8, 7, 12, 9, 10, 4, 5, 6, 1):
        incoming[n].wait()
    row_block = pl.multiple_of((rw // 2) * 128, 128)
    col_block = pl.multiple_of(cl * n_cols, 128)

    def row_vec(ref, *index):
        v = ref[index + (pl.ds(row_block, 128),)]
        return jnp.where(core == 1, pltpu.roll(v, 64, 1), v)[:, :n_rows]

    rot_q = [[row_vec(rot, x, pl.ds(y, 1)) for y in range(3)] for x in range(3)]
    rot_k = [
        [rot[x, pl.ds(y, 1), pl.ds(col_block, n_cols)] for y in range(3)] for x in range(3)
    ]
    apply = lambda m, p: [m[x][0] * p[0] + m[x][1] * p[1] + m[x][2] * p[2] for x in range(3)]
    add_shift = lambda g, t: [g[x] + t[x] for x in range(3)]
    qg = add_shift(
        apply(rot_q, [qp[y] for y in range(3)]),
        [row_vec(shift, pl.ds(x, 1)) for x in range(3)],
    )
    shift_k = [shift[pl.ds(x, 1), pl.ds(col_block, n_cols)] for x in range(3)]
    kg = add_shift(apply(rot_k, [kp[y] for y in range(3)]), shift_k)
    vg = add_shift(apply(rot_k, [vp[y] for y in range(3)]), shift_k)
    gg = apply(rot_q, [gpt[y].T for y in range(3)])
    tall = lambda ref: jnp.concatenate([ref[:, :128].T, ref[:, 128:].T], 0)
    q_all = tall(qt)
    g_all = tall(got)
    q_sq = qg[0] * qg[0] + qg[1] * qg[1] + qg[2] * qg[2]
    k_sq = kg[0] * kg[0] + kg[1] * kg[1] + kg[2] * kg[2]
    size = q_sq.shape[0]
    back = lambda x, n: pltpu.roll(x, size - n, 0)
    q_sq = q_sq + back(q_sq, 1) + back(q_sq, 2) + back(q_sq, 3)
    k_sq = k_sq + pltpu.roll(k_sq, 1, 0) + pltpu.roll(k_sq, 2, 0) + pltpu.roll(k_sq, 3, 0)
    coef = coef_scale * soft(hw[...])

    for h in range(heads):
        c = coef[:, h : h + 1]
        qc[h, :PAD, :] = (scale * inner) * q_all[PAD * h : PAD * h + PAD]
        kc[h, :PAD, :] = kt[PAD * h : PAD * h + PAD, :]
        for x in range(3):
            qc[h, PAD + 4 * x : PAD + 4 * x + 4, :] = (2.0 * c) * qg[x][4 * h : 4 * h + 4]
            kc[h, PAD + 4 * x : PAD + 4 * x + 4, :] = kg[x][4 * h : 4 * h + 4]
        qc[h, 28:29, :] = jnp.broadcast_to(-c, (1, n_rows))
        qc[h, 29:30, :] = -c * q_sq[4 * h : 4 * h + 1]
        qc[h, 30:32, :] = jnp.zeros((2, n_rows), F32)
        kc[h, 28:29, :] = k_sq[4 * h + 3 : 4 * h + 4]
        kc[h, 29:30, :] = jnp.ones((1, n_cols), F32)
        kc[h, 30:32, :] = jnp.zeros((2, n_cols), F32)

    def point_rows(head, points, h):
        body = [points[x][8 * h : 8 * h + 8] for x in range(3)]
        return jnp.concatenate([head] + body + [jnp.zeros_like(body[0])], 0)

    for h in range(heads):
        q0, q1, q2 = split3(qc[h])
        k0, k1, k2 = split3(kc[h])
        lbase[h] = dot(
            jnp.concatenate([q0, q0, q1, q0, q2, q1], 0),
            jnp.concatenate([k0, k1, k0, k2, k0, k1], 0),
            TN,
        )
        g0, g1 = split2(point_rows(g_all[PAD * h : PAD * h + PAD], gg, h))
        v0, v1 = split2(point_rows(vt[PAD * h : PAD * h + PAD, :], vg, h))
        dbase[h] = dot(
            jnp.concatenate([g0, g0, g1], 0), jnp.concatenate([v0, v1, v0], 0), TN
        )

    for p in range(parts):
        loads[p].wait()

        for i in range(rows_per):
            r = p * rows_per + i
            res = dot(wgb[r], pair[r], NT)
            fb0[r * STRIDE : r * STRIDE + 2 * PAD, :] = res[:, :128]
            fb1[r * STRIDE : r * STRIDE + 2 * PAD, :] = res[:, 128:]

    limit = rc[0] - cl * n_cols
    valid = lane_of((n_rows, n_cols)) < limit
    lane = lane_of((n_rows, 128))
    packed = jnp.ones((n_rows, 128), F32)
    picked = lambda ref0, ref1, h: jnp.concatenate(
        [ref0[pl.ds(h, n_rows, stride=STRIDE), :], ref1[pl.ds(h, n_rows, stride=STRIDE), :]], 1
    )
    for h in range(heads):
        logit = lbase[h] + scale * picked(fb0, fb1, h)
        logit = jnp.where(valid, logit, F32(-1000000000.0))
        peak = jnp.max(logit, axis=1, keepdims=True)
        e = jnp.exp(logit - peak)
        d = dbase[h] + picked(fb0, fb1, PAD + h)
        lbase[h] = e
        dbase[h] = d
        packed = jnp.where(lane == h, peak, packed)
        packed = jnp.where(lane == PAD + h, jnp.sum(e, axis=1, keepdims=True), packed)
        packed = jnp.where(lane == 2 * PAD + h, jnp.sum(e * d, axis=1, keepdims=True), packed)
    half = n_rows // 2
    own = jnp.where(lane[:half] < 64, packed[:half], pltpu.roll(packed[half:], 64, 1))
    stat[...] = own

    pl.semaphore_wait(barrier, len(everyone))
    sends = []
    sends.append(push(stat, stat_z, s_send.at[0], s_recv.at[0], *h_peer))

    rd0[...] = jnp.zeros_like(rd0)
    rd1[...] = jnp.zeros_like(rd1)
    key_head, lane64 = group_mask(4, 4, 64)
    key_mask = key_head == lane64
    val_head, _ = group_mask(3, 8, 64)
    val_mask = val_head == lane64
    sub16 = lax.broadcasted_iota(jnp.int32, (PAD, n_rows), 0) % 4
    sub16k = lax.broadcasted_iota(jnp.int32, (PAD, n_cols), 0) % 4
    qb, gb, kb, vb = [], [], [], []
    for g in range(3):
        pts = slice(PAD * g, PAD * g + PAD)
        base = jnp.concatenate(
            [q_all[64 * g : 64 * g + 64]] + [qg[x][pts] for x in range(3)]
            + [jnp.ones((PAD, n_rows), F32)], 0
        )
        qb.append(split2(spread_heads(base, key_mask)))
        weights = jnp.concatenate(
            [jnp.zeros((64, n_rows), F32)] + [-2.0 * qg[x][pts] for x in range(3)]
            + [jnp.where(sub16 == 0, q_sq[pts], jnp.where(sub16 == 3, 1.0, 0.0))], 0
        )
        wq[g] = weights.T
        base = jnp.concatenate(
            [kt[64 * g : 64 * g + 64, :]] + [kg[x][pts] for x in range(3)]
            + [jnp.where(sub16k == 3, k_sq[pts], jnp.where(sub16k == 0, 1.0, 0.0))], 0
        )
        kb.append(split2(base))
        oct_rows = slice(32 * g, 32 * g + 32)
        base = jnp.concatenate(
            [vg[x][oct_rows] for x in range(3)] + [jnp.zeros((32, n_cols), F32)], 0
        )
        vb.append(split2(base))
    for g in range(4):
        pts = slice(24 * g, 24 * g + 24)
        base = jnp.concatenate(
            [g_all[48 * g : 48 * g + 48]] + [gg[x][pts] for x in range(3)]
            + [jnp.zeros((8, n_rows), F32)], 0
        )
        gb.append(split2(spread_heads(base, val_mask)))
    query_masks = [key_head == k for k in range(4)]
    point_head, _ = group_mask(0, 8, 64)
    point_masks = [point_head == k for k in range(4)]

    def query_group(pairs, masks, hi, lo, first):
        blocks = lambda x: jnp.concatenate(
            [jnp.where(m, x, jnp.zeros_like(x)) for m in masks], 1
        )
        lefts = lambda ref: jnp.concatenate(
            [ref[pl.ds((first + k) * n_rows, n_rows)] for k in range(4)], 1
        )
        top = lefts(hi)
        res = dot(jnp.concatenate([top, lefts(lo)], 0), blocks(pairs[0]), NT)
        return res[:n_rows] + res[n_rows:] + dot(top, blocks(pairs[1]), NT)

    both_rows = lambda r: jnp.concatenate(
        [rd0[r * STRIDE : r * STRIDE + 2 * PAD, :], rd1[r * STRIDE : r * STRIDE + 2 * PAD, :]], 1
    )
    nearby = pltpu.roll(packed, 128 - 2 * PAD, 1) / pltpu.roll(packed, 128 - PAD, 1)
    for h in range(heads):
        e = lbase[h]
        d = dbase[h] - nearby[:, h : h + 1]
        dbase[h] = d
        both = e * d
        rows = pl.ds(h * n_rows, n_rows)
        a_hi[rows], a_lo[rows] = split2(e)
        d_hi[rows], d_lo[rows] = split2(both)
        rd0[pl.ds(h, n_rows, stride=STRIDE), :] = both[:, :128]
        rd1[pl.ds(h, n_rows, stride=STRIDE), :] = both[:, 128:]
        rd0[pl.ds(PAD + h, n_rows, stride=STRIDE), :] = e[:, :128]
        rd1[pl.ds(PAD + h, n_rows, stride=STRIDE), :] = e[:, 128:]
    for g in range(3):
        qu[g] = query_group(kb[g], query_masks, d_hi, d_lo, 4 * g)
        qu[3 + g] = query_group(kb[g], query_masks, a_hi, a_lo, 4 * g)
        qu[6 + g] = query_group(vb[g], point_masks, a_hi, a_lo, 4 * g)
    for r in range(n_rows):
        res = dot(jnp.concatenate(split2(both_rows(r)), 0), pair[r], NN)
        tt[r] = res[: 2 * PAD] + res[2 * PAD :]

    def landed(dst, send, recv, peer):
        pltpu.make_async_remote_copy(
            src_ref=dst, dst_ref=dst, send_sem=send, recv_sem=recv,
            device_id={"row": peer[0], "col": peer[1]}, device_id_type=MESH,
        ).wait_recv()

    landed(stat_z, s_send.at[0], s_recv.at[0], h_peer)
    pairwise = merge_stats([stat[...], stat_z[...]])
    stat_m[...] = pairwise
    for k in range(1, XN):
        sends.append(
            push(stat_m, stat_x.at[k - 1], s_send.at[k], s_recv.at[k], *x_peer(k))
        )
    for k in range(1, XN):
        landed(stat_x.at[k - 1], s_send.at[k], s_recv.at[k], x_peer(k))
    total = merge_stats([stat_m[...]] + [stat_x[k] for k in range(XN - 1)])
    mass = pltpu.roll(total, 128 - PAD, 1)
    factor = jnp.exp(stat[...] - total) / mass
    delta = pltpu.roll(total, 128 - 2 * PAD, 1) / mass
    factor = jnp.concatenate([factor, pltpu.roll(factor, 64, 1)], 0)
    delta = jnp.concatenate([delta, pltpu.roll(delta, 64, 1)], 0)

    def share(n, slots, place, count, peer, first):
        for k in range(1, count):
            sends.append(
                push(
                    ar_s.at[n], slots.at[place], a_send.at[first + k], a_recv.at[first + k],
                    *peer(k)
                )
            )

    def collect(slots, place, count, peer, first):
        for k in range(1, count):
            landed(
                slots.at[lax.rem(place + count - k, count)], a_send.at[first + k],
                a_recv.at[first + k], peer(k)
            )
        grand = slots[0]
        for k in range(1, count):
            grand = grand + slots[k]
        return grand

    moved = nearby - delta
    row_factor = jnp.concatenate([factor, jnp.zeros_like(factor)], 0).T[:PAD]
    row_moved = jnp.concatenate([moved[:, :PAD], jnp.zeros((n_rows, 128 - PAD), F32)], 1)
    row_moved = jnp.concatenate([row_moved, jnp.zeros_like(row_moved)], 0).T[:PAD]
    acc = jnp.zeros((PAD, 128), F32)
    for r in range(n_rows):
        term = tt[r, :PAD, :] + row_moved[:, r : r + 1] * tt[r, PAD:, :]
        acc = acc + row_factor[:, r : r + 1] * term
    lane_key = jnp.where(lane < 64, lane // PAD, (lane % PAD) // 4)
    lane_point = (lane % 32) // 8

    def spread(x, g, owner):
        out = jnp.broadcast_to(x[:, 4 * g : 4 * g + 1], (n_rows, 128))
        for k in range(1, 4):
            out = jnp.where(owner == k, x[:, 4 * g + k : 4 * g + k + 1], out)
        return out

    distance, q_results = [], []
    for g in range(3):
        res = spread(factor, g, lane_key) * (qu[g] + spread(moved, g, lane_key) * qu[3 + g])
        distance.append(jnp.sum(res * wq[g], axis=0, keepdims=True))
        q_results.append(res)
    acc = scale * acc
    sub = lax.broadcasted_iota(jnp.int32, (PAD, 128), 0)
    lane1 = lane_of((1, 128))
    owner = jnp.where(lane1 < 112, (lane1 % PAD) // 4, (lane1 - 112) // 4)
    dist_row = jnp.zeros((1, 128), F32)
    for h in range(heads):
        part = jnp.sum(jnp.where(owner == h % 4, distance[h // 4], 0.0), axis=1, keepdims=True)
        dist_row = jnp.where(lane1 == h, part, dist_row)
    acc = jnp.where(sub == heads, dist_row, acc)
    ar_s[0] = acc
    ar_z[z8] = acc

    share(0, ar_z, z8, ZL * ZH, ring_peer, -1)

    def make_head(h):
        att = lbase[h] * factor[:, h : h + 1]
        dl = att * (dbase[h] + moved[:, h : h + 1])
        rows = pl.ds(h * n_rows, n_rows)
        a_hi[rows], a_lo[rows] = split2(att)
        d_hi[rows], d_lo[rows] = split2(dl)
        rd0[pl.ds(h, n_rows, stride=STRIDE), :] = dl[:, :128]
        rd1[pl.ds(h, n_rows, stride=STRIDE), :] = dl[:, 128:]
        rd0[pl.ds(PAD + h, n_rows, stride=STRIDE), :] = att[:, :128]
        rd1[pl.ds(PAD + h, n_rows, stride=STRIDE), :] = att[:, 128:]

    def key_group(g, pairs, hi, lo, first, count):
        depth = count * n_rows
        rows = pl.ds(first * n_rows, depth)
        left, small = pairs[0][:, :depth], pairs[1][:, :depth]
        res = dot(jnp.concatenate([left, small], 0), hi[rows], NN)
        res = res[:128] + res[128:] + dot(left, lo[rows], NN)
        flat = res.T.reshape(ZL * YN, CORES, 8, 128)
        for c in range(CORES):
            ks[g, c] = flat[:, c]
        sends.append(
            push(ks.at[g, 1 - core], ks_rx.at[g], k_send.at[g], k_recv.at[g], *sibling)
        )

    z_first = (0, 3)

    def order(g):
        first, second = (y_peer, yy), (z_peer, zl)
        return (second, first) if g in z_first else (first, second)

    def y_stage(g):
        landed(ks_rx.at[g], k_send.at[g], k_recv.at[g], sibling)
        both = (ks[g, core] + ks_rx[g]).reshape(ZL, YN, 8, 128)
        peer, place = order(g)[0]
        for n in range(YN):
            sy[n, g] = both[n] if g in z_first else both[:, n]
        for k in range(1, YN):
            sends.append(
                push(
                    sy.at[lax.rem(place + k, YN), g], sy_rx.at[k - 1, g],
                    y_send.at[k - 1, g], y_recv.at[k - 1, g], *peer(k)
                )
            )

    def z_stage(g):
        (peer, place), (after, slot) = order(g)
        for k in range(1, YN):
            landed(sy_rx.at[k - 1, g], y_send.at[k - 1, g], y_recv.at[k - 1, g], peer(k))
        mine = sy[place, g] + sy_rx[0, g] + sy_rx[1, g] + sy_rx[2, g]
        for n in range(ZL):
            sz[n, g] = mine[n]
        for k in range(1, ZL):
            sends.append(
                push(
                    sz.at[lax.rem(slot + k, ZL), g], sz_rx.at[k - 1, g],
                    z_send.at[k - 1, g], z_recv.at[k - 1, g], *after(k)
                )
            )

    def last_stage(g):
        _, (peer, place) = order(g)
        for k in range(1, ZL):
            landed(sz_rx.at[k - 1, g], z_send.at[k - 1, g], z_recv.at[k - 1, g], peer(k))
        kf_out[g] = sz[place, g] + sz_rx[0, g] + sz_rx[1, g] + sz_rx[2, g]

    for h in range(4):
        make_head(h)
    key_group(0, qb[0], d_hi, d_lo, 0, 4)
    key_group(3, gb[0], a_hi, a_lo, 0, 3)
    for h in range(4, 8):
        make_head(h)
    key_group(1, qb[1], d_hi, d_lo, 4, 4)
    key_group(4, gb[1], a_hi, a_lo, 3, 3)
    for h in range(8, 12):
        make_head(h)
    key_group(2, qb[2], d_hi, d_lo, 8, 4)
    key_group(5, gb[2], a_hi, a_lo, 6, 3)
    key_group(6, gb[3], a_hi, a_lo, 9, 3)

    for g in (0, 3, 1, 4, 2, 5, 6):
        y_stage(g)
    for g in range(3):
        q_results.append(spread(factor, g, lane_point) * qu[6 + g])
    for g in range(6):
        flat = q_results[g].reshape(XN, ZH, 8, 128)
        for x in range(XN):
            for z in range(ZH):
                qs[x, z, g] = flat[x, z]
    for k in range(1, XN):
        sends.append(
            push(
                qs.at[lax.rem(xx + k, XN)], qs_rx.at[k - 1],
                q_send.at[k - 1], q_recv.at[k - 1], *x_peer(k)
            )
        )
    w_hi, w_lo = split2(scale * w_t)

    def pair_rows(first, count):
        for r in range(first, first + count):
            a = both_rows(r).astype(BF16)
            lhs = jnp.concatenate([a, a[:PAD]], 0)
            rhs = jnp.concatenate([w_hi, wgb[r, PAD:, :], w_lo], 0)
            pg_out[r] = dot(lhs, rhs, TN).astype(BF16)

    pair_rows(0, n_rows)
    z_stage(0)
    z_stage(3)
    for k in range(1, XN):
        landed(qs_rx.at[k - 1], q_send.at[k - 1], q_recv.at[k - 1], x_peer(k))
    qz[...] = qs[xx] + qs_rx[0] + qs_rx[1] + qs_rx[2]
    sends.append(push(qz.at[1 - zh], qz_rx, q_send.at[3], q_recv.at[3], *h_peer))
    grand = collect(ar_z, z8, ZL * ZH, ring_peer, -1)
    ar_s[1] = grand
    ar_x[xc8] = grand
    share(1, ar_x, xc8, XN * CORES, plane_peer, 6)
    for g in (1, 4, 2, 5, 6):
        z_stage(g)
    grand = collect(ar_x, xc8, XN * CORES, plane_peer, 6)
    ar_s[2] = grand
    ar_y[yy] = grand
    share(2, ar_y, yy, YN, y_peer, 13)
    landed(qz_rx, q_send.at[3], q_recv.at[3], h_peer)
    qf_out[...] = qz[zh] + qz_rx[...]
    for g in (0, 3, 1, 4, 2, 5, 6):
        last_stage(g)
    wr_out[...] = collect(ar_y, yy, YN, y_peer, 13)
    for copy in sends:
        copy.wait_send()


def finish_kernel(
    heads, n_rows, scale, inner, coef_scale,
    pg, kf, qf, wr, hw_hbm, qp_hbm, kp_hbm, vp_hbm, rot_hbm, shift_hbm, gpt_hbm,
    pg_out, qgrad, qpgrad, qframe, kgrad, vgrad, kpgrad, vpgrad, kframe, weight, head_out,
    hw, qp, kp, vp, rot, shift, gpt, turned, in_sem, sem,
):
    incoming = []
    sources = (hw_hbm, qp_hbm, kp_hbm, vp_hbm, rot_hbm, shift_hbm, gpt_hbm)
    for n, (source, target) in enumerate(zip(sources, (hw, qp, kp, vp, rot, shift, gpt))):
        incoming.append(pltpu.make_async_copy(source, target, in_sem.at[n]))
        incoming[-1].start()
    copy = pltpu.make_async_copy(pg, pg_out, sem)
    copy.start()
    rw = lax.axis_index("row")
    cl = lax.axis_index("col")
    weight[...] = wr[:heads, :]
    for load in incoming:
        load.wait()
    sig = 1.0 / (1.0 + jnp.exp(-hw[...]))
    head_out[...] = wr[heads : heads + 1, :heads] * (-coef_scale) * sig
    coef = coef_scale * soft(hw[...])

    def frames(start):
        block = pl.multiple_of((start // 128) * 128, 128)
        rows = [rot[x, pl.ds(y, 1), pl.ds(block, 128)] for x in range(3) for y in range(3)]
        rows += [shift[pl.ds(x, 1), pl.ds(block, 128)] for x in range(3)]
        rows = jnp.concatenate(rows + [jnp.zeros((4, 128), F32)], 0)
        turned[:, :PAD] = rows.T
        own = turned[pl.ds(pl.multiple_of(start % 128, 8), 8), :PAD]
        entry = lambda k: own[:, k : k + 1]
        return [[entry(3 * x + y) for y in range(3)] for x in range(3)], [
            entry(9 + x) for x in range(3)
        ]

    def local(ref, lanes, offset):
        out = []
        for y in range(3):
            x = ref[y] if lanes is None else ref[y, :, lanes]
            x = x.T
            turned[: x.shape[0], : x.shape[1]] = x
            out.append(turned[pl.ds(pl.multiple_of(offset, 8), 8), : x.shape[1]])
        return out

    apply = lambda m, p: [m[x][0] * p[0] + m[x][1] * p[1] + m[x][2] * p[2] for x in range(3)]
    undo = lambda m, v: [m[0][y] * v[0] + m[1][y] * v[1] + m[2][y] * v[2] for y in range(3)]
    add_all = lambda x: jnp.sum(x, axis=1, keepdims=True)
    lane8 = lane_of((8, 128))

    def gather(parts, offset, size):
        return jnp.concatenate([p[:, offset : offset + size] for p in parts], 1)

    c48 = jnp.zeros((1, 128), F32)
    lane1 = lane_of((1, 128))
    for h in range(heads):
        c48 = jnp.where(lane1 // 4 == h, coef[:, h : h + 1], c48)
    c48 = c48[:, :48]

    def frame_out(ref, entries):
        tile = jnp.zeros((8, 128), F32)
        for k, value in enumerate(entries):
            tile = jnp.where(lane8 == k, value, tile)
        tile = tile.T
        for x in range(3):
            ref[x] = tile[4 * x : 4 * x + 4, :]

    rot_q, shift_q = frames(rw * n_rows + cl * 8)
    points = local(qp, None, cl * 8)
    cotan = [gpt[y, pl.ds(pl.multiple_of(cl * 8, 8), 8), :] for y in range(3)]
    qg = [v + shift_q[x] for x, v in enumerate(apply(rot_q, points))]
    gg = apply(rot_q, cotan)
    parts = [qf[g] for g in range(3)]
    qgrad[...] = (scale * inner) * gather(parts, 0, 64)
    ones = []
    for p in parts:
        v = jnp.where((lane8 >= 112) & (lane8 % 4 == 0), p, 0.0)
        ones.append(v + pltpu.roll(v, 1, 1) + pltpu.roll(v, 2, 1) + pltpu.roll(v, 3, 1))
    ones = gather(ones, 112, PAD)
    dqg = [
        -2.0 * c48 * (qg[x] * ones - gather(parts, 64 + PAD * x, PAD)) for x in range(3)
    ]
    parts = [qf[3 + g] for g in range(3)]
    opt = [gather(parts, 32 * x, 32) - shift_q[x] for x in range(3)]
    for y, v in enumerate(undo(rot_q, dqg)):
        qpgrad[y] = v
    entries = []
    for x in range(3):
        for y in range(3):
            entries.append(add_all(dqg[x] * points[y]) + add_all(opt[x] * cotan[y]))
        entries.append(add_all(dqg[x]) - add_all(gg[x]))
    frame_out(qframe, entries)

    rot_k, shift_k = frames(cl * 256 + rw * 8)
    lanes = pl.ds(pl.multiple_of((rw // 16) * 128, 128), 128)
    points = local(kp, lanes, (rw % 16) * 8)
    vpoints = local(vp, lanes, (rw % 16) * 8)
    kg = [v + shift_k[x] for x, v in enumerate(apply(rot_k, points))]
    parts = [kf[g] for g in range(3)]
    kgrad[...] = (scale * inner) * gather(parts, 0, 64)
    ones = gather(parts, 112, PAD)
    dkg = [2.0 * c48 * (gather(parts, 64 + PAD * x, PAD) - kg[x] * ones) for x in range(3)]
    parts = [kf[3 + g] for g in range(4)]
    vgrad[...] = gather(parts, 0, 48)
    dvg = [gather(parts, 48 + 24 * x, 24) for x in range(3)]
    for y, v in enumerate(undo(rot_k, dkg)):
        kpgrad[y] = v
    for y, v in enumerate(undo(rot_k, dvg)):
        vpgrad[y] = v
    entries = []
    for x in range(3):
        for y in range(3):
            entries.append(add_all(dkg[x] * points[y]) + add_all(dvg[x] * vpoints[y]))
        entries.append(add_all(dkg[x]) + add_all(dvg[x]))
    frame_out(kframe, entries)
    copy.wait()


def per_device(
    pair_rep, bias_weight, head_weight, queries, key_vectors, values, query_points, key_points,
    value_points, rotations, translations, residue_count, grad_output, grad_points, grad_pair,
):
    channels, heads = bias_weight.shape
    width = queries.shape[0] // heads
    qpoints = query_points.shape[1] // heads
    n_rows = queries.shape[1]
    n_cols = key_vectors.shape[1]
    logit_scale = math.sqrt(1.0 / 3.0)
    point_scale = math.sqrt(2.0 / (9.0 * qpoints))
    inner_scale = 1.0 / math.sqrt(width)
    coef_scale = 0.5 * logit_scale * point_scale
    hw = head_weight.reshape(1, heads)
    gpt = grad_points.transpose(0, 2, 1)

    vm = pl.BlockSpec(memory_space=pltpu.VMEM)
    hbm = pl.BlockSpec(memory_space=pltpu.HBM)
    big = (heads, n_rows, n_cols)
    flat = (heads * n_rows, n_cols)
    dma = pltpu.SemaphoreType.DMA
    inputs = (
        bias_weight.T, hw, grad_pair.transpose(1, 0, 2), queries.T, key_vectors, values,
        query_points, key_points, value_points, rotations, translations, grad_output.T, gpt,
    )
    like = lambda x: pltpu.VMEM(x.shape, x.dtype)
    inputs = tuple(pltpu.with_memory_space_constraint(x, pltpu.HBM) for x in inputs)
    pg, kf, qf, wr = pl.pallas_call(
        functools.partial(
            mega_kernel, heads, n_rows, n_cols, logit_scale, inner_scale, coef_scale
        ),
        in_specs=[pl.BlockSpec(memory_space=pltpu.SMEM), *[hbm] * 14],
        out_specs=[vm] * 4,
        out_shape=[
            pltpu.VMEM(pair_rep.shape, BF16),
            jax.ShapeDtypeStruct((7, 8, 128), F32),
            jax.ShapeDtypeStruct((6, 8, 128), F32),
            jax.ShapeDtypeStruct((PAD, 128), F32),
        ],
        scratch_shapes=[
            *[like(x) for x in inputs],
            pltpu.VMEM(pair_rep.shape, BF16),
            pltpu.VMEM(big, F32),
            pltpu.VMEM(big, F32),
            *[pltpu.VMEM((n_rows * STRIDE, 128), F32)] * 4,
            *[pltpu.VMEM(flat, BF16)] * 4,
            pltpu.VMEM((n_rows * STRIDE, 128), F32),
            pltpu.VMEM((n_rows, 2 * PAD, 128), BF16),
            pltpu.VMEM((heads, 32, n_rows), F32),
            pltpu.VMEM((heads, 32, n_cols), F32),
            pltpu.VMEM((3, n_rows, 128), F32),
            pltpu.VMEM((n_rows, 2 * PAD, 128), F32),
            pltpu.VMEM((9, n_rows, 128), F32),
            pltpu.VMEM((32, 128), F32),
            pltpu.VMEM((32, 128), F32),
            pltpu.VMEM((32, 128), F32),
            pltpu.VMEM((3, 32, 128), F32),
            pltpu.VMEM((7, CORES, ZL * YN, 8, 128), F32),
            pltpu.VMEM((7, ZL * YN, 8, 128), F32),
            pltpu.VMEM((YN, 7, ZL, 8, 128), F32),
            pltpu.VMEM((YN - 1, 7, ZL, 8, 128), F32),
            pltpu.VMEM((ZL, 7, 8, 128), F32),
            pltpu.VMEM((ZL - 1, 7, 8, 128), F32),
            pltpu.VMEM((XN, ZH, 6, 8, 128), F32),
            pltpu.VMEM((XN - 1, ZH, 6, 8, 128), F32),
            pltpu.VMEM((ZH, 6, 8, 128), F32),
            pltpu.VMEM((6, 8, 128), F32),
            pltpu.VMEM((YN, PAD, 128), F32),
            pltpu.VMEM((XN * CORES, PAD, 128), F32),
            pltpu.VMEM((ZL * ZH, PAD, 128), F32),
            pltpu.VMEM((3, PAD, 128), F32),
            dma((4,)), dma((13,)),
            dma((4,)), dma((4,)),
            dma((7,)), dma((7,)),
            dma((3, 7)), dma((3, 7)),
            dma((3, 7)), dma((3, 7)),
            dma((4,)), dma((4,)),
            dma((17,)), dma((17,)),
        ],
        compiler_params=pltpu.CompilerParams(
            collective_id=0, has_side_effects=True, vmem_limit_bytes=VMEM_LIMIT
        ),
        name="mega",
    )(
        residue_count, pair_rep, *inputs
    )
    share = 8
    late = (hw, query_points, key_points, value_points, rotations, translations, gpt)
    f32 = lambda *shape: jax.ShapeDtypeStruct(shape, F32)
    outs = pl.pallas_call(
        functools.partial(
            finish_kernel, heads, n_rows, logit_scale, inner_scale, coef_scale
        ),
        in_specs=[vm] * 4 + [hbm] * 7,
        out_specs=[hbm] + [vm] * 10,
        out_shape=[
            jax.ShapeDtypeStruct(pair_rep.shape, BF16),
            f32(share, heads * width),
            f32(3, share, 48),
            f32(3, 4, share),
            f32(share, heads * width),
            f32(share, heads * width),
            f32(3, share, 48),
            f32(3, share, 96),
            f32(3, 4, share),
            f32(heads, channels),
            f32(1, heads),
        ],
        scratch_shapes=[*[like(x) for x in late], pltpu.VMEM((128, 128), F32), dma((7,)), dma],
        compiler_params=pltpu.CompilerParams(vmem_limit_bytes=VMEM_LIMIT),
        name="finish",
    )(pg, kf, qf, wr, *late)
    (pair_grad, qgrad, qpgrad, qframe, kgrad, vgrad, kpgrad, vpgrad, kframe, weight, head) = outs
    flip = lambda x: x.transpose(0, 2, 1)
    return (
        pair_grad, qgrad.T, flip(qpgrad), qframe, kgrad.T, vgrad.T, flip(kpgrad), flip(vpgrad),
        kframe, weight.T, head.reshape(heads),
    )


def solution(mesh):
    return jax.shard_map(
        per_device,
        mesh=mesh,
        in_specs=(
            P("row", "col", None),
            P(),
            P(),
            P(None, "row"),
            P(None, "col"),
            P(None, "col"),
            P(None, None, "row"),
            P(None, None, "col"),
            P(None, None, "col"),
            P(),
            P(),
            P(),
            P(None, "row"),
            P(None, None, "row"),
            P("row", None, None),
        ),
        out_specs=(
            P("row", "col", None),
            P(None, ("row", "col")),
            P(None, None, ("row", "col")),
            P(None, None, ("row", "col")),
            P(None, ("col", "row")),
            P(None, ("col", "row")),
            P(None, None, ("col", "row")),
            P(None, None, ("col", "row")),
            P(None, None, ("col", "row")),
            P(),
            P(),
        ),
        check_vma=False,
    )
```

```python
import functools
import math

import jax
import jax.numpy as jnp
from jax import lax
from jax.experimental import pallas as pl
from jax.experimental.pallas import tpu as pltpu
from jax.sharding import PartitionSpec as P

F32 = jnp.float32
BF16 = jnp.bfloat16
PAD = 16
VMEM_LIMIT = 50331648
ZL, YN, CORES = 4, 4, 2
XN, ZH = 4, 2
STRIDE = 40
MESH = pl.DeviceIdType.MESH


def dot(a, b, dims):
    return lax.dot_general(a, b, (dims, ((), ())), preferred_element_type=F32)


TN = ((0,), (0,))
NT = ((1,), (1,))
NN = ((1,), (0,))


def split2(x):
    hi = x.astype(BF16)
    return hi, (x - hi.astype(F32)).astype(BF16)


def split3(x):
    hi = x.astype(BF16)
    rest = x - hi.astype(F32)
    mid = rest.astype(BF16)
    return hi, mid, (rest - mid.astype(F32)).astype(BF16)


def lane_of(shape):
    return lax.broadcasted_iota(jnp.int32, shape, 1)


def merge_stats(parts):
    top = functools.reduce(jnp.maximum, parts)
    lane = lax.rem(lane_of(top.shape), 64)
    out = None
    for part in parts:
        f = jnp.exp(part - top)
        spread = jnp.where(lane < 2 * PAD, pltpu.roll(f, PAD, 1), pltpu.roll(f, 2 * PAD, 1))
        term = part * spread
        out = term if out is None else out + term
    return jnp.where(lane < PAD, top, out)


def push(src, dst, send, recv, row, col):
    copy = pltpu.make_async_remote_copy(
        src_ref=src, dst_ref=dst, send_sem=send, recv_sem=recv,
        device_id={"row": row, "col": col}, device_id_type=MESH,
    )
    copy.start()
    return copy


def group_mask(width, point, spread):
    row = lax.broadcasted_iota(jnp.int32, (128, 256), 0)
    lane = lane_of((128, 256))
    if width:
        body = (row - width * PAD) % (width * point)
        head = jnp.where(row < width * PAD, row // PAD, body // point)
    else:
        head = (row % 32) // point
    return head, lane // spread


def spread_heads(left, mask):
    left = jnp.concatenate([left, jnp.zeros_like(left)], 1)
    left = left + pltpu.roll(left, 64, 1)
    return jnp.where(mask, jnp.concatenate([left, left], 1), 0.0)


def soft(head_weight):
    return jnp.maximum(head_weight, 0.0) + jnp.log(1.0 + jnp.exp(-jnp.abs(head_weight)))


def mega_kernel(
    heads, n_rows, n_cols, scale, inner, coef_scale,
    rc, pair_hbm, *refs,
):
    sources, refs = refs[:13], refs[13:]
    pg_out, kf_out, qf_out, wr_out = refs[:4]
    staged, refs = refs[4:17], refs[17:]
    bw, hw, gp_t, qt, kt, vt, qp, kp, vp, rot, shift, got, gpt = staged
    (
    pair, lbase, dbase, fb0, fb1, rd0, rd1, a_hi, a_lo, d_hi, d_lo,
    wgf, wgb, qc, kc, wq, tt, qu, stat, stat_z, stat_m, stat_x,
    ks, ks_rx, sy, sy_rx, sz, sz_rx, qs, qs_rx, qz, qz_rx,
    ar_y, ar_x, ar_z, ar_s,
    pair_sem, in_sem, s_send, s_recv, k_send, k_recv, y_send, y_recv, z_send, z_recv,
    q_send, q_recv, a_send, a_recv,
    ) = refs
    rw = lax.axis_index("row")
    cl = lax.axis_index("col")
    core = lax.rem(rw, CORES)
    yy = lax.rem(rw // CORES, YN)
    zl = rw // (CORES * YN)
    zh = lax.rem(cl, ZH)
    xx = cl // ZH
    row_of = lambda z, y, c: (z * YN + y) * CORES + c
    sibling = (row_of(zl, yy, 1 - core), cl)
    y_peer = lambda k: (row_of(zl, lax.rem(yy + k, YN), core), cl)
    z_peer = lambda k: (row_of(lax.rem(zl + k, ZL), yy, core), cl)
    x_peer = lambda k: (rw, lax.rem(xx + k, XN) * ZH + zh)
    xc8 = xx * CORES + core

    def plane_peer(k):
        idx = lax.rem(xc8 + k, XN * CORES)
        return (row_of(zl, yy, lax.rem(idx, CORES)), (idx // CORES) * ZH + zh)

    h_peer = (rw, xx * ZH + 1 - zh)
    z8 = zh * ZL + zl

    def ring_peer(k):
        idx = lax.rem(z8 + k, ZL * ZH)
        return (row_of(lax.rem(idx, ZL), yy, core), xx * ZH + idx // ZL)

    incoming = []
    for n, (source, target) in enumerate(zip(sources, staged)):
        incoming.append(pltpu.make_async_copy(source, target, in_sem.at[n]))
    parts = 4
    rows_per = n_rows // parts
    loads = []
    for p in range(parts):
        piece = pl.ds(p * rows_per, rows_per)
        loads.append(pltpu.make_async_copy(pair_hbm.at[piece], pair.at[piece], pair_sem.at[p]))
    for n in (2, 0):
        incoming[n].start()
    loads[0].start()
    for n in (11, 3, 8, 7, 12, 9, 10, 4, 5, 6, 1):
        incoming[n].start()
    for p in range(1, parts):
        loads[p].start()
    everyone = [y_peer(k) for k in range(1, YN)]
    everyone += [plane_peer(k) for k in range(1, XN * CORES)]
    everyone += [ring_peer(k) for k in range(1, ZL * ZH)]
    barrier = pltpu.get_barrier_semaphore()
    for peer in everyone:
        pl.semaphore_signal(
            barrier, inc=1, device_id={"row": peer[0], "col": peer[1]}, device_id_type=MESH
        )

    wgf[...] = jnp.zeros_like(wgf)
    incoming[2].wait()
    incoming[0].wait()
    w_all = bw[...].astype(F32)
    w_t = jnp.concatenate([w_all, jnp.zeros((PAD - heads, 128), F32)], 0)
    for h in range(heads):
        wgf[pl.ds(PAD + h, n_rows, stride=STRIDE), :] = gp_t[h].astype(F32)
    w_bf = w_t.astype(BF16)
    for r in range(n_rows):
        wgb[r, :PAD, :] = w_bf
        wgb[r, PAD:, :] = wgf[r * STRIDE + PAD : r * STRIDE + 2 * PAD, :].astype(BF16)

    def bias_rows(p):
        loads[p].wait()
        zero = jnp.zeros((2 * PAD, 128), BF16)
        for i in range(0, rows_per, 2):
            r = p * rows_per + i
            left = jnp.concatenate(
                [
                    jnp.concatenate([wgb[r], zero], 1),
                    jnp.concatenate([zero, wgb[r + 1]], 1),
                ], 0
            )
            res = dot(left, jnp.concatenate([pair[r], pair[r + 1]], 1), NT)
            for n in range(2):
                rows = slice((r + n) * STRIDE, (r + n) * STRIDE + 2 * PAD)
                fb0[rows, :] = res[2 * PAD * n : 2 * PAD * n + 2 * PAD, :128]
                fb1[rows, :] = res[2 * PAD * n : 2 * PAD * n + 2 * PAD, 128:]

    for n in (11, 3, 8, 7, 12, 9, 10, 4, 5, 6, 1):
        incoming[n].wait()
    bias_rows(0)
    row_block = pl.multiple_of((rw // 2) * 128, 128)
    col_block = pl.multiple_of(cl * n_cols, 128)

    def row_vec(ref, *index):
        v = ref[index + (pl.ds(row_block, 128),)]
        return jnp.where(core == 1, pltpu.roll(v, 64, 1), v)[:, :n_rows]

    rot_q = [[row_vec(rot, x, pl.ds(y, 1)) for y in range(3)] for x in range(3)]
    rot_k = [
        [rot[x, pl.ds(y, 1), pl.ds(col_block, n_cols)] for y in range(3)] for x in range(3)
    ]
    apply = lambda m, p: [m[x][0] * p[0] + m[x][1] * p[1] + m[x][2] * p[2] for x in range(3)]
    add_shift = lambda g, t: [g[x] + t[x] for x in range(3)]
    qg = add_shift(
        apply(rot_q, [qp[y] for y in range(3)]),
        [row_vec(shift, pl.ds(x, 1)) for x in range(3)],
    )
    shift_k = [shift[pl.ds(x, 1), pl.ds(col_block, n_cols)] for x in range(3)]
    kg = add_shift(apply(rot_k, [kp[y] for y in range(3)]), shift_k)
    vg = add_shift(apply(rot_k, [vp[y] for y in range(3)]), shift_k)
    gg = apply(rot_q, [gpt[y].T for y in range(3)])
    tall = lambda ref: jnp.concatenate([ref[:, :128].T, ref[:, 128:].T], 0)
    q_all = tall(qt)
    g_all = tall(got)
    q_sq = qg[0] * qg[0] + qg[1] * qg[1] + qg[2] * qg[2]
    k_sq = kg[0] * kg[0] + kg[1] * kg[1] + kg[2] * kg[2]
    size = q_sq.shape[0]
    back = lambda x, n: pltpu.roll(x, size - n, 0)
    q_sq = q_sq + back(q_sq, 1) + back(q_sq, 2) + back(q_sq, 3)
    k_sq = k_sq + pltpu.roll(k_sq, 1, 0) + pltpu.roll(k_sq, 2, 0) + pltpu.roll(k_sq, 3, 0)
    coef = coef_scale * soft(hw[...])

    for h in range(heads):
        c = coef[:, h : h + 1]
        qc[h, :PAD, :] = (scale * inner) * q_all[PAD * h : PAD * h + PAD]
        kc[h, :PAD, :] = kt[PAD * h : PAD * h + PAD, :]
        for x in range(3):
            qc[h, PAD + 4 * x : PAD + 4 * x + 4, :] = (2.0 * c) * qg[x][4 * h : 4 * h + 4]
            kc[h, PAD + 4 * x : PAD + 4 * x + 4, :] = kg[x][4 * h : 4 * h + 4]
        qc[h, 28:29, :] = jnp.broadcast_to(-c, (1, n_rows))
        qc[h, 29:30, :] = -c * q_sq[4 * h : 4 * h + 1]
        qc[h, 30:32, :] = jnp.zeros((2, n_rows), F32)
        kc[h, 28:29, :] = k_sq[4 * h + 3 : 4 * h + 4]
        kc[h, 29:30, :] = jnp.ones((1, n_cols), F32)
        kc[h, 30:32, :] = jnp.zeros((2, n_cols), F32)

    def point_rows(head, points, h):
        body = [points[x][8 * h : 8 * h + 8] for x in range(3)]
        return jnp.concatenate([head] + body + [jnp.zeros_like(body[0])], 0)

    for h in range(heads):
        q0, q1, q2 = split3(qc[h])
        k0, k1, k2 = split3(kc[h])
        lbase[h] = dot(
            jnp.concatenate([q0, q0, q1, q0, q2, q1], 0),
            jnp.concatenate([k0, k1, k0, k2, k0, k1], 0),
            TN,
        )
        g0, g1 = split2(point_rows(g_all[PAD * h : PAD * h + PAD], gg, h))
        v0, v1 = split2(point_rows(vt[PAD * h : PAD * h + PAD, :], vg, h))
        dbase[h] = dot(
            jnp.concatenate([g0, g0, g1], 0), jnp.concatenate([v0, v1, v0], 0), TN
        )

    for p in range(1, parts):
        bias_rows(p)

    limit = rc[0] - cl * n_cols
    valid = lane_of((n_rows, n_cols)) < limit
    lane = lane_of((n_rows, 128))
    packed = jnp.ones((n_rows, 128), F32)
    picked = lambda ref0, ref1, h: jnp.concatenate(
        [ref0[pl.ds(h, n_rows, stride=STRIDE), :], ref1[pl.ds(h, n_rows, stride=STRIDE), :]], 1
    )
    for h in range(heads):
        logit = lbase[h] + scale * picked(fb0, fb1, h)
        logit = jnp.where(valid, logit, F32(-1000000000.0))
        peak = jnp.max(logit, axis=1, keepdims=True)
        e = jnp.exp(logit - peak)
        d = dbase[h] + picked(fb0, fb1, PAD + h)
        lbase[h] = e
        dbase[h] = d
        packed = jnp.where(lane == h, peak, packed)
        packed = jnp.where(lane == PAD + h, jnp.sum(e, axis=1, keepdims=True), packed)
        packed = jnp.where(lane == 2 * PAD + h, jnp.sum(e * d, axis=1, keepdims=True), packed)
    half = n_rows // 2
    own = jnp.where(lane[:half] < 64, packed[:half], pltpu.roll(packed[half:], 64, 1))
    stat[...] = own

    pl.semaphore_wait(barrier, len(everyone))
    sends = []
    sends.append(push(stat, stat_z, s_send.at[0], s_recv.at[0], *h_peer))

    rd0[...] = jnp.zeros_like(rd0)
    rd1[...] = jnp.zeros_like(rd1)
    key_head, lane64 = group_mask(4, 4, 64)
    key_mask = key_head == lane64
    val_head, _ = group_mask(3, 8, 64)
    val_mask = val_head == lane64
    sub16 = lax.broadcasted_iota(jnp.int32, (PAD, n_rows), 0) % 4
    sub16k = lax.broadcasted_iota(jnp.int32, (PAD, n_cols), 0) % 4
    qb, gb, kb, vb = [], [], [], []
    for g in range(3):
        pts = slice(PAD * g, PAD * g + PAD)
        base = jnp.concatenate(
            [q_all[64 * g : 64 * g + 64]] + [qg[x][pts] for x in range(3)]
            + [jnp.ones((PAD, n_rows), F32)], 0
        )
        qb.append(split2(spread_heads(base, key_mask)))
        weights = jnp.concatenate(
            [jnp.zeros((64, n_rows), F32)] + [-2.0 * qg[x][pts] for x in range(3)]
            + [jnp.where(sub16 == 0, q_sq[pts], jnp.where(sub16 == 3, 1.0, 0.0))], 0
        )
        wq[g] = weights.T
        base = jnp.concatenate(
            [kt[64 * g : 64 * g + 64, :]] + [kg[x][pts] for x in range(3)]
            + [jnp.where(sub16k == 3, k_sq[pts], jnp.where(sub16k == 0, 1.0, 0.0))], 0
        )
        kb.append(split2(base))
        oct_rows = slice(32 * g, 32 * g + 32)
        base = jnp.concatenate(
            [vg[x][oct_rows] for x in range(3)] + [jnp.zeros((32, n_cols), F32)], 0
        )
        vb.append(split2(base))
    for g in range(4):
        pts = slice(24 * g, 24 * g + 24)
        base = jnp.concatenate(
            [g_all[48 * g : 48 * g + 48]] + [gg[x][pts] for x in range(3)]
            + [jnp.zeros((8, n_rows), F32)], 0
        )
        gb.append(split2(spread_heads(base, val_mask)))
    query_masks = [key_head == k for k in range(4)]
    point_head, _ = group_mask(0, 8, 64)
    point_masks = [point_head == k for k in range(4)]

    def query_group(pairs, masks, hi, lo, first):
        blocks = lambda x: jnp.concatenate(
            [jnp.where(m, x, jnp.zeros_like(x)) for m in masks], 1
        )
        lefts = lambda ref: jnp.concatenate(
            [ref[pl.ds((first + k) * n_rows, n_rows)] for k in range(4)], 1
        )
        top = lefts(hi)
        res = dot(jnp.concatenate([top, lefts(lo)], 0), blocks(pairs[0]), NT)
        return res[:n_rows] + res[n_rows:] + dot(top, blocks(pairs[1]), NT)

    both_rows = lambda r: jnp.concatenate(
        [rd0[r * STRIDE : r * STRIDE + 2 * PAD, :], rd1[r * STRIDE : r * STRIDE + 2 * PAD, :]], 1
    )
    nearby = pltpu.roll(packed, 128 - 2 * PAD, 1) / pltpu.roll(packed, 128 - PAD, 1)
    for h in range(heads):
        e = lbase[h]
        d = dbase[h] - nearby[:, h : h + 1]
        dbase[h] = d
        both = e * d
        rows = pl.ds(h * n_rows, n_rows)
        a_hi[rows], a_lo[rows] = split2(e)
        d_hi[rows], d_lo[rows] = split2(both)
        rd0[pl.ds(h, n_rows, stride=STRIDE), :] = both[:, :128]
        rd1[pl.ds(h, n_rows, stride=STRIDE), :] = both[:, 128:]
        rd0[pl.ds(PAD + h, n_rows, stride=STRIDE), :] = e[:, :128]
        rd1[pl.ds(PAD + h, n_rows, stride=STRIDE), :] = e[:, 128:]
    for g in range(3):
        qu[g] = query_group(kb[g], query_masks, d_hi, d_lo, 4 * g)
        qu[3 + g] = query_group(kb[g], query_masks, a_hi, a_lo, 4 * g)
        qu[6 + g] = query_group(vb[g], point_masks, a_hi, a_lo, 4 * g)
    for r in range(n_rows):
        res = dot(jnp.concatenate(split2(both_rows(r)), 0), pair[r], NN)
        tt[r] = res[: 2 * PAD] + res[2 * PAD :]

    def landed(dst, send, recv, peer):
        pltpu.make_async_remote_copy(
            src_ref=dst, dst_ref=dst, send_sem=send, recv_sem=recv,
            device_id={"row": peer[0], "col": peer[1]}, device_id_type=MESH,
        ).wait_recv()

    landed(stat_z, s_send.at[0], s_recv.at[0], h_peer)
    pairwise = merge_stats([stat[...], stat_z[...]])
    stat_m[...] = pairwise
    for k in range(1, XN):
        sends.append(
            push(stat_m, stat_x.at[k - 1], s_send.at[k], s_recv.at[k], *x_peer(k))
        )
    for k in range(1, XN):
        landed(stat_x.at[k - 1], s_send.at[k], s_recv.at[k], x_peer(k))
    total = merge_stats([stat_m[...]] + [stat_x[k] for k in range(XN - 1)])
    mass = pltpu.roll(total, 128 - PAD, 1)
    factor = jnp.exp(stat[...] - total) / mass
    delta = pltpu.roll(total, 128 - 2 * PAD, 1) / mass
    factor = jnp.concatenate([factor, pltpu.roll(factor, 64, 1)], 0)
    delta = jnp.concatenate([delta, pltpu.roll(delta, 64, 1)], 0)

    def share(n, slots, place, count, peer, first):
        for k in range(1, count):
            sends.append(
                push(
                    ar_s.at[n], slots.at[place], a_send.at[first + k], a_recv.at[first + k],
                    *peer(k)
                )
            )

    def collect(slots, place, count, peer, first):
        for k in range(1, count):
            landed(
                slots.at[lax.rem(place + count - k, count)], a_send.at[first + k],
                a_recv.at[first + k], peer(k)
            )
        grand = slots[0]
        for k in range(1, count):
            grand = grand + slots[k]
        return grand

    moved = nearby - delta
    row_factor = jnp.concatenate([factor, jnp.zeros_like(factor)], 0).T[:PAD]
    row_moved = jnp.concatenate([moved[:, :PAD], jnp.zeros((n_rows, 128 - PAD), F32)], 1)
    row_moved = jnp.concatenate([row_moved, jnp.zeros_like(row_moved)], 0).T[:PAD]
    acc = jnp.zeros((PAD, 128), F32)
    for r in range(n_rows):
        term = tt[r, :PAD, :] + row_moved[:, r : r + 1] * tt[r, PAD:, :]
        acc = acc + row_factor[:, r : r + 1] * term
    lane_key = jnp.where(lane < 64, lane // PAD, (lane % PAD) // 4)
    lane_point = (lane % 32) // 8

    def spread(x, g, owner):
        out = jnp.broadcast_to(x[:, 4 * g : 4 * g + 1], (n_rows, 128))
        for k in range(1, 4):
            out = jnp.where(owner == k, x[:, 4 * g + k : 4 * g + k + 1], out)
        return out

    distance, q_results = [], []
    for g in range(3):
        res = spread(factor, g, lane_key) * (qu[g] + spread(moved, g, lane_key) * qu[3 + g])
        distance.append(jnp.sum(res * wq[g], axis=0, keepdims=True))
        q_results.append(res)
    acc = scale * acc
    sub = lax.broadcasted_iota(jnp.int32, (PAD, 128), 0)
    lane1 = lane_of((1, 128))
    owner = jnp.where(lane1 < 112, (lane1 % PAD) // 4, (lane1 - 112) // 4)
    dist_row = jnp.zeros((1, 128), F32)
    for h in range(heads):
        part = jnp.sum(jnp.where(owner == h % 4, distance[h // 4], 0.0), axis=1, keepdims=True)
        dist_row = jnp.where(lane1 == h, part, dist_row)
    acc = jnp.where(sub == heads, dist_row, acc)
    ar_s[0] = acc
    ar_z[z8] = acc

    share(0, ar_z, z8, ZL * ZH, ring_peer, -1)

    def make_head(h):
        att = lbase[h] * factor[:, h : h + 1]
        dl = att * (dbase[h] + moved[:, h : h + 1])
        rows = pl.ds(h * n_rows, n_rows)
        a_hi[rows], a_lo[rows] = split2(att)
        d_hi[rows], d_lo[rows] = split2(dl)
        rd0[pl.ds(h, n_rows, stride=STRIDE), :] = dl[:, :128]
        rd1[pl.ds(h, n_rows, stride=STRIDE), :] = dl[:, 128:]
        rd0[pl.ds(PAD + h, n_rows, stride=STRIDE), :] = att[:, :128]
        rd1[pl.ds(PAD + h, n_rows, stride=STRIDE), :] = att[:, 128:]

    def key_group(g, pairs, hi, lo, first, count):
        depth = count * n_rows
        rows = pl.ds(first * n_rows, depth)
        left, small = pairs[0][:, :depth], pairs[1][:, :depth]
        res = dot(jnp.concatenate([left, small], 0), hi[rows], NN)
        res = res[:128] + res[128:] + dot(left, lo[rows], NN)
        flat = res.T.reshape(ZL * YN, CORES, 8, 128)
        for c in range(CORES):
            ks[g, c] = flat[:, c]
        sends.append(
            push(ks.at[g, 1 - core], ks_rx.at[g], k_send.at[g], k_recv.at[g], *sibling)
        )

    z_first = (0, 3)

    def order(g):
        first, second = (y_peer, yy), (z_peer, zl)
        return (second, first) if g in z_first else (first, second)

    def y_stage(g):
        landed(ks_rx.at[g], k_send.at[g], k_recv.at[g], sibling)
        both = (ks[g, core] + ks_rx[g]).reshape(ZL, YN, 8, 128)
        peer, place = order(g)[0]
        for n in range(YN):
            sy[n, g] = both[n] if g in z_first else both[:, n]
        for k in range(1, YN):
            sends.append(
                push(
                    sy.at[lax.rem(place + k, YN), g], sy_rx.at[k - 1, g],
                    y_send.at[k - 1, g], y_recv.at[k - 1, g], *peer(k)
                )
            )

    def z_stage(g):
        (peer, place), (after, slot) = order(g)
        for k in range(1, YN):
            landed(sy_rx.at[k - 1, g], y_send.at[k - 1, g], y_recv.at[k - 1, g], peer(k))
        mine = sy[place, g] + sy_rx[0, g] + sy_rx[1, g] + sy_rx[2, g]
        for n in range(ZL):
            sz[n, g] = mine[n]
        for k in range(1, ZL):
            sends.append(
                push(
                    sz.at[lax.rem(slot + k, ZL), g], sz_rx.at[k - 1, g],
                    z_send.at[k - 1, g], z_recv.at[k - 1, g], *after(k)
                )
            )

    def last_stage(g):
        _, (peer, place) = order(g)
        for k in range(1, ZL):
            landed(sz_rx.at[k - 1, g], z_send.at[k - 1, g], z_recv.at[k - 1, g], peer(k))
        kf_out[g] = sz[place, g] + sz_rx[0, g] + sz_rx[1, g] + sz_rx[2, g]

    for h in range(4):
        make_head(h)
    key_group(0, qb[0], d_hi, d_lo, 0, 4)
    key_group(3, gb[0], a_hi, a_lo, 0, 3)
    for h in range(4, 8):
        make_head(h)
    key_group(1, qb[1], d_hi, d_lo, 4, 4)
    key_group(4, gb[1], a_hi, a_lo, 3, 3)
    for h in range(8, 12):
        make_head(h)
    key_group(2, qb[2], d_hi, d_lo, 8, 4)
    key_group(5, gb[2], a_hi, a_lo, 6, 3)
    key_group(6, gb[3], a_hi, a_lo, 9, 3)

    for g in (0, 3, 1, 4, 2, 5, 6):
        y_stage(g)
    for g in range(3):
        q_results.append(spread(factor, g, lane_point) * qu[6 + g])
    for g in range(6):
        flat = q_results[g].reshape(XN, ZH, 8, 128)
        for x in range(XN):
            for z in range(ZH):
                qs[x, z, g] = flat[x, z]
    for k in range(1, XN):
        sends.append(
            push(
                qs.at[lax.rem(xx + k, XN)], qs_rx.at[k - 1],
                q_send.at[k - 1], q_recv.at[k - 1], *x_peer(k)
            )
        )
    w_hi, w_lo = split2(scale * w_t)

    def pair_rows(first, count):
        for r in range(first, first + count):
            a = both_rows(r).astype(BF16)
            lhs = jnp.concatenate([a, a[:PAD]], 0)
            rhs = jnp.concatenate([w_hi, wgb[r, PAD:, :], w_lo], 0)
            pg_out[r] = dot(lhs, rhs, TN).astype(BF16)

    pair_rows(0, n_rows)
    grand = collect(ar_z, z8, ZL * ZH, ring_peer, -1)
    ar_s[1] = grand
    ar_x[xc8] = grand
    share(1, ar_x, xc8, XN * CORES, plane_peer, 6)
    z_stage(0)
    z_stage(3)
    for k in range(1, XN):
        landed(qs_rx.at[k - 1], q_send.at[k - 1], q_recv.at[k - 1], x_peer(k))
    qz[...] = qs[xx] + qs_rx[0] + qs_rx[1] + qs_rx[2]
    sends.append(push(qz.at[1 - zh], qz_rx, q_send.at[3], q_recv.at[3], *h_peer))
    z_stage(1)
    z_stage(4)
    z_stage(2)
    z_stage(5)
    grand = collect(ar_x, xc8, XN * CORES, plane_peer, 6)
    ar_s[2] = grand
    ar_y[yy] = grand
    share(2, ar_y, yy, YN, y_peer, 13)
    z_stage(6)
    landed(qz_rx, q_send.at[3], q_recv.at[3], h_peer)
    qf_out[...] = qz[zh] + qz_rx[...]
    for g in (0, 3, 1, 4, 2, 5, 6):
        last_stage(g)
    wr_out[...] = collect(ar_y, yy, YN, y_peer, 13)
    for copy in sends:
        copy.wait_send()


def finish_kernel(
    heads, n_rows, scale, inner, coef_scale,
    pg, kf, qf, wr, hw, qp, kp, vp, rot, shift, gpt,
    pg_out, qgrad, qpgrad, qframe, kgrad, vgrad, kpgrad, vpgrad, kframe, weight, head_out,
    turned, sem,
):
    copies = []
    for n in range(4):
        piece = pl.ds(n * (n_rows // 4), n_rows // 4)
        copies.append(pltpu.make_async_copy(pg.at[piece], pg_out.at[piece], sem.at[n]))
        copies[-1].start()
    rw = lax.axis_index("row")
    cl = lax.axis_index("col")
    weight[...] = wr[:heads, :]
    sig = 1.0 / (1.0 + jnp.exp(-hw[...]))
    head_out[...] = wr[heads : heads + 1, :heads] * (-coef_scale) * sig
    coef = coef_scale * soft(hw[...])

    def frames(start):
        block = pl.multiple_of((start // 128) * 128, 128)
        rows = [rot[x, pl.ds(y, 1), pl.ds(block, 128)] for x in range(3) for y in range(3)]
        rows += [shift[pl.ds(x, 1), pl.ds(block, 128)] for x in range(3)]
        rows = jnp.concatenate(rows + [jnp.zeros((4, 128), F32)], 0)
        turned[:, :PAD] = rows.T
        own = turned[pl.ds(pl.multiple_of(start % 128, 8), 8), :PAD]
        entry = lambda k: own[:, k : k + 1]
        return [[entry(3 * x + y) for y in range(3)] for x in range(3)], [
            entry(9 + x) for x in range(3)
        ]

    def local(ref, lanes, offset):
        out = []
        for y in range(3):
            x = ref[y] if lanes is None else ref[y, :, lanes]
            x = x.T
            turned[: x.shape[0], : x.shape[1]] = x
            out.append(turned[pl.ds(pl.multiple_of(offset, 8), 8), : x.shape[1]])
        return out

    apply = lambda m, p: [m[x][0] * p[0] + m[x][1] * p[1] + m[x][2] * p[2] for x in range(3)]
    undo = lambda m, v: [m[0][y] * v[0] + m[1][y] * v[1] + m[2][y] * v[2] for y in range(3)]
    add_all = lambda x: jnp.sum(x, axis=1, keepdims=True)
    lane8 = lane_of((8, 128))

    def gather(parts, offset, size):
        return jnp.concatenate([p[:, offset : offset + size] for p in parts], 1)

    c48 = jnp.zeros((1, 128), F32)
    lane1 = lane_of((1, 128))
    for h in range(heads):
        c48 = jnp.where(lane1 // 4 == h, coef[:, h : h + 1], c48)
    c48 = c48[:, :48]

    def frame_out(ref, entries):
        tile = jnp.zeros((8, 128), F32)
        for k, value in enumerate(entries):
            tile = jnp.where(lane8 == k, value, tile)
        tile = tile.T
        for x in range(3):
            ref[x] = tile[4 * x : 4 * x + 4, :]

    rot_q, shift_q = frames(rw * n_rows + cl * 8)
    points = local(qp, None, cl * 8)
    cotan = [gpt[y, pl.ds(pl.multiple_of(cl * 8, 8), 8), :] for y in range(3)]
    qg = [v + shift_q[x] for x, v in enumerate(apply(rot_q, points))]
    gg = apply(rot_q, cotan)
    parts = [qf[g] for g in range(3)]
    qgrad[...] = (scale * inner) * gather(parts, 0, 64)
    ones = []
    for p in parts:
        v = jnp.where((lane8 >= 112) & (lane8 % 4 == 0), p, 0.0)
        ones.append(v + pltpu.roll(v, 1, 1) + pltpu.roll(v, 2, 1) + pltpu.roll(v, 3, 1))
    ones = gather(ones, 112, PAD)
    dqg = [
        -2.0 * c48 * (qg[x] * ones - gather(parts, 64 + PAD * x, PAD)) for x in range(3)
    ]
    parts = [qf[3 + g] for g in range(3)]
    opt = [gather(parts, 32 * x, 32) - shift_q[x] for x in range(3)]
    for y, v in enumerate(undo(rot_q, dqg)):
        qpgrad[y] = v
    entries = []
    for x in range(3):
        for y in range(3):
            entries.append(add_all(dqg[x] * points[y]) + add_all(opt[x] * cotan[y]))
        entries.append(add_all(dqg[x]) - add_all(gg[x]))
    frame_out(qframe, entries)

    rot_k, shift_k = frames(cl * 256 + rw * 8)
    lanes = pl.ds(pl.multiple_of((rw // 16) * 128, 128), 128)
    points = local(kp, lanes, (rw % 16) * 8)
    vpoints = local(vp, lanes, (rw % 16) * 8)
    kg = [v + shift_k[x] for x, v in enumerate(apply(rot_k, points))]
    parts = [kf[g] for g in range(3)]
    kgrad[...] = (scale * inner) * gather(parts, 0, 64)
    ones = gather(parts, 112, PAD)
    dkg = [2.0 * c48 * (gather(parts, 64 + PAD * x, PAD) - kg[x] * ones) for x in range(3)]
    parts = [kf[3 + g] for g in range(4)]
    vgrad[...] = gather(parts, 0, 48)
    dvg = [gather(parts, 48 + 24 * x, 24) for x in range(3)]
    for y, v in enumerate(undo(rot_k, dkg)):
        kpgrad[y] = v
    for y, v in enumerate(undo(rot_k, dvg)):
        vpgrad[y] = v
    entries = []
    for x in range(3):
        for y in range(3):
            entries.append(add_all(dkg[x] * points[y]) + add_all(dvg[x] * vpoints[y]))
        entries.append(add_all(dkg[x]) + add_all(dvg[x]))
    frame_out(kframe, entries)
    for copy in copies:
        copy.wait()


def per_device(
    pair_rep, bias_weight, head_weight, queries, key_vectors, values, query_points, key_points,
    value_points, rotations, translations, residue_count, grad_output, grad_points, grad_pair,
):
    channels, heads = bias_weight.shape
    width = queries.shape[0] // heads
    qpoints = query_points.shape[1] // heads
    n_rows = queries.shape[1]
    n_cols = key_vectors.shape[1]
    logit_scale = math.sqrt(1.0 / 3.0)
    point_scale = math.sqrt(2.0 / (9.0 * qpoints))
    inner_scale = 1.0 / math.sqrt(width)
    coef_scale = 0.5 * logit_scale * point_scale
    hw = head_weight.reshape(1, heads)
    gpt = grad_points.transpose(0, 2, 1)

    vm = pl.BlockSpec(memory_space=pltpu.VMEM)
    hbm = pl.BlockSpec(memory_space=pltpu.HBM)
    big = (heads, n_rows, n_cols)
    flat = (heads * n_rows, n_cols)
    dma = pltpu.SemaphoreType.DMA
    inputs = (
        bias_weight.T, hw, grad_pair.transpose(1, 0, 2), queries.T, key_vectors, values,
        query_points, key_points, value_points, rotations, translations, grad_output.T, gpt,
    )
    like = lambda x: pltpu.VMEM(x.shape, x.dtype)
    inputs = tuple(pltpu.with_memory_space_constraint(x, pltpu.HBM) for x in inputs)
    pg, kf, qf, wr = pl.pallas_call(
        functools.partial(
            mega_kernel, heads, n_rows, n_cols, logit_scale, inner_scale, coef_scale
        ),
        in_specs=[pl.BlockSpec(memory_space=pltpu.SMEM), *[hbm] * 14],
        out_specs=[vm] * 4,
        out_shape=[
            pltpu.VMEM(pair_rep.shape, BF16),
            jax.ShapeDtypeStruct((7, 8, 128), F32),
            jax.ShapeDtypeStruct((6, 8, 128), F32),
            jax.ShapeDtypeStruct((PAD, 128), F32),
        ],
        scratch_shapes=[
            *[like(x) for x in inputs],
            pltpu.VMEM(pair_rep.shape, BF16),
            pltpu.VMEM(big, F32),
            pltpu.VMEM(big, F32),
            *[pltpu.VMEM((n_rows * STRIDE, 128), F32)] * 4,
            *[pltpu.VMEM(flat, BF16)] * 4,
            pltpu.VMEM((n_rows * STRIDE, 128), F32),
            pltpu.VMEM((n_rows, 2 * PAD, 128), BF16),
            pltpu.VMEM((heads, 32, n_rows), F32),
            pltpu.VMEM((heads, 32, n_cols), F32),
            pltpu.VMEM((3, n_rows, 128), F32),
            pltpu.VMEM((n_rows, 2 * PAD, 128), F32),
            pltpu.VMEM((9, n_rows, 128), F32),
            pltpu.VMEM((32, 128), F32),
            pltpu.VMEM((32, 128), F32),
            pltpu.VMEM((32, 128), F32),
            pltpu.VMEM((3, 32, 128), F32),
            pltpu.VMEM((7, CORES, ZL * YN, 8, 128), F32),
            pltpu.VMEM((7, ZL * YN, 8, 128), F32),
            pltpu.VMEM((YN, 7, ZL, 8, 128), F32),
            pltpu.VMEM((YN - 1, 7, ZL, 8, 128), F32),
            pltpu.VMEM((ZL, 7, 8, 128), F32),
            pltpu.VMEM((ZL - 1, 7, 8, 128), F32),
            pltpu.VMEM((XN, ZH, 6, 8, 128), F32),
            pltpu.VMEM((XN - 1, ZH, 6, 8, 128), F32),
            pltpu.VMEM((ZH, 6, 8, 128), F32),
            pltpu.VMEM((6, 8, 128), F32),
            pltpu.VMEM((YN, PAD, 128), F32),
            pltpu.VMEM((XN * CORES, PAD, 128), F32),
            pltpu.VMEM((ZL * ZH, PAD, 128), F32),
            pltpu.VMEM((3, PAD, 128), F32),
            dma((4,)), dma((13,)),
            dma((4,)), dma((4,)),
            dma((7,)), dma((7,)),
            dma((3, 7)), dma((3, 7)),
            dma((3, 7)), dma((3, 7)),
            dma((4,)), dma((4,)),
            dma((17,)), dma((17,)),
        ],
        compiler_params=pltpu.CompilerParams(
            collective_id=0, has_side_effects=True, vmem_limit_bytes=VMEM_LIMIT
        ),
        name="mega",
    )(
        residue_count, pair_rep, *inputs
    )
    share = 8
    late = (hw, query_points, key_points, value_points, rotations, translations, gpt)
    f32 = lambda *shape: jax.ShapeDtypeStruct(shape, F32)
    outs = pl.pallas_call(
        functools.partial(
            finish_kernel, heads, n_rows, logit_scale, inner_scale, coef_scale
        ),
        in_specs=[vm] * 11,
        out_specs=[hbm] + [vm] * 10,
        out_shape=[
            jax.ShapeDtypeStruct(pair_rep.shape, BF16),
            f32(share, heads * width),
            f32(3, share, 48),
            f32(3, 4, share),
            f32(share, heads * width),
            f32(share, heads * width),
            f32(3, share, 48),
            f32(3, share, 96),
            f32(3, 4, share),
            f32(heads, channels),
            f32(1, heads),
        ],
        scratch_shapes=[pltpu.VMEM((128, 128), F32), dma((4,))],
        compiler_params=pltpu.CompilerParams(vmem_limit_bytes=VMEM_LIMIT),
        name="finish",
    )(pg, kf, qf, wr, *late)
    (pair_grad, qgrad, qpgrad, qframe, kgrad, vgrad, kpgrad, vpgrad, kframe, weight, head) = outs
    flip = lambda x: x.transpose(0, 2, 1)
    return (
        pair_grad, qgrad.T, flip(qpgrad), qframe, kgrad.T, vgrad.T, flip(kpgrad), flip(vpgrad),
        kframe, weight.T, head.reshape(heads),
    )


def solution(mesh):
    return jax.shard_map(
        per_device,
        mesh=mesh,
        in_specs=(
            P("row", "col", None),
            P(),
            P(),
            P(None, "row"),
            P(None, "col"),
            P(None, "col"),
            P(None, None, "row"),
            P(None, None, "col"),
            P(None, None, "col"),
            P(),
            P(),
            P(),
            P(None, "row"),
            P(None, None, "row"),
            P("row", None, None),
        ),
        out_specs=(
            P("row", "col", None),
            P(None, ("row", "col")),
            P(None, None, ("row", "col")),
            P(None, None, ("row", "col")),
            P(None, ("col", "row")),
            P(None, ("col", "row")),
            P(None, None, ("col", "row")),
            P(None, None, ("col", "row")),
            P(None, None, ("col", "row")),
            P(),
            P(),
        ),
        check_vma=False,
    )
```

```python
import functools
import math

import jax
import jax.numpy as jnp
from jax import lax
from jax.experimental import pallas as pl
from jax.experimental.pallas import tpu as pltpu
from jax.sharding import PartitionSpec as P

F32 = jnp.float32
BF16 = jnp.bfloat16
PAD = 16
VMEM_LIMIT = 50331648
ZL, YN, CORES = 4, 4, 2
XN, ZH = 4, 2
STRIDE = 40
MESH = pl.DeviceIdType.MESH


def dot(a, b, dims):
    return lax.dot_general(a, b, (dims, ((), ())), preferred_element_type=F32)


TN = ((0,), (0,))
NT = ((1,), (1,))
NN = ((1,), (0,))


def split2(x):
    hi = x.astype(BF16)
    return hi, (x - hi.astype(F32)).astype(BF16)


def split3(x):
    hi = x.astype(BF16)
    rest = x - hi.astype(F32)
    mid = rest.astype(BF16)
    return hi, mid, (rest - mid.astype(F32)).astype(BF16)


def lane_of(shape):
    return lax.broadcasted_iota(jnp.int32, shape, 1)


def merge_stats(parts):
    top = functools.reduce(jnp.maximum, parts)
    lane = lax.rem(lane_of(top.shape), 64)
    out = None
    for part in parts:
        f = jnp.exp(part - top)
        spread = jnp.where(lane < 2 * PAD, pltpu.roll(f, PAD, 1), pltpu.roll(f, 2 * PAD, 1))
        term = part * spread
        out = term if out is None else out + term
    return jnp.where(lane < PAD, top, out)


def push(src, dst, send, recv, row, col):
    copy = pltpu.make_async_remote_copy(
        src_ref=src, dst_ref=dst, send_sem=send, recv_sem=recv,
        device_id={"row": row, "col": col}, device_id_type=MESH,
    )
    copy.start()
    return copy


def group_mask(width, point, spread):
    row = lax.broadcasted_iota(jnp.int32, (128, 256), 0)
    lane = lane_of((128, 256))
    if width:
        body = (row - width * PAD) % (width * point)
        head = jnp.where(row < width * PAD, row // PAD, body // point)
    else:
        head = (row % 32) // point
    return head, lane // spread


def spread_heads(left, mask):
    left = jnp.concatenate([left, jnp.zeros_like(left)], 1)
    left = left + pltpu.roll(left, 64, 1)
    return jnp.where(mask, jnp.concatenate([left, left], 1), 0.0)


def soft(head_weight):
    return jnp.maximum(head_weight, 0.0) + jnp.log(1.0 + jnp.exp(-jnp.abs(head_weight)))


def mega_kernel(
    heads, n_rows, n_cols, scale, inner, coef_scale,
    pair_hbm, *refs,
):
    sources, refs = refs[:14], refs[14:]
    pg_out, kf_out, qf_out, wr_out = refs[:4]
    staged, refs = refs[4:18], refs[18:]
    bw, hw, gp_t, qt, kt, vt, qp, kp, vp, rot, shift, got, gpt, rc = staged
    (
    pair, lbase, dbase, fb0, fb1, rd0, rd1, a_hi, a_lo, d_hi, d_lo,
    wgf, wgb, qc, kc, wq, tt, qu, stat, stat_z, stat_m, stat_x,
    ks, ks_rx, sy, sy_rx, sz, sz_rx, qs, qs_rx, qz, qz_rx,
    ar_y, ar_x, ar_z, ar_s,
    pair_sem, in_sem, s_send, s_recv, k_send, k_recv, y_send, y_recv, z_send, z_recv,
    q_send, q_recv, a_send, a_recv,
    ) = refs
    rw = lax.axis_index("row")
    cl = lax.axis_index("col")
    core = lax.rem(rw, CORES)
    yy = lax.rem(rw // CORES, YN)
    zl = rw // (CORES * YN)
    zh = lax.rem(cl, ZH)
    xx = cl // ZH
    row_of = lambda z, y, c: (z * YN + y) * CORES + c
    sibling = (row_of(zl, yy, 1 - core), cl)
    y_peer = lambda k: (row_of(zl, lax.rem(yy + k, YN), core), cl)
    z_peer = lambda k: (row_of(lax.rem(zl + k, ZL), yy, core), cl)
    x_peer = lambda k: (rw, lax.rem(xx + k, XN) * ZH + zh)
    xc8 = xx * CORES + core

    def plane_peer(k):
        idx = lax.rem(xc8 + k, XN * CORES)
        return (row_of(zl, yy, lax.rem(idx, CORES)), (idx // CORES) * ZH + zh)

    h_peer = (rw, xx * ZH + 1 - zh)
    z8 = zh * ZL + zl

    def ring_peer(k):
        idx = lax.rem(z8 + k, ZL * ZH)
        return (row_of(lax.rem(idx, ZL), yy, core), xx * ZH + idx // ZL)

    incoming = []
    for n, (source, target) in enumerate(zip(sources, staged)):
        incoming.append(pltpu.make_async_copy(source, target, in_sem.at[n]))
    parts = 4
    rows_per = n_rows // parts
    loads = []
    for p in range(parts):
        piece = pl.ds(p * rows_per, rows_per)
        loads.append(pltpu.make_async_copy(pair_hbm.at[piece], pair.at[piece], pair_sem.at[p]))
    for n in (2, 0):
        incoming[n].start()
    loads[0].start()
    for n in (11, 3, 8, 7, 12, 9, 10, 4, 5, 6, 1, 13):
        incoming[n].start()
    for p in range(1, parts):
        loads[p].start()
    everyone = [y_peer(k) for k in range(1, YN)]
    everyone += [plane_peer(k) for k in range(1, XN * CORES)]
    everyone += [ring_peer(k) for k in range(1, ZL * ZH)]
    barrier = pltpu.get_barrier_semaphore()
    for peer in everyone:
        pl.semaphore_signal(
            barrier, inc=1, device_id={"row": peer[0], "col": peer[1]}, device_id_type=MESH
        )

    wgf[...] = jnp.zeros_like(wgf)
    incoming[2].wait()
    incoming[0].wait()
    w_all = bw[...].astype(F32)
    w_t = jnp.concatenate([w_all, jnp.zeros((PAD - heads, 128), F32)], 0)
    for h in range(heads):
        wgf[pl.ds(PAD + h, n_rows, stride=STRIDE), :] = gp_t[h].astype(F32)
    w_bf = w_t.astype(BF16)
    for r in range(n_rows):
        wgb[r, :PAD, :] = w_bf
        wgb[r, PAD:, :] = wgf[r * STRIDE + PAD : r * STRIDE + 2 * PAD, :].astype(BF16)

    def bias_rows(p):
        loads[p].wait()
        zero = jnp.zeros((2 * PAD, 128), BF16)
        for i in range(0, rows_per, 2):
            r = p * rows_per + i
            left = jnp.concatenate(
                [
                    jnp.concatenate([wgb[r], zero], 1),
                    jnp.concatenate([zero, wgb[r + 1]], 1),
                ], 0
            )
            res = dot(left, jnp.concatenate([pair[r], pair[r + 1]], 1), NT)
            for n in range(2):
                rows = slice((r + n) * STRIDE, (r + n) * STRIDE + 2 * PAD)
                fb0[rows, :] = res[2 * PAD * n : 2 * PAD * n + 2 * PAD, :128]
                fb1[rows, :] = res[2 * PAD * n : 2 * PAD * n + 2 * PAD, 128:]

    for n in (11, 3, 8, 7, 12, 9, 10, 4, 5, 6, 1, 13):
        incoming[n].wait()
    bias_rows(0)
    row_block = pl.multiple_of((rw // 2) * 128, 128)
    col_block = pl.multiple_of(cl * n_cols, 128)

    def row_vec(ref, *index):
        v = ref[index + (pl.ds(row_block, 128),)]
        return jnp.where(core == 1, pltpu.roll(v, 64, 1), v)[:, :n_rows]

    rot_q = [[row_vec(rot, x, pl.ds(y, 1)) for y in range(3)] for x in range(3)]
    rot_k = [
        [rot[x, pl.ds(y, 1), pl.ds(col_block, n_cols)] for y in range(3)] for x in range(3)
    ]
    apply = lambda m, p: [m[x][0] * p[0] + m[x][1] * p[1] + m[x][2] * p[2] for x in range(3)]
    add_shift = lambda g, t: [g[x] + t[x] for x in range(3)]
    qg = add_shift(
        apply(rot_q, [qp[y] for y in range(3)]),
        [row_vec(shift, pl.ds(x, 1)) for x in range(3)],
    )
    shift_k = [shift[pl.ds(x, 1), pl.ds(col_block, n_cols)] for x in range(3)]
    kg = add_shift(apply(rot_k, [kp[y] for y in range(3)]), shift_k)
    vg = add_shift(apply(rot_k, [vp[y] for y in range(3)]), shift_k)
    gg = apply(rot_q, [gpt[y].T for y in range(3)])
    tall = lambda ref: jnp.concatenate([ref[:, :128].T, ref[:, 128:].T], 0)
    q_all = tall(qt)
    g_all = tall(got)
    q_sq = qg[0] * qg[0] + qg[1] * qg[1] + qg[2] * qg[2]
    k_sq = kg[0] * kg[0] + kg[1] * kg[1] + kg[2] * kg[2]
    size = q_sq.shape[0]
    back = lambda x, n: pltpu.roll(x, size - n, 0)
    q_sq = q_sq + back(q_sq, 1) + back(q_sq, 2) + back(q_sq, 3)
    k_sq = k_sq + pltpu.roll(k_sq, 1, 0) + pltpu.roll(k_sq, 2, 0) + pltpu.roll(k_sq, 3, 0)
    coef = coef_scale * soft(hw[...])

    for h in range(heads):
        c = coef[:, h : h + 1]
        qc[h, :PAD, :] = (scale * inner) * q_all[PAD * h : PAD * h + PAD]
        kc[h, :PAD, :] = kt[PAD * h : PAD * h + PAD, :]
        for x in range(3):
            qc[h, PAD + 4 * x : PAD + 4 * x + 4, :] = (2.0 * c) * qg[x][4 * h : 4 * h + 4]
            kc[h, PAD + 4 * x : PAD + 4 * x + 4, :] = kg[x][4 * h : 4 * h + 4]
        qc[h, 28:29, :] = jnp.broadcast_to(-c, (1, n_rows))
        qc[h, 29:30, :] = -c * q_sq[4 * h : 4 * h + 1]
        qc[h, 30:32, :] = jnp.zeros((2, n_rows), F32)
        kc[h, 28:29, :] = k_sq[4 * h + 3 : 4 * h + 4]
        kc[h, 29:30, :] = jnp.ones((1, n_cols), F32)
        kc[h, 30:32, :] = jnp.zeros((2, n_cols), F32)

    def point_rows(head, points, h):
        body = [points[x][8 * h : 8 * h + 8] for x in range(3)]
        return jnp.concatenate([head] + body + [jnp.zeros_like(body[0])], 0)

    for h in range(heads):
        q0, q1, q2 = split3(qc[h])
        k0, k1, k2 = split3(kc[h])
        lbase[h] = dot(
            jnp.concatenate([q0, q0, q1, q0, q2, q1], 0),
            jnp.concatenate([k0, k1, k0, k2, k0, k1], 0),
            TN,
        )
        g0, g1 = split2(point_rows(g_all[PAD * h : PAD * h + PAD], gg, h))
        v0, v1 = split2(point_rows(vt[PAD * h : PAD * h + PAD, :], vg, h))
        dbase[h] = dot(
            jnp.concatenate([g0, g0, g1], 0), jnp.concatenate([v0, v1, v0], 0), TN
        )

    for p in range(1, parts):
        bias_rows(p)

    limit = rc[...] - cl * n_cols
    valid = lane_of((n_rows, n_cols)) < limit
    lane = lane_of((n_rows, 128))
    packed = jnp.ones((n_rows, 128), F32)
    picked = lambda ref0, ref1, h: jnp.concatenate(
        [ref0[pl.ds(h, n_rows, stride=STRIDE), :], ref1[pl.ds(h, n_rows, stride=STRIDE), :]], 1
    )
    for h in range(heads):
        logit = lbase[h] + scale * picked(fb0, fb1, h)
        logit = jnp.where(valid, logit, F32(-1000000000.0))
        peak = jnp.max(logit, axis=1, keepdims=True)
        e = jnp.exp(logit - peak)
        d = dbase[h] + picked(fb0, fb1, PAD + h)
        lbase[h] = e
        dbase[h] = d
        packed = jnp.where(lane == h, peak, packed)
        packed = jnp.where(lane == PAD + h, jnp.sum(e, axis=1, keepdims=True), packed)
        packed = jnp.where(lane == 2 * PAD + h, jnp.sum(e * d, axis=1, keepdims=True), packed)
    half = n_rows // 2
    own = jnp.where(lane[:half] < 64, packed[:half], pltpu.roll(packed[half:], 64, 1))
    stat[...] = own

    pl.semaphore_wait(barrier, len(everyone))
    sends = []
    sends.append(push(stat, stat_z, s_send.at[0], s_recv.at[0], *h_peer))

    rd0[...] = jnp.zeros_like(rd0)
    rd1[...] = jnp.zeros_like(rd1)
    key_head, lane64 = group_mask(4, 4, 64)
    key_mask = key_head == lane64
    val_head, _ = group_mask(3, 8, 64)
    val_mask = val_head == lane64
    sub16 = lax.broadcasted_iota(jnp.int32, (PAD, n_rows), 0) % 4
    sub16k = lax.broadcasted_iota(jnp.int32, (PAD, n_cols), 0) % 4
    qb, gb, kb, vb = [], [], [], []
    for g in range(3):
        pts = slice(PAD * g, PAD * g + PAD)
        base = jnp.concatenate(
            [q_all[64 * g : 64 * g + 64]] + [qg[x][pts] for x in range(3)]
            + [jnp.ones((PAD, n_rows), F32)], 0
        )
        qb.append(split2(spread_heads(base, key_mask)))
        weights = jnp.concatenate(
            [jnp.zeros((64, n_rows), F32)] + [-2.0 * qg[x][pts] for x in range(3)]
            + [jnp.where(sub16 == 0, q_sq[pts], jnp.where(sub16 == 3, 1.0, 0.0))], 0
        )
        wq[g] = weights.T
        base = jnp.concatenate(
            [kt[64 * g : 64 * g + 64, :]] + [kg[x][pts] for x in range(3)]
            + [jnp.where(sub16k == 3, k_sq[pts], jnp.where(sub16k == 0, 1.0, 0.0))], 0
        )
        kb.append(split2(base))
        oct_rows = slice(32 * g, 32 * g + 32)
        base = jnp.concatenate(
            [vg[x][oct_rows] for x in range(3)] + [jnp.zeros((32, n_cols), F32)], 0
        )
        vb.append(split2(base))
    for g in range(4):
        pts = slice(24 * g, 24 * g + 24)
        base = jnp.concatenate(
            [g_all[48 * g : 48 * g + 48]] + [gg[x][pts] for x in range(3)]
            + [jnp.zeros((8, n_rows), F32)], 0
        )
        gb.append(split2(spread_heads(base, val_mask)))
    query_masks = [key_head == k for k in range(4)]
    point_head, _ = group_mask(0, 8, 64)
    point_masks = [point_head == k for k in range(4)]

    def query_group(pairs, masks, hi, lo, first):
        blocks = lambda x: jnp.concatenate(
            [jnp.where(m, x, jnp.zeros_like(x)) for m in masks], 1
        )
        lefts = lambda ref: jnp.concatenate(
            [ref[pl.ds((first + k) * n_rows, n_rows)] for k in range(4)], 1
        )
        top = lefts(hi)
        res = dot(jnp.concatenate([top, lefts(lo)], 0), blocks(pairs[0]), NT)
        return res[:n_rows] + res[n_rows:] + dot(top, blocks(pairs[1]), NT)

    both_rows = lambda r: jnp.concatenate(
        [rd0[r * STRIDE : r * STRIDE + 2 * PAD, :], rd1[r * STRIDE : r * STRIDE + 2 * PAD, :]], 1
    )
    nearby = pltpu.roll(packed, 128 - 2 * PAD, 1) / pltpu.roll(packed, 128 - PAD, 1)
    for h in range(heads):
        e = lbase[h]
        d = dbase[h] - nearby[:, h : h + 1]
        dbase[h] = d
        both = e * d
        rows = pl.ds(h * n_rows, n_rows)
        a_hi[rows], a_lo[rows] = split2(e)
        d_hi[rows], d_lo[rows] = split2(both)
        rd0[pl.ds(h, n_rows, stride=STRIDE), :] = both[:, :128]
        rd1[pl.ds(h, n_rows, stride=STRIDE), :] = both[:, 128:]
        rd0[pl.ds(PAD + h, n_rows, stride=STRIDE), :] = e[:, :128]
        rd1[pl.ds(PAD + h, n_rows, stride=STRIDE), :] = e[:, 128:]
    for g in range(3):
        qu[g] = query_group(kb[g], query_masks, d_hi, d_lo, 4 * g)
        qu[3 + g] = query_group(kb[g], query_masks, a_hi, a_lo, 4 * g)
        qu[6 + g] = query_group(vb[g], point_masks, a_hi, a_lo, 4 * g)
    for r in range(n_rows):
        res = dot(jnp.concatenate(split2(both_rows(r)), 0), pair[r], NN)
        tt[r] = res[: 2 * PAD] + res[2 * PAD :]

    def landed(dst, send, recv, peer):
        pltpu.make_async_remote_copy(
            src_ref=dst, dst_ref=dst, send_sem=send, recv_sem=recv,
            device_id={"row": peer[0], "col": peer[1]}, device_id_type=MESH,
        ).wait_recv()

    landed(stat_z, s_send.at[0], s_recv.at[0], h_peer)
    pairwise = merge_stats([stat[...], stat_z[...]])
    stat_m[...] = pairwise
    for k in range(1, XN):
        sends.append(
            push(stat_m, stat_x.at[k - 1], s_send.at[k], s_recv.at[k], *x_peer(k))
        )
    for k in range(1, XN):
        landed(stat_x.at[k - 1], s_send.at[k], s_recv.at[k], x_peer(k))
    total = merge_stats([stat_m[...]] + [stat_x[k] for k in range(XN - 1)])
    mass = pltpu.roll(total, 128 - PAD, 1)
    factor = jnp.exp(stat[...] - total) / mass
    delta = pltpu.roll(total, 128 - 2 * PAD, 1) / mass
    factor = jnp.concatenate([factor, pltpu.roll(factor, 64, 1)], 0)
    delta = jnp.concatenate([delta, pltpu.roll(delta, 64, 1)], 0)

    def share(n, slots, place, count, peer, first):
        for k in range(1, count):
            sends.append(
                push(
                    ar_s.at[n], slots.at[place], a_send.at[first + k], a_recv.at[first + k],
                    *peer(k)
                )
            )

    def collect(slots, place, count, peer, first):
        for k in range(1, count):
            landed(
                slots.at[lax.rem(place + count - k, count)], a_send.at[first + k],
                a_recv.at[first + k], peer(k)
            )
        grand = slots[0]
        for k in range(1, count):
            grand = grand + slots[k]
        return grand

    moved = nearby - delta
    row_factor = jnp.concatenate([factor, jnp.zeros_like(factor)], 0).T[:PAD]
    row_moved = jnp.concatenate([moved[:, :PAD], jnp.zeros((n_rows, 128 - PAD), F32)], 1)
    row_moved = jnp.concatenate([row_moved, jnp.zeros_like(row_moved)], 0).T[:PAD]
    acc = jnp.zeros((PAD, 128), F32)
    for r in range(n_rows):
        term = tt[r, :PAD, :] + row_moved[:, r : r + 1] * tt[r, PAD:, :]
        acc = acc + row_factor[:, r : r + 1] * term
    lane_key = jnp.where(lane < 64, lane // PAD, (lane % PAD) // 4)
    lane_point = (lane % 32) // 8

    def spread(x, g, owner):
        out = jnp.broadcast_to(x[:, 4 * g : 4 * g + 1], (n_rows, 128))
        for k in range(1, 4):
            out = jnp.where(owner == k, x[:, 4 * g + k : 4 * g + k + 1], out)
        return out

    distance, q_results = [], []
    for g in range(3):
        res = spread(factor, g, lane_key) * (qu[g] + spread(moved, g, lane_key) * qu[3 + g])
        distance.append(jnp.sum(res * wq[g], axis=0, keepdims=True))
        q_results.append(res)
    acc = scale * acc
    sub = lax.broadcasted_iota(jnp.int32, (PAD, 128), 0)
    lane1 = lane_of((1, 128))
    owner = jnp.where(lane1 < 112, (lane1 % PAD) // 4, (lane1 - 112) // 4)
    dist_row = jnp.zeros((1, 128), F32)
    for h in range(heads):
        part = jnp.sum(jnp.where(owner == h % 4, distance[h // 4], 0.0), axis=1, keepdims=True)
        dist_row = jnp.where(lane1 == h, part, dist_row)
    acc = jnp.where(sub == heads, dist_row, acc)
    ar_s[0] = acc
    ar_z[z8] = acc

    share(0, ar_z, z8, ZL * ZH, ring_peer, -1)

    def make_head(h):
        att = lbase[h] * factor[:, h : h + 1]
        dl = att * (dbase[h] + moved[:, h : h + 1])
        rows = pl.ds(h * n_rows, n_rows)
        a_hi[rows], a_lo[rows] = split2(att)
        d_hi[rows], d_lo[rows] = split2(dl)
        rd0[pl.ds(h, n_rows, stride=STRIDE), :] = dl[:, :128]
        rd1[pl.ds(h, n_rows, stride=STRIDE), :] = dl[:, 128:]
        rd0[pl.ds(PAD + h, n_rows, stride=STRIDE), :] = att[:, :128]
        rd1[pl.ds(PAD + h, n_rows, stride=STRIDE), :] = att[:, 128:]

    def key_group(g, pairs, hi, lo, first, count):
        depth = count * n_rows
        rows = pl.ds(first * n_rows, depth)
        left, small = pairs[0][:, :depth], pairs[1][:, :depth]
        res = dot(jnp.concatenate([left, small], 0), hi[rows], NN)
        res = res[:128] + res[128:] + dot(left, lo[rows], NN)
        flat = res.T.reshape(ZL * YN, CORES, 8, 128)
        for c in range(CORES):
            ks[g, c] = flat[:, c]
        sends.append(
            push(ks.at[g, 1 - core], ks_rx.at[g], k_send.at[g], k_recv.at[g], *sibling)
        )

    z_first = (0, 3)

    def order(g):
        first, second = (y_peer, yy), (z_peer, zl)
        return (second, first) if g in z_first else (first, second)

    def y_stage(g):
        landed(ks_rx.at[g], k_send.at[g], k_recv.at[g], sibling)
        both = (ks[g, core] + ks_rx[g]).reshape(ZL, YN, 8, 128)
        peer, place = order(g)[0]
        for n in range(YN):
            sy[n, g] = both[n] if g in z_first else both[:, n]
        for k in range(1, YN):
            sends.append(
                push(
                    sy.at[lax.rem(place + k, YN), g], sy_rx.at[k - 1, g],
                    y_send.at[k - 1, g], y_recv.at[k - 1, g], *peer(k)
                )
            )

    def z_stage(g):
        (peer, place), (after, slot) = order(g)
        for k in range(1, YN):
            landed(sy_rx.at[k - 1, g], y_send.at[k - 1, g], y_recv.at[k - 1, g], peer(k))
        mine = sy[place, g] + sy_rx[0, g] + sy_rx[1, g] + sy_rx[2, g]
        for n in range(ZL):
            sz[n, g] = mine[n]
        for k in range(1, ZL):
            sends.append(
                push(
                    sz.at[lax.rem(slot + k, ZL), g], sz_rx.at[k - 1, g],
                    z_send.at[k - 1, g], z_recv.at[k - 1, g], *after(k)
                )
            )

    def last_stage(g):
        _, (peer, place) = order(g)
        for k in range(1, ZL):
            landed(sz_rx.at[k - 1, g], z_send.at[k - 1, g], z_recv.at[k - 1, g], peer(k))
        kf_out[g] = sz[place, g] + sz_rx[0, g] + sz_rx[1, g] + sz_rx[2, g]

    for h in range(4):
        make_head(h)
    key_group(0, qb[0], d_hi, d_lo, 0, 4)
    key_group(3, gb[0], a_hi, a_lo, 0, 3)
    for h in range(4, 8):
        make_head(h)
    key_group(1, qb[1], d_hi, d_lo, 4, 4)
    key_group(4, gb[1], a_hi, a_lo, 3, 3)
    for h in range(8, 12):
        make_head(h)
    key_group(2, qb[2], d_hi, d_lo, 8, 4)
    key_group(5, gb[2], a_hi, a_lo, 6, 3)
    key_group(6, gb[3], a_hi, a_lo, 9, 3)

    for g in (0, 3, 1, 4, 2, 5, 6):
        y_stage(g)
    for g in range(3):
        q_results.append(spread(factor, g, lane_point) * qu[6 + g])
    for g in range(6):
        flat = q_results[g].reshape(XN, ZH, 8, 128)
        for x in range(XN):
            for z in range(ZH):
                qs[x, z, g] = flat[x, z]
    for k in range(1, XN):
        sends.append(
            push(
                qs.at[lax.rem(xx + k, XN)], qs_rx.at[k - 1],
                q_send.at[k - 1], q_recv.at[k - 1], *x_peer(k)
            )
        )
    w_hi, w_lo = split2(scale * w_t)

    def pair_rows(first, count):
        for r in range(first, first + count):
            a = both_rows(r).astype(BF16)
            lhs = jnp.concatenate([a, a[:PAD]], 0)
            rhs = jnp.concatenate([w_hi, wgb[r, PAD:, :], w_lo], 0)
            pg_out[r] = dot(lhs, rhs, TN).astype(BF16)

    pair_rows(0, n_rows)
    grand = collect(ar_z, z8, ZL * ZH, ring_peer, -1)
    ar_s[1] = grand
    ar_x[xc8] = grand
    share(1, ar_x, xc8, XN * CORES, plane_peer, 6)
    z_stage(0)
    z_stage(3)
    for k in range(1, XN):
        landed(qs_rx.at[k - 1], q_send.at[k - 1], q_recv.at[k - 1], x_peer(k))
    qz[...] = qs[xx] + qs_rx[0] + qs_rx[1] + qs_rx[2]
    sends.append(push(qz.at[1 - zh], qz_rx, q_send.at[3], q_recv.at[3], *h_peer))
    z_stage(1)
    z_stage(4)
    z_stage(2)
    z_stage(5)
    grand = collect(ar_x, xc8, XN * CORES, plane_peer, 6)
    ar_s[2] = grand
    ar_y[yy] = grand
    share(2, ar_y, yy, YN, y_peer, 13)
    z_stage(6)
    landed(qz_rx, q_send.at[3], q_recv.at[3], h_peer)
    qf_out[...] = qz[zh] + qz_rx[...]
    for g in (0, 3, 1, 4, 2, 5, 6):
        last_stage(g)
    wr_out[...] = collect(ar_y, yy, YN, y_peer, 13)
    for copy in sends:
        copy.wait_send()


def finish_kernel(
    heads, n_rows, scale, inner, coef_scale,
    pg, kf, qf, wr, hw, qp, kp, vp, rot, shift, gpt,
    pg_out, qgrad, qpgrad, qframe, kgrad, vgrad, kpgrad, vpgrad, kframe, weight, head_out,
    turned, sem,
):
    copies = []
    for n in range(4):
        piece = pl.ds(n * (n_rows // 4), n_rows // 4)
        copies.append(pltpu.make_async_copy(pg.at[piece], pg_out.at[piece], sem.at[n]))
        copies[-1].start()
    rw = lax.axis_index("row")
    cl = lax.axis_index("col")
    weight[...] = wr[:heads, :]
    sig = 1.0 / (1.0 + jnp.exp(-hw[...]))
    head_out[...] = wr[heads : heads + 1, :heads] * (-coef_scale) * sig
    coef = coef_scale * soft(hw[...])

    def frames(start):
        block = pl.multiple_of((start // 128) * 128, 128)
        rows = [rot[x, pl.ds(y, 1), pl.ds(block, 128)] for x in range(3) for y in range(3)]
        rows += [shift[pl.ds(x, 1), pl.ds(block, 128)] for x in range(3)]
        rows = jnp.concatenate(rows + [jnp.zeros((4, 128), F32)], 0)
        turned[:, :PAD] = rows.T
        own = turned[pl.ds(pl.multiple_of(start % 128, 8), 8), :PAD]
        entry = lambda k: own[:, k : k + 1]
        return [[entry(3 * x + y) for y in range(3)] for x in range(3)], [
            entry(9 + x) for x in range(3)
        ]

    def local(ref, lanes, offset):
        out = []
        for y in range(3):
            x = ref[y] if lanes is None else ref[y, :, lanes]
            x = x.T
            turned[: x.shape[0], : x.shape[1]] = x
            out.append(turned[pl.ds(pl.multiple_of(offset, 8), 8), : x.shape[1]])
        return out

    apply = lambda m, p: [m[x][0] * p[0] + m[x][1] * p[1] + m[x][2] * p[2] for x in range(3)]
    undo = lambda m, v: [m[0][y] * v[0] + m[1][y] * v[1] + m[2][y] * v[2] for y in range(3)]
    add_all = lambda x: jnp.sum(x, axis=1, keepdims=True)
    lane8 = lane_of((8, 128))

    def gather(parts, offset, size):
        return jnp.concatenate([p[:, offset : offset + size] for p in parts], 1)

    c48 = jnp.zeros((1, 128), F32)
    lane1 = lane_of((1, 128))
    for h in range(heads):
        c48 = jnp.where(lane1 // 4 == h, coef[:, h : h + 1], c48)
    c48 = c48[:, :48]

    def frame_out(ref, entries):
        tile = jnp.zeros((8, 128), F32)
        for k, value in enumerate(entries):
            tile = jnp.where(lane8 == k, value, tile)
        tile = tile.T
        for x in range(3):
            ref[x] = tile[4 * x : 4 * x + 4, :]

    rot_q, shift_q = frames(rw * n_rows + cl * 8)
    points = local(qp, None, cl * 8)
    cotan = [gpt[y, pl.ds(pl.multiple_of(cl * 8, 8), 8), :] for y in range(3)]
    qg = [v + shift_q[x] for x, v in enumerate(apply(rot_q, points))]
    gg = apply(rot_q, cotan)
    parts = [qf[g] for g in range(3)]
    qgrad[...] = (scale * inner) * gather(parts, 0, 64)
    ones = []
    for p in parts:
        v = jnp.where((lane8 >= 112) & (lane8 % 4 == 0), p, 0.0)
        ones.append(v + pltpu.roll(v, 1, 1) + pltpu.roll(v, 2, 1) + pltpu.roll(v, 3, 1))
    ones = gather(ones, 112, PAD)
    dqg = [
        -2.0 * c48 * (qg[x] * ones - gather(parts, 64 + PAD * x, PAD)) for x in range(3)
    ]
    parts = [qf[3 + g] for g in range(3)]
    opt = [gather(parts, 32 * x, 32) - shift_q[x] for x in range(3)]
    for y, v in enumerate(undo(rot_q, dqg)):
        qpgrad[y] = v
    entries = []
    for x in range(3):
        for y in range(3):
            entries.append(add_all(dqg[x] * points[y]) + add_all(opt[x] * cotan[y]))
        entries.append(add_all(dqg[x]) - add_all(gg[x]))
    frame_out(qframe, entries)

    rot_k, shift_k = frames(cl * 256 + rw * 8)
    lanes = pl.ds(pl.multiple_of((rw // 16) * 128, 128), 128)
    points = local(kp, lanes, (rw % 16) * 8)
    vpoints = local(vp, lanes, (rw % 16) * 8)
    kg = [v + shift_k[x] for x, v in enumerate(apply(rot_k, points))]
    parts = [kf[g] for g in range(3)]
    kgrad[...] = (scale * inner) * gather(parts, 0, 64)
    ones = gather(parts, 112, PAD)
    dkg = [2.0 * c48 * (gather(parts, 64 + PAD * x, PAD) - kg[x] * ones) for x in range(3)]
    parts = [kf[3 + g] for g in range(4)]
    vgrad[...] = gather(parts, 0, 48)
    dvg = [gather(parts, 48 + 24 * x, 24) for x in range(3)]
    for y, v in enumerate(undo(rot_k, dkg)):
        kpgrad[y] = v
    for y, v in enumerate(undo(rot_k, dvg)):
        vpgrad[y] = v
    entries = []
    for x in range(3):
        for y in range(3):
            entries.append(add_all(dkg[x] * points[y]) + add_all(dvg[x] * vpoints[y]))
        entries.append(add_all(dkg[x]) + add_all(dvg[x]))
    frame_out(kframe, entries)
    for copy in copies:
        copy.wait()


def per_device(
    pair_rep, bias_weight, head_weight, queries, key_vectors, values, query_points, key_points,
    value_points, rotations, translations, residue_count, grad_output, grad_points, grad_pair,
):
    channels, heads = bias_weight.shape
    width = queries.shape[0] // heads
    qpoints = query_points.shape[1] // heads
    n_rows = queries.shape[1]
    n_cols = key_vectors.shape[1]
    logit_scale = math.sqrt(1.0 / 3.0)
    point_scale = math.sqrt(2.0 / (9.0 * qpoints))
    inner_scale = 1.0 / math.sqrt(width)
    coef_scale = 0.5 * logit_scale * point_scale
    hw = head_weight.reshape(1, heads)
    gpt = grad_points.transpose(0, 2, 1)

    vm = pl.BlockSpec(memory_space=pltpu.VMEM)
    hbm = pl.BlockSpec(memory_space=pltpu.HBM)
    big = (heads, n_rows, n_cols)
    flat = (heads * n_rows, n_cols)
    dma = pltpu.SemaphoreType.DMA
    inputs = (
        bias_weight.T, hw, grad_pair.transpose(1, 0, 2), queries.T, key_vectors, values,
        query_points, key_points, value_points, rotations, translations, grad_output.T, gpt,
        residue_count.reshape(1, 1),
    )
    like = lambda x: pltpu.VMEM(x.shape, x.dtype)
    inputs = tuple(
        pltpu.with_memory_space_constraint(x, pltpu.HBM) for x in inputs[:-1]
    ) + inputs[-1:]
    pg, kf, qf, wr = pl.pallas_call(
        functools.partial(
            mega_kernel, heads, n_rows, n_cols, logit_scale, inner_scale, coef_scale
        ),
        in_specs=[hbm] * 14 + [pl.BlockSpec(memory_space=pl.ANY)],
        out_specs=[vm] * 4,
        out_shape=[
            pltpu.VMEM(pair_rep.shape, BF16),
            jax.ShapeDtypeStruct((7, 8, 128), F32),
            jax.ShapeDtypeStruct((6, 8, 128), F32),
            jax.ShapeDtypeStruct((PAD, 128), F32),
        ],
        scratch_shapes=[
            *[like(x) for x in inputs],
            pltpu.VMEM(pair_rep.shape, BF16),
            pltpu.VMEM(big, F32),
            pltpu.VMEM(big, F32),
            *[pltpu.VMEM((n_rows * STRIDE, 128), F32)] * 4,
            *[pltpu.VMEM(flat, BF16)] * 4,
            pltpu.VMEM((n_rows * STRIDE, 128), F32),
            pltpu.VMEM((n_rows, 2 * PAD, 128), BF16),
            pltpu.VMEM((heads, 32, n_rows), F32),
            pltpu.VMEM((heads, 32, n_cols), F32),
            pltpu.VMEM((3, n_rows, 128), F32),
            pltpu.VMEM((n_rows, 2 * PAD, 128), F32),
            pltpu.VMEM((9, n_rows, 128), F32),
            pltpu.VMEM((32, 128), F32),
            pltpu.VMEM((32, 128), F32),
            pltpu.VMEM((32, 128), F32),
            pltpu.VMEM((3, 32, 128), F32),
            pltpu.VMEM((7, CORES, ZL * YN, 8, 128), F32),
            pltpu.VMEM((7, ZL * YN, 8, 128), F32),
            pltpu.VMEM((YN, 7, ZL, 8, 128), F32),
            pltpu.VMEM((YN - 1, 7, ZL, 8, 128), F32),
            pltpu.VMEM((ZL, 7, 8, 128), F32),
            pltpu.VMEM((ZL - 1, 7, 8, 128), F32),
            pltpu.VMEM((XN, ZH, 6, 8, 128), F32),
            pltpu.VMEM((XN - 1, ZH, 6, 8, 128), F32),
            pltpu.VMEM((ZH, 6, 8, 128), F32),
            pltpu.VMEM((6, 8, 128), F32),
            pltpu.VMEM((YN, PAD, 128), F32),
            pltpu.VMEM((XN * CORES, PAD, 128), F32),
            pltpu.VMEM((ZL * ZH, PAD, 128), F32),
            pltpu.VMEM((3, PAD, 128), F32),
            dma((4,)), dma((14,)),
            dma((4,)), dma((4,)),
            dma((7,)), dma((7,)),
            dma((3, 7)), dma((3, 7)),
            dma((3, 7)), dma((3, 7)),
            dma((4,)), dma((4,)),
            dma((17,)), dma((17,)),
        ],
        compiler_params=pltpu.CompilerParams(
            collective_id=0, has_side_effects=True, vmem_limit_bytes=VMEM_LIMIT
        ),
        name="mega",
    )(
        pair_rep, *inputs
    )
    share = 8
    late = (hw, query_points, key_points, value_points, rotations, translations, gpt)
    f32 = lambda *shape: jax.ShapeDtypeStruct(shape, F32)
    outs = pl.pallas_call(
        functools.partial(
            finish_kernel, heads, n_rows, logit_scale, inner_scale, coef_scale
        ),
        in_specs=[vm] * 11,
        out_specs=[hbm] + [vm] * 10,
        out_shape=[
            jax.ShapeDtypeStruct(pair_rep.shape, BF16),
            f32(share, heads * width),
            f32(3, share, 48),
            f32(3, 4, share),
            f32(share, heads * width),
            f32(share, heads * width),
            f32(3, share, 48),
            f32(3, share, 96),
            f32(3, 4, share),
            f32(heads, channels),
            f32(1, heads),
        ],
        scratch_shapes=[pltpu.VMEM((128, 128), F32), dma((4,))],
        compiler_params=pltpu.CompilerParams(vmem_limit_bytes=VMEM_LIMIT),
        name="finish",
    )(pg, kf, qf, wr, *late)
    (pair_grad, qgrad, qpgrad, qframe, kgrad, vgrad, kpgrad, vpgrad, kframe, weight, head) = outs
    flip = lambda x: x.transpose(0, 2, 1)
    return (
        pair_grad, qgrad.T, flip(qpgrad), qframe, kgrad.T, vgrad.T, flip(kpgrad), flip(vpgrad),
        kframe, weight.T, head.reshape(heads),
    )


def solution(mesh):
    return jax.shard_map(
        per_device,
        mesh=mesh,
        in_specs=(
            P("row", "col", None),
            P(),
            P(),
            P(None, "row"),
            P(None, "col"),
            P(None, "col"),
            P(None, None, "row"),
            P(None, None, "col"),
            P(None, None, "col"),
            P(),
            P(),
            P(),
            P(None, "row"),
            P(None, None, "row"),
            P("row", None, None),
        ),
        out_specs=(
            P("row", "col", None),
            P(None, ("row", "col")),
            P(None, None, ("row", "col")),
            P(None, None, ("row", "col")),
            P(None, ("col", "row")),
            P(None, ("col", "row")),
            P(None, None, ("col", "row")),
            P(None, None, ("col", "row")),
            P(None, None, ("col", "row")),
            P(),
            P(),
        ),
        check_vma=False,
    )
```
